128 devices in a mesh: gz: 16 (over z_hi, x, core), gy: 8 (over z_lo, y).
Axes of the slice: x: 4, y: 4, z: 4 (z_hi: 2, z_lo: 2; z = z_hi * 2 + z_lo), core: 2. Of those that a mesh axis runs over, the one named last changes fastest.
Arguments:
- source: float32 [512, 256, 256], P(('gz', 'gy')), may hold values from -8 to 8
- vertical: float32 [512], P(('gz', 'gy')), may hold values from 1 to 64
- reaction: float32 [512, 256, 256], P(('gz', 'gy')), may hold values from 0.05 to 2
Outputs:
- solution: float32 [512, 256, 256], P(('gz', 'gy'))
- norms: float32 [2], replicated
The draws below stay inside these ranges and needn't reach their ends.
All inputs are finite; a program needn't handle non-finite values.
Results may differ from the reference program's by a relative error of at most 0.0001.
Values sent between devices are 32-bit elements; how exact they have to be, the bound alone decides.
A program may use at most 192 MiB of HBM per device.

```python
import math
import jax
import jax.numpy as jnp

NX = 256
LEVELS = 5
SWITCH = 2
CYCLES = 2
SWEEPS = 2
COARSE = 4
NZ = 512


def draw_source(key, part):
    rough = jax.random.truncated_normal(key, -6.0, 6.0, (NZ, NX, NX), jnp.float32)
    return rough


def levels(key, dims, pieces, least, high):
    def one(position, parts):
        steps = jax.random.uniform(jax.random.fold_in(jax.random.fold_in(key, 6), position), (parts,), jnp.float32, least / len(pieces), high / len(pieces))
        return jnp.repeat(jnp.exp(steps), dims[position] // parts).reshape((-1,) + (1,) * (len(dims) - position - 1))

    level = one(*pieces[0])
    for cut in pieces[1:]:
        level = level * one(*cut)
    return level


def setup_inputs(seed: int = 0) -> dict:
    splits = jax.random.split(jax.random.key(seed), 4)
    return {
        "source": draw_source(jax.random.fold_in(splits[3], 71), 0),
        "vertical": jnp.clip(jnp.exp(math.log(64.0) - 4.158883 * jax.random.uniform(splits[1], (NZ,), jnp.float32) ** levels(splits[1], (NZ,), ((0, 128),), -0.2, 0.2)), 1.0, 64.0),
        "reaction": jnp.clip(jnp.exp(math.log(2.0) - 3.6888794 * jax.random.uniform(splits[2], (NZ, NX, NX), jnp.float32) ** levels(splits[2], (NZ, NX, NX), ((0, 128),), -0.2, 0.2)), 0.05, 2.0),
    }


DAMPING = 0.8
COUPLING = 1.0


def plane_sum(values):
    padded = jnp.pad(values, ((0, 0), (1, 1), (1, 1)))
    return padded[:, 2:, 1:-1] + padded[:, :-2, 1:-1] + padded[:, 1:-1, 2:] + padded[:, 1:-1, :-2]


def plane_residual(target, padded, vertical, diagonal, weight):
    centre = padded[1:-1]
    applied = diagonal * centre - vertical * (padded[2:] + padded[:-2]) - weight * plane_sum(centre)
    return target - applied


def around_sum(padded):
    return padded[2:, 1:-1] + padded[:-2, 1:-1] + padded[1:-1, 2:] + padded[1:-1, :-2]


def line_sum(values):
    return around_sum(jnp.pad(values, ((1, 1), (1, 1), (0, 0))))


def shift_left(values, filler):
    return jnp.concatenate([values[..., 1:], jnp.full_like(values[..., :1], filler)], axis=-1)


def shift_right(values, filler):
    return jnp.concatenate([jnp.full_like(values[..., :1], filler), values[..., :-1]], axis=-1)


def odd_even(lower, middle, upper, right):
    length = middle.shape[-1]
    if length == 1:
        return right / middle
    if length % 2 == 1:
        widths = [(0, 0)] * (middle.ndim - 1) + [(0, 1)]
        solved = odd_even(jnp.pad(lower, widths), jnp.pad(middle, widths, constant_values=1.0),
                          jnp.pad(upper, widths), jnp.pad(right, widths))
        return solved[..., :length]
    even_lower = lower[..., 0::2]
    even_middle = middle[..., 0::2]
    even_upper = upper[..., 0::2]
    even_right = right[..., 0::2]
    odd_lower = lower[..., 1::2]
    odd_middle = middle[..., 1::2]
    odd_upper = upper[..., 1::2]
    odd_right = right[..., 1::2]
    next_lower = shift_left(even_lower, 0.0)
    next_middle = shift_left(even_middle, 1.0)
    next_upper = shift_left(even_upper, 0.0)
    next_right = shift_left(even_right, 0.0)
    factor_left = -odd_lower / even_middle
    factor_right = -odd_upper / next_middle
    reduced = odd_even(factor_left * even_lower,
                       odd_middle + factor_left * even_upper + factor_right * next_lower,
                       factor_right * next_upper,
                       odd_right + factor_left * even_right + factor_right * next_right)
    before = shift_right(reduced, 0.0)
    evens = (even_right - even_lower * before - even_upper * reduced) / even_middle
    return jnp.stack([evens, reduced], axis=-1).reshape(middle.shape)


def line_relax(target, around, vertical, diagonal, weight):
    right = target + weight * around
    coupled = jnp.broadcast_to(-vertical, diagonal.shape)
    edge = jnp.zeros_like(coupled[..., :1])
    lower = jnp.concatenate([edge, coupled[..., 1:]], axis=-1)
    upper = jnp.concatenate([coupled[..., :-1], edge], axis=-1)
    return odd_even(lower, diagonal, upper, right)


def line_residual(target, values, around, vertical, diagonal, weight):
    padded = jnp.pad(values, ((0, 0), (0, 0), (1, 1)))
    applied = diagonal * values - vertical * (padded[..., 2:] + padded[..., :-2]) - weight * around
    return target - applied


def shrink_planes(values):
    depth, row_count, column_count = values.shape
    return values.reshape(depth, row_count // 2, 2, column_count // 2, 2).sum(axis=(2, 4)) * 0.25


def grow_planes(values):
    depth, row_count, column_count = values.shape
    spread = jnp.broadcast_to(values[:, :, None, :, None], (depth, row_count, 2, column_count, 2))
    return spread.reshape(depth, 2 * row_count, 2 * column_count)


def shrink_lines(values):
    row_count, column_count, depth = values.shape
    return values.reshape(row_count // 2, 2, column_count // 2, 2, depth).sum(axis=(1, 3)) * 0.25


def grow_lines(values):
    row_count, column_count, depth = values.shape
    spread = jnp.broadcast_to(values[:, None, :, None, :], (row_count, 2, column_count, 2, depth))
    return spread.reshape(2 * row_count, 2 * column_count, depth)


def pad_planes(values):
    return jnp.pad(values, ((1, 1), (0, 0), (0, 0)))


def reference(source, vertical, reaction):
    vertical_col = vertical.reshape(-1, 1, 1)
    reactions = [reaction]
    for height in range(1, LEVELS):
        if height < SWITCH:
            reactions.append(shrink_planes(reactions[-1]))
        elif height == SWITCH:
            reactions.append(jnp.transpose(shrink_planes(reactions[-1]), (1, 2, 0)))
        else:
            reactions.append(shrink_lines(reactions[-1]))
    weights = [COUPLING / 4.0 ** height for height in range(LEVELS)]
    diagonals = []
    for height in range(LEVELS):
        coefficient = vertical_col if height < SWITCH else vertical
        diagonals.append(2.0 * coefficient + 4.0 * weights[height] + reactions[height])

    def descend(height, values, target):
        weight = weights[height]
        diagonal = diagonals[height]
        if height < SWITCH:
            def sweep_plane(values):
                residual = plane_residual(target, pad_planes(values), vertical_col, diagonal, weight)
                return values + DAMPING * residual / diagonal

            for repeat in range(SWEEPS):
                values = sweep_plane(values)
            residual = plane_residual(target, pad_planes(values), vertical_col, diagonal, weight)
            coarse = shrink_planes(residual)
            if height + 1 == SWITCH:
                coarse = jnp.transpose(coarse, (1, 2, 0))
                correction = descend(height + 1, jnp.zeros_like(coarse), coarse)
                correction = jnp.transpose(correction, (2, 0, 1))
            else:
                correction = descend(height + 1, jnp.zeros_like(coarse), coarse)
            values = values + grow_planes(correction)
            for repeat in range(SWEEPS):
                values = sweep_plane(values)
            return values

        def relax_line(values):
            return line_relax(target, line_sum(values), vertical, diagonal, weight)

        if height == LEVELS - 1:
            for repeat in range(COARSE):
                values = relax_line(values)
            return values
        for repeat in range(SWEEPS):
            values = relax_line(values)
        residual = line_residual(target, values, line_sum(values), vertical, diagonal, weight)
        coarse = shrink_lines(residual)
        correction = descend(height + 1, jnp.zeros_like(coarse), coarse)
        values = values + grow_lines(correction)
        for repeat in range(SWEEPS):
            values = relax_line(values)
        return values

    solution = jnp.zeros_like(source)
    scores = []
    for cycle_index in range(CYCLES):
        solution = descend(0, solution, source)
        residual = plane_residual(source, pad_planes(solution), vertical_col, diagonals[0], weights[0])
        scores.append(jnp.mean(residual * residual))
    return solution, jnp.stack(scores)
```

```python
import functools

import jax
import jax.numpy as jnp
from jax import lax
from jax.experimental import pallas as pl
from jax.experimental.pallas import tpu as pltpu
from jax.sharding import PartitionSpec as P

F32 = jnp.float32
MESH = pl.DeviceIdType.MESH
CYCLES = 2
STEPS = 9
EVENTS = 11
OMEGA = 0.8
H = (1.0, 0.25, 1.0 / 16, 1.0 / 64, 1.0 / 256)
GROUP_Z = 16
GROUP_Y = 8
DEVICES = 128
PAD = 8


def snake_wide(g):
    high, quarter, core = lax.div(g, 8), lax.div(lax.rem(g, 8), 2), lax.rem(g, 2)
    return high * 8 + 2 * (quarter + high * (3 - 2 * quarter)) + core


def snake_narrow(g):
    high, quarter = lax.div(g, 4), lax.rem(g, 4)
    return high * 4 + quarter + high * (3 - 2 * quarter)


def dot(a, b):
    return jnp.dot(a, b, preferred_element_type=F32, precision=lax.Precision.HIGHEST)


def roll_lanes(v, s):
    return pltpu.roll(v, s % 128, 1)


def roll_rows(v, s):
    return pltpu.roll(v, s % 8, 0)


def lane_iota():
    return lax.broadcasted_iota(jnp.int32, (8, 128), 1)


def row_iota():
    return lax.broadcasted_iota(jnp.int32, (8, 128), 0)


def below(v, s):
    if s < 4:
        inner = lane_iota() % 4 >= s
        return [
            jnp.where(inner, roll_lanes(v[g], s), roll_lanes(v[g - 1], s - 4 if g else s + 4))
            for g in range(8)
        ]
    if s < 32:
        t = s // 4
        return [v[g - t] if g >= t else roll_lanes(v[g - t + 8], 8) for g in range(8)]
    return [roll_lanes(v[g], s // 4) for g in range(8)]


def above(v, s):
    if s < 4:
        inner = lane_iota() % 4 < 4 - s
        return [
            jnp.where(
                inner,
                roll_lanes(v[g], -s),
                roll_lanes(v[(g + 1) % 8], 4 - s if g < 7 else -4 - s),
            )
            for g in range(8)
        ]
    if s < 32:
        t = s // 4
        return [v[g + t] if g + t < 8 else roll_lanes(v[g + t - 8], -8) for g in range(8)]
    return [roll_lanes(v[g], -(s // 4)) for g in range(8)]


def kernel(
    source, vertical, reaction, out, norms,
    vb, g0, d0, j0, r0, wb, g1, d1, j1, r1, e1, compact, spread, lhs,
    send_as, recv_as, send_bs, recv_bs, send_a, recv_a, send_b, recv_b,
    back_b, got_b, back_a, got_a, grown,
    dl, vl, cf, val, hx, hy, ys, rhs2, rhs3, res,
    nacc, nb, nz,
    in_sem, z_send, z_recv, as_send, as_recv, bs_send, bs_recv, a_send, a_recv, b_send, b_recv,
    bb_send, bb_recv, ba_send, ba_recv, h_send, h_recv, n_send, n_recv,
):
    gz, gy = lax.axis_index("gz"), lax.axis_index("gy")
    me = gz * GROUP_Y + gy
    wide, narrow = snake_wide(gz), snake_narrow(gy)

    def device(d):
        d = lax.rem(d + DEVICES, DEVICES)
        return (lax.div(d, GROUP_Y), lax.rem(d, GROUP_Y))

    loads = []
    for p in range(4):
        for half in range(2):
            lanes = pl.ds(half * 128, 128)
            loads.append(pltpu.make_async_copy(source.at[p, :, lanes], g0.at[p, half], in_sem.at[0, p, half]))
            loads.append(pltpu.make_async_copy(reaction.at[p, :, lanes], r0.at[p, half], in_sem.at[1, p, half]))
    for copy in loads:
        copy.start()

    @pl.loop(0, 12)
    def _(i):
        for half in range(2):
            vb[lax.div(i, 6), lax.rem(i, 6), half] = jnp.zeros((256 + 2 * PAD, 128), F32)
        wb[lax.div(i, 6), lax.rem(i, 6)] = jnp.zeros((128 + 2 * PAD, 128), F32)

    @pl.when(wide == 0)
    def _():
        for e in range(EVENTS):
            hx[e, 0] = jnp.zeros((64, 128), F32)

    @pl.when(wide == GROUP_Z - 1)
    def _():
        for e in range(EVENTS):
            hx[e, 1] = jnp.zeros((64, 128), F32)

    @pl.when(narrow == 0)
    def _():
        for e in range(EVENTS):
            hy[e, 0] = jnp.zeros((16, 128), F32)

    @pl.when(narrow == GROUP_Y - 1)
    def _():
        for e in range(EVENTS):
            hy[e, 1] = jnp.zeros((16, 128), F32)

    from_lane = lax.broadcasted_iota(jnp.int32, (128, 128), 0)
    to_lane = lax.broadcasted_iota(jnp.int32, (128, 128), 1)
    for half in range(2):
        compact[half] = jnp.where(to_lane == 64 * half + from_lane // 2, 0.25, 0.0).astype(F32)
        spread[half] = jnp.where(from_lane == 64 * half + to_lane // 2, 1.0, 0.0).astype(F32)

    barrier = pltpu.get_barrier_semaphore()
    for k in range(1, GROUP_Z):
        pl.semaphore_signal(barrier, inc=1, device_id=(lax.rem(gz + k, GROUP_Z), gy), device_id_type=MESH)
    for k in range(1, GROUP_Y):
        pl.semaphore_signal(barrier, inc=1, device_id=(gz, lax.rem(gy + k, GROUP_Y)), device_id_type=MESH)

    rim = jnp.logical_or(gy == 0, gy == GROUP_Y - 1)

    @pl.when(gy == 0)
    def _():
        pl.semaphore_signal(barrier, inc=1, device_id=device(me - 1), device_id_type=MESH)

    @pl.when(gy == GROUP_Y - 1)
    def _():
        pl.semaphore_signal(barrier, inc=1, device_id=device(me + 1), device_id_type=MESH)

    pl.semaphore_wait(barrier, GROUP_Z + GROUP_Y - 2 + rim.astype(jnp.int32))

    def line_up(first, last, low, high, level, slot):
        up = pltpu.make_async_remote_copy(
            src_ref=last, dst_ref=low, send_sem=z_send.at[level, slot, 0],
            recv_sem=z_recv.at[level, slot, 0], device_id=device(me + 1), device_id_type=MESH,
        )
        down = pltpu.make_async_remote_copy(
            src_ref=first, dst_ref=high, send_sem=z_send.at[level, slot, 1],
            recv_sem=z_recv.at[level, slot, 1], device_id=device(me - 1), device_id_type=MESH,
        )

        @pl.when(me < DEVICES - 1)
        def _():
            up.start()

        @pl.when(me > 0)
        def _():
            down.start()

        @pl.when(me < DEVICES - 1)
        def _():
            up.wait_send()
            down.wait_recv()

        @pl.when(me > 0)
        def _():
            down.wait_send()
            up.wait_recv()

    def exchange0(slot):
        rows = pl.ds(PAD, 256)
        line_up(
            vb.at[slot, 1, :, rows], vb.at[slot, 4, :, rows],
            vb.at[slot, 0, :, rows], vb.at[slot, 5, :, rows], 0, slot,
        )

    def exchange1(slot):
        rows = pl.ds(PAD, 128)
        line_up(
            wb.at[slot, 1, rows], wb.at[slot, 4, rows], wb.at[slot, 0, rows], wb.at[slot, 5, rows],
            1, slot,
        )

    def all_wide(src, pick, dst, place, send_sem, recv_sem):
        copies = []
        for k in range(1, GROUP_Z):
            peer = lax.rem(gz + k, GROUP_Z)
            copies.append(
                pltpu.make_async_remote_copy(
                    src_ref=src.at[pick(peer)], dst_ref=dst.at[place], send_sem=send_sem.at[k],
                    recv_sem=recv_sem.at[k], device_id=(peer, gy), device_id_type=MESH,
                )
            )
        for copy in copies:
            copy.start()
        dst[place] = src[pick(gz)]
        for copy in copies:
            copy.wait()

    def all_narrow(src, pick, dst, place, send_sem, recv_sem):
        copies = []
        for k in range(1, GROUP_Y):
            peer = lax.rem(gy + k, GROUP_Y)
            copies.append(
                pltpu.make_async_remote_copy(
                    src_ref=src.at[pick(peer)], dst_ref=dst.at[place], send_sem=send_sem.at[k],
                    recv_sem=recv_sem.at[k], device_id=(gz, peer), device_id_type=MESH,
                )
            )
        for copy in copies:
            copy.start()
        dst[place] = src[pick(gy)]
        for copy in copies:
            copy.wait()

    BLOCK = 32
    lanes0 = lax.broadcasted_iota(jnp.int32, (BLOCK, 128), 1)

    def around0(slot, p, row):
        rows = pl.ds(PAD + row, BLOCK)
        centre = [vb[slot, p + 1, half, rows, :] for half in range(2)]
        left = [pltpu.roll(c, 1, 1) for c in centre]
        right = [pltpu.roll(c, 127, 1) for c in centre]
        sums = [
            jnp.where(lanes0 == 0, 0.0, left[0]) + jnp.where(lanes0 == 127, right[1], right[0]),
            jnp.where(lanes0 == 0, left[0], left[1]) + jnp.where(lanes0 == 127, 0.0, right[1]),
        ]
        coupled = vertical[p]
        total = []
        for half in range(2):
            beside = vb[slot, p + 1, half, pl.ds(PAD + row - 1, BLOCK), :]
            beside = beside + vb[slot, p + 1, half, pl.ds(PAD + row + 1, BLOCK), :]
            along = vb[slot, p, half, rows, :] + vb[slot, p + 2, half, rows, :]
            total.append(H[0] * (sums[half] + beside) + coupled * along)
        return centre, total

    def sweep0(old, new):
        @pl.loop(0, 4)
        def _(p):
            for row in range(0, 256, BLOCK):
                centre, total = around0(old, p, row)
                rows = pl.ds(row, BLOCK)
                for half in range(2):
                    fresh = (1.0 - OMEGA) * centre[half] + j0[p, half, rows, :] * (g0[p, half, rows, :] + total[half])
                    vb[new, p + 1, half, pl.ds(PAD + row, BLOCK), :] = fresh

    def residual0(slot, keep, sums):
        @pl.loop(0, 4)
        def _(p):
            for row in range(0, 256, BLOCK):
                centre, total = around0(slot, p, row)
                rows = pl.ds(row, BLOCK)
                for half in range(2):
                    left = g0[p, half, rows, :] + total[half] - d0[p, half, rows, :] * centre[half]
                    if keep:
                        r0[p, half, rows, :] = left
                    else:
                        nacc[sums] += (left * left).reshape(BLOCK // 8, 8, 128).sum(axis=0)

    lanes1 = lax.broadcasted_iota(jnp.int32, (BLOCK, 128), 1)

    def around1(slot, p, row):
        rows = pl.ds(PAD + row, BLOCK)
        centre = wb[slot, p + 1, rows, :]
        sums = jnp.where(lanes1 == 0, 0.0, pltpu.roll(centre, 1, 1))
        sums = sums + jnp.where(lanes1 == 127, 0.0, pltpu.roll(centre, 127, 1))
        sums = sums + wb[slot, p + 1, pl.ds(PAD + row - 1, BLOCK), :]
        sums = sums + wb[slot, p + 1, pl.ds(PAD + row + 1, BLOCK), :]
        along = wb[slot, p, rows, :] + wb[slot, p + 2, rows, :]
        return centre, H[1] * sums + vertical[p] * along

    def sweep1(old, store):
        @pl.loop(0, 4)
        def _(p):
            for row in range(0, 128, BLOCK):
                centre, total = around1(old, p, row)
                rows = pl.ds(row, BLOCK)
                store(p, row, (1.0 - OMEGA) * centre + j1[p, rows, :] * (g1[p, rows, :] + total))

    def store_second(p, row, fresh):
        wb[1, p + 1, pl.ds(PAD + row, BLOCK), :] = fresh

    def store_error(p, row, fresh):
        e1[p, pl.ds(row, BLOCK), :] = fresh

    def residual1():
        @pl.loop(0, 4)
        def _(p):
            for row in range(0, 128, BLOCK):
                centre, total = around1(1, p, row)
                rows = pl.ds(row, BLOCK)
                r1[p, rows, :] = g1[p, rows, :] + total - d1[p, rows, :] * centre

    def shrink0(src, dst):
        @pl.loop(0, 4)
        def _(p):
            total = jnp.zeros((128, 128), F32)
            for half in range(2):
                pairs = src[p, half, pl.ds(0, 128, 2), :] + src[p, half, pl.ds(1, 128, 2), :]
                total = total + dot(pairs, compact[half])
            dst[p] = total

    def shrink1(src):
        total = jnp.zeros((128, 128), F32)
        for a in range(2):
            for b in range(2):
                for p in range(4):
                    first = 4 * a + 2 * b
                    pairs = src[p, pl.ds(first, 16, 8), :] + src[p, pl.ds(first + 1, 16, 8), :]
                    lhs[a, pl.ds(b * 4 + p, 16, 8), :] = pairs
            total = total + dot(lhs[a], compact[a])
        return total

    for copy in loads:
        copy.wait()
    shrink0(r0, r1)

    @pl.loop(0, 4)
    def _(p):
        coupled = 2.0 * vertical[p]
        for half in range(2):
            for row in range(0, 256, 64):
                rows = pl.ds(row, 64)
                diagonal = coupled + 4.0 * H[0] + r0[p, half, rows, :]
                d0[p, half, rows, :] = diagonal
                j0[p, half, rows, :] = OMEGA / diagonal
        diagonal = coupled + 4.0 * H[1] + r1[p]
        d1[p] = diagonal
        j1[p] = OMEGA / diagonal

    send_as[:, 0:8, :] = shrink1(r1).reshape(16, 8, 128)
    plane = row_iota() % 4
    coupling = jnp.zeros((8, 128), F32)
    for p in range(4):
        coupling = jnp.where(plane == p, vertical[p], coupling)
    for x in range(16):
        send_as[x, 8:16, :] = coupling
    all_wide(send_as, snake_wide, recv_as, gz, as_send, as_recv)
    for f in range(2):
        turned = recv_as[:, 8 * f : 8 * f + 8, :].reshape(128, 128).T
        for a in range(2):
            send_bs[:, 2 * f + a] = turned[64 * a : 64 * a + 64].reshape(8, 8, 128)
    all_narrow(send_bs, snake_narrow, recv_bs, gy, bs_send, bs_recv)

    lane, row = lane_iota(), row_iota()
    odd_x = lax.div(lax.rem(lane, 8), 4) == 1

    def tile(g):
        return pl.ds(8 * g, 8)

    def shrink2(v):
        result = []
        for a in range(2):
            mine = []
            for g in range(8):
                t = v[a][g]
                t = t + jnp.where(odd_x, roll_lanes(t, 4), roll_lanes(t, -4))
                t = t + jnp.where(row % 2 == 1, roll_rows(t, 1), roll_rows(t, -1))
                mine.append(0.25 * t)
            result.append(mine)
        return result

    def shrink3(v):
        mine = []
        for g in range(8):
            t = v[0][g] + v[1][g]
            t = t + jnp.where(row % 4 >= 2, roll_rows(t, 2), roll_rows(t, -2))
            mine.append(0.25 * t)
        return [mine]

    couplings = [recv_bs[g, 2] for g in range(8)]
    for g in range(8):
        first = jnp.where(jnp.logical_and(lane < 8, lane % 4 == 0), 0.0, couplings[g]) if g == 0 else couplings[g]
        last = jnp.where(jnp.logical_and(lane >= 120, lane % 4 == 3), 0.0, couplings[g]) if g == 7 else couplings[g]
        vl[0, tile(g), :] = first
        vl[1, tile(g), :] = last
    react2 = [[recv_bs[g, a] for g in range(8)] for a in range(2)]
    react3 = shrink2(react2)
    react4 = shrink3(react3)
    for i, (level, lines) in enumerate(((2, react2[0]), (2, react2[1]), (3, react3[0]), (3, react3[1]), (4, react4[0]))):
        for g in range(8):
            dl[i, tile(g), :] = 2.0 * couplings[g] + 4.0 * H[level] + lines[g]

    @pl.loop(0, 5)
    def _(i):
        low = [-vl[0, tile(g), :] for g in range(8)]
        high = [-vl[1, tile(g), :] for g in range(8)]
        middle = [dl[i, tile(g), :] for g in range(8)]
        for k in range(STEPS):
            s = 1 << k
            middle_below, middle_above = below(middle, s), above(middle, s)
            left = [-low[g] / middle_below[g] for g in range(8)]
            right = [-high[g] / middle_above[g] for g in range(8)]
            for g in range(8):
                cf[i, 2 * k, tile(g), :] = left[g]
                cf[i, 2 * k + 1, tile(g), :] = right[g]
            high_below, low_above = below(high, s), above(low, s)
            middle = [middle[g] + left[g] * high_below[g] + right[g] * low_above[g] for g in range(8)]
            if k < STEPS - 1:
                low_below, high_above = below(low, s), above(high, s)
                low = [left[g] * low_below[g] for g in range(8)]
                high = [right[g] * high_above[g] for g in range(8)]
        for g in range(8):
            cf[i, 2 * STEPS, tile(g), :] = 1.0 / middle[g]

    first_of = {2: 0, 3: 2, 4: 4}
    count_of = {2: 2, 3: 2, 4: 1}

    def solve(level, right):
        solved = []
        for a in range(count_of[level]):
            i = first_of[level] + a
            r = right[a]
            for k in range(STEPS):
                s = 1 << k
                down, up = below(r, s), above(r, s)
                r = [
                    r[g] + cf[i, 2 * k, tile(g), :] * down[g] + cf[i, 2 * k + 1, tile(g), :] * up[g]
                    for g in range(8)
                ]
            solved.append([r[g] * cf[i, 2 * STEPS, tile(g), :] for g in range(8)])
        return solved

    def around(level, event, v):
        count = count_of[level]
        for a in range(count):
            for g in range(8):
                val[event, pl.ds((a * 8 + g) * 8, 8), :] = v[a][g]
        size = 8 * count
        ys[event, 0, 0:size, :] = val[event, pl.ds(0, size, 8), :]
        ys[event, 1, 0:size, :] = val[event, pl.ds(7, size, 8), :]
        ends = pl.ds(0, size)
        copies = []
        for side, src, dst, there in (
            (0, val.at[event, pl.ds(64 * (count - 1), 64)], hx.at[event, 0], (snake_wide(wide + 1), gy)),
            (1, val.at[event, pl.ds(0, 64)], hx.at[event, 1], (snake_wide(wide - 1), gy)),
            (2, ys.at[event, 1, ends], hy.at[event, 0, ends], (gz, snake_narrow(narrow + 1))),
            (3, ys.at[event, 0, ends], hy.at[event, 1, ends], (gz, snake_narrow(narrow - 1))),
        ):
            copies.append(
                pltpu.make_async_remote_copy(
                    src_ref=src, dst_ref=dst, send_sem=h_send.at[event, side],
                    recv_sem=h_recv.at[event, side], device_id=there, device_id_type=MESH,
                )
            )
        has = (wide < GROUP_Z - 1, wide > 0, narrow < GROUP_Y - 1, narrow > 0)
        for side in range(4):
            pl.when(has[side])(copies[side].start)
        for side in range(4):
            pl.when(has[side])(copies[side].wait_send)
            pl.when(has[side])(copies[side ^ 1].wait_recv)
        result = []
        for a in range(count):
            mine = []
            for g in range(8):
                left, right = hx[event, 0, tile(g), :], hx[event, 1, tile(g), :]
                if level == 2:
                    both = v[0][g] + v[1][g]
                    inner, outer = (both, left + v[0][g]) if a == 0 else (v[1][g] + right, both)
                    total = jnp.where(odd_x, roll_lanes(inner, 4), roll_lanes(outer, -4))
                elif level == 3:
                    total = left + v[1][g] if a == 0 else v[0][g] + right
                else:
                    total = left + right
                low = jnp.broadcast_to(hy[event, 0, pl.ds(a * 8 + g, 1), :], (8, 128))
                high = jnp.broadcast_to(hy[event, 1, pl.ds(a * 8 + g, 1), :], (8, 128))
                shift = 1 << (level - 2)
                total = total + jnp.where(row < shift, low, roll_rows(v[a][g], shift))
                total = total + jnp.where(row >= 8 - shift, high, roll_rows(v[a][g], -shift))
                mine.append(total)
            result.append(mine)
        return result

    def relax(level, target, total):
        return solve(
            level,
            [
                [target[a][g] + H[level] * total[a][g] for g in range(8)]
                for a in range(count_of[level])
            ],
        )

    def residual(level, target, v, total):
        result = []
        for a in range(count_of[level]):
            down, up = below(v[a], 1), above(v[a], 1)
            result.append([
                target[a][g] + H[level] * total[a][g] - dl[first_of[level] + a, tile(g), :] * v[a][g]
                + vl[0, tile(g), :] * down[g] + vl[1, tile(g), :] * up[g]
                for g in range(8)
            ])
        return result

    def load(ref, count):
        return [[ref[a, tile(g), :] for g in range(8)] for a in range(count)]

    def keep(ref, v):
        for a in range(len(v)):
            for g in range(8):
                ref[a, tile(g), :] = v[a][g]

    def lines():
        target2 = lambda: [[recv_b[g, a] for g in range(8)] for a in range(2)]
        v = solve(2, target2())
        v = relax(2, target2(), around(2, 0, v))
        r = residual(2, target2(), v, around(2, 1, v))
        keep(rhs2, v)
        keep(rhs3, shrink2(r))
        target3 = lambda: load(rhs3, 2)
        v = solve(3, target3())
        v = relax(3, target3(), around(3, 2, v))
        r = residual(3, target3(), v, around(3, 3, v))
        keep(res, v)
        target4 = shrink3(r)
        v = solve(4, target4)
        for e in range(3):
            v = relax(4, target4, around(4, 4 + e, v))
        w = load(res, 2)
        v = [[w[a][g] + v[0][g] for g in range(8)] for a in range(2)]
        v = relax(3, target3(), around(3, 7, v))
        v = relax(3, target3(), around(3, 8, v))
        w = load(rhs2, 2)
        v = [[w[a][g] + v[a][g] for g in range(8)] for a in range(2)]
        v = relax(2, target2(), around(2, 9, v))
        v = relax(2, target2(), around(2, 10, v))
        for a in range(2):
            for g in range(8):
                back_b[g, a] = v[a][g]

    nacc[...] = jnp.zeros((CYCLES, 8, 128), F32)

    @pl.loop(0, CYCLES)
    def _(cycle):
        this = lax.rem(cycle, 2)
        other = 1 - this
        sweep0(this, other)
        exchange0(other)
        sweep0(other, this)
        exchange0(this)
        residual0(this, True, 0)
        shrink0(r0, g1)

        @pl.loop(0, 4)
        def _(p):
            wb[0, p + 1, pl.ds(PAD, 128), :] = j1[p] * g1[p]

        exchange1(0)
        sweep1(0, store_second)
        exchange1(1)
        residual1()

        send_a[...] = shrink1(r1).reshape(16, 8, 128)
        all_wide(send_a, snake_wide, recv_a, gz, a_send, a_recv)
        turned = recv_a[...].reshape(128, 128).T
        for a in range(2):
            send_b[:, a] = turned[64 * a : 64 * a + 64].reshape(8, 8, 128)
        all_narrow(send_b, snake_narrow, recv_b, gy, b_send, b_recv)
        lines()
        all_narrow(back_b, lambda g: g, got_b, narrow, bb_send, bb_recv)
        turned = jnp.concatenate([got_b[:, a].reshape(64, 128) for a in range(2)], axis=0).T
        back_a[...] = turned.reshape(16, 8, 128)
        all_wide(back_a, lambda g: g, got_a, wide, ba_send, ba_recv)

        @pl.loop(0, 4)
        def _(p):
            wb[0, p + 1, pl.ds(PAD, 128), :] = wb[1, p + 1, pl.ds(PAD, 128), :]

        for a in range(2):
            grown[a] = dot(got_a[...].reshape(128, 128), spread[a])
        for a in range(2):
            for b in range(2):
                for p in range(4):
                    piece = grown[a, pl.ds(b * 4 + p, 16, 8), :]
                    for i in range(2):
                        rows = pl.ds(PAD + 4 * a + 2 * b + i, 16, 8)
                        wb[0, p + 1, rows, :] = wb[0, p + 1, rows, :] + piece
        exchange1(0)
        sweep1(0, store_second)
        exchange1(1)
        sweep1(1, store_error)

        @pl.loop(0, 4)
        def _(p):
            for half in range(2):
                piece = dot(e1[p], spread[half])
                for i in range(2):
                    rows = pl.ds(PAD + i, 128, 2)
                    vb[other, p + 1, half, rows, :] = vb[this, p + 1, half, rows, :] + piece

        exchange0(other)
        sweep0(other, this)
        exchange0(this)
        sweep0(this, other)
        exchange0(other)
        residual0(other, False, cycle)

    stores = []
    for p in range(4):
        for half in range(2):
            stores.append(
                pltpu.make_async_copy(
                    vb.at[CYCLES % 2, p + 1, half, pl.ds(PAD, 256)],
                    out.at[p, :, pl.ds(half * 128, 128)],
                    in_sem.at[0, p, half],
                )
            )
    for copy in stores:
        copy.start()

    all_narrow_sum(nacc, nb, gz, gy, n_send, n_recv)
    total = nb[0]
    for g in range(1, GROUP_Y):
        total = total + nb[g]
    nacc[...] = total
    all_wide_sum(nacc, nz, gz, gy, n_send, n_recv)
    total = nz[0]
    for g in range(1, GROUP_Z):
        total = total + nz[g]
    for c in range(CYCLES):
        norms[c] = jnp.sum(total[c]) * (1.0 / (512 * 256 * 256))
    for copy in stores:
        copy.wait()


def all_narrow_sum(src, dst, gz, gy, send_sem, recv_sem):
    copies = []
    for k in range(1, GROUP_Y):
        peer = lax.rem(gy + k, GROUP_Y)
        copies.append(
            pltpu.make_async_remote_copy(
                src_ref=src, dst_ref=dst.at[gy], send_sem=send_sem.at[0, k],
                recv_sem=recv_sem.at[0, k], device_id=(gz, peer), device_id_type=MESH,
            )
        )
    for copy in copies:
        copy.start()
    dst[gy] = src[...]
    for copy in copies:
        copy.wait()


def all_wide_sum(src, dst, gz, gy, send_sem, recv_sem):
    copies = []
    for k in range(1, GROUP_Z):
        peer = lax.rem(gz + k, GROUP_Z)
        copies.append(
            pltpu.make_async_remote_copy(
                src_ref=src, dst_ref=dst.at[gz], send_sem=send_sem.at[1, k],
                recv_sem=recv_sem.at[1, k], device_id=(peer, gy), device_id_type=MESH,
            )
        )
    for copy in copies:
        copy.start()
    dst[gz] = src[...]
    for copy in copies:
        copy.wait()


def vmem(*shape):
    return pltpu.VMEM(shape, F32)


def shards(source, vertical, reaction):
    dma = pltpu.SemaphoreType.DMA
    solved, norms = pl.pallas_call(
        kernel,
        out_shape=(
            jax.ShapeDtypeStruct((4, 256, 256), F32),
            jax.ShapeDtypeStruct((CYCLES,), F32),
        ),
        in_specs=[
            pl.BlockSpec(memory_space=pl.ANY),
            pl.BlockSpec(memory_space=pltpu.SMEM),
            pl.BlockSpec(memory_space=pl.ANY),
        ],
        out_specs=(pl.BlockSpec(memory_space=pl.ANY), pl.BlockSpec(memory_space=pltpu.SMEM)),
        scratch_shapes=[
            vmem(2, 6, 2, 256 + 2 * PAD, 128),
            vmem(4, 2, 256, 128),
            vmem(4, 2, 256, 128),
            vmem(4, 2, 256, 128),
            vmem(4, 2, 256, 128),
            vmem(2, 6, 128 + 2 * PAD, 128),
            vmem(4, 128, 128),
            vmem(4, 128, 128),
            vmem(4, 128, 128),
            vmem(4, 128, 128),
            vmem(4, 128, 128),
            vmem(2, 128, 128),
            vmem(2, 128, 128),
            vmem(2, 128, 128),
            vmem(16, 16, 128),
            vmem(16, 16, 128),
            vmem(8, 4, 8, 128),
            vmem(8, 4, 8, 128),
            vmem(16, 8, 128),
            vmem(16, 8, 128),
            vmem(8, 2, 8, 128),
            vmem(8, 2, 8, 128),
            vmem(8, 2, 8, 128),
            vmem(8, 2, 8, 128),
            vmem(16, 8, 128),
            vmem(16, 8, 128),
            vmem(2, 128, 128),
            vmem(5, 64, 128),
            vmem(2, 64, 128),
            vmem(5, 2 * STEPS + 1, 64, 128),
            vmem(EVENTS, 128, 128),
            vmem(EVENTS, 2, 64, 128),
            vmem(EVENTS, 2, 16, 128),
            vmem(EVENTS, 2, 16, 128),
            vmem(2, 64, 128),
            vmem(2, 64, 128),
            vmem(2, 64, 128),
            vmem(CYCLES, 8, 128),
            vmem(GROUP_Y, CYCLES, 8, 128),
            vmem(GROUP_Z, CYCLES, 8, 128),
            dma((2, 4, 2)),
            dma((2, 2, 2)),
            dma((2, 2, 2)),
            dma((GROUP_Z,)),
            dma((GROUP_Z,)),
            dma((GROUP_Y,)),
            dma((GROUP_Y,)),
            dma((GROUP_Z,)),
            dma((GROUP_Z,)),
            dma((GROUP_Y,)),
            dma((GROUP_Y,)),
            dma((GROUP_Y,)),
            dma((GROUP_Y,)),
            dma((GROUP_Z,)),
            dma((GROUP_Z,)),
            dma((EVENTS, 4)),
            dma((EVENTS, 4)),
            dma((2, GROUP_Z)),
            dma((2, GROUP_Z)),
        ],
        compiler_params=pltpu.CompilerParams(
            collective_id=0, has_side_effects=True, vmem_limit_bytes=48 * 1024 * 1024
        ),
    )(source, vertical, reaction)
    return solved, norms


def solution(mesh):
    planes = P(("gz", "gy"), None, None)
    return jax.shard_map(
        shards,
        mesh=mesh,
        in_specs=(planes, P(("gz", "gy")), planes),
        out_specs=(planes, P()),
        check_vma=False,
    )
```

```python
import functools

import jax
import jax.numpy as jnp
from jax import lax
from jax.experimental import pallas as pl
from jax.experimental.pallas import tpu as pltpu
from jax.sharding import PartitionSpec as P

F32 = jnp.float32
MESH = pl.DeviceIdType.MESH
CYCLES = 2
STEPS = 9
EVENTS = 11
OMEGA = 0.8
H = (1.0, 0.25, 1.0 / 16, 1.0 / 64, 1.0 / 256)
GROUP_Z = 16
GROUP_Y = 8
DEVICES = 128
PAD = 8


def snake_wide(g):
    high, quarter, core = lax.div(g, 8), lax.div(lax.rem(g, 8), 2), lax.rem(g, 2)
    return high * 8 + 2 * (quarter + high * (3 - 2 * quarter)) + core


def snake_narrow(g):
    high, quarter = lax.div(g, 4), lax.rem(g, 4)
    return high * 4 + quarter + high * (3 - 2 * quarter)


def dot(a, b):
    total = None
    for part in range(3):
        piece = a.astype(jnp.bfloat16)
        product = jnp.dot(piece, b, preferred_element_type=F32)
        total = product if total is None else total + product
        if part < 2:
            a = a - piece.astype(F32)
    return total


def roll_lanes(v, s):
    return pltpu.roll(v, s % 128, 1)


def roll_rows(v, s):
    return pltpu.roll(v, s % 8, 0)


def lane_iota():
    return lax.broadcasted_iota(jnp.int32, (8, 128), 1)


def row_iota():
    return lax.broadcasted_iota(jnp.int32, (8, 128), 0)


def below(v, s):
    if s < 4:
        inner = lane_iota() % 4 >= s
        return [
            jnp.where(inner, roll_lanes(v[g], s), roll_lanes(v[g - 1], s - 4 if g else s + 4))
            for g in range(8)
        ]
    if s < 32:
        t = s // 4
        return [v[g - t] if g >= t else roll_lanes(v[g - t + 8], 8) for g in range(8)]
    return [roll_lanes(v[g], s // 4) for g in range(8)]


def above(v, s):
    if s < 4:
        inner = lane_iota() % 4 < 4 - s
        return [
            jnp.where(
                inner,
                roll_lanes(v[g], -s),
                roll_lanes(v[(g + 1) % 8], 4 - s if g < 7 else -4 - s),
            )
            for g in range(8)
        ]
    if s < 32:
        t = s // 4
        return [v[g + t] if g + t < 8 else roll_lanes(v[g + t - 8], -8) for g in range(8)]
    return [roll_lanes(v[g], -(s // 4)) for g in range(8)]


def kernel(
    source, vertical, reaction, out, norms,
    vb, g0, d0, j0, r0, vt, wb, g1, d1, j1, r1, e1, compact, spread, lhs,
    send_as, recv_as, send_bs, recv_bs, send_a, recv_a, send_b, recv_b,
    back_b, got_b, back_a, got_a, beyond, ends, grown,
    dl, vl, cf, val, hx, hy, ys, rhs2, rhs3, res,
    nacc, nb, nz,
    in_sem, z_send, z_recv, c_send, c_recv,
    as_send, as_recv, bs_send, bs_recv, a_send, a_recv, b_send, b_recv,
    bb_send, bb_recv, ba_send, ba_recv, h_send, h_recv, n_send, n_recv,
):
    gz, gy = lax.axis_index("gz"), lax.axis_index("gy")
    me = gz * GROUP_Y + gy
    wide, narrow = snake_wide(gz), snake_narrow(gy)

    def device(d):
        d = lax.rem(d + DEVICES, DEVICES)
        return (lax.div(d, GROUP_Y), lax.rem(d, GROUP_Y))

    loads = []
    for p in range(4):
        for half in range(2):
            lanes = pl.ds(half * 128, 128)
            loads.append(pltpu.make_async_copy(source.at[p, :, lanes], g0.at[p + 2, half], in_sem.at[0, p, half]))
            loads.append(pltpu.make_async_copy(reaction.at[p, :, lanes], r0.at[p, half], in_sem.at[1, p, half]))
    for copy in loads:
        copy.start()

    @pl.loop(0, 30)
    def _(i):
        for half in range(2):
            for row in (0, PAD + 256):
                vb[lax.div(i, 10), lax.rem(i, 10), half, pl.ds(row, PAD), :] = jnp.zeros((PAD, 128), F32)

    @pl.loop(0, 28)
    def _(i):
        for row in (0, PAD + 128):
            wb[lax.div(i, 14), lax.rem(i, 14), pl.ds(row, PAD), :] = jnp.zeros((PAD, 128), F32)

    for p in range(4):
        vt[p + 4] = jnp.full((8, 128), vertical[p], F32)

    @pl.when(jnp.logical_or(me < 2, me >= DEVICES - 2))
    def _():
        @pl.loop(0, 30)
        def _(i):
            for half in range(2):
                vb[lax.div(i, 10), lax.rem(i, 10), half] = jnp.zeros((256 + 2 * PAD, 128), F32)

        @pl.loop(0, 28)
        def _(i):
            wb[lax.div(i, 14), lax.rem(i, 14)] = jnp.zeros((128 + 2 * PAD, 128), F32)

        for i in (0, 1, 6, 7):
            for half in range(2):
                g0[i, half] = jnp.zeros((256, 128), F32)
                j0[i, half] = jnp.zeros((256, 128), F32)
        for i in (0, 1, 2, 3, 8, 9, 10, 11):
            vt[i] = jnp.zeros((8, 128), F32)
            g1[i] = jnp.zeros((128, 128), F32)
            j1[i] = jnp.zeros((128, 128), F32)
        for i in (0, 2):
            got_a[i] = jnp.zeros((16, 8, 128), F32)
        for i in range(2):
            beyond[i] = jnp.zeros((32, 128), F32)

    @pl.when(wide == 0)
    def _():
        for e in range(EVENTS):
            hx[e, 0] = jnp.zeros((64, 128), F32)

    @pl.when(wide == GROUP_Z - 1)
    def _():
        for e in range(EVENTS):
            hx[e, 1] = jnp.zeros((64, 128), F32)

    @pl.when(narrow == 0)
    def _():
        for e in range(EVENTS):
            hy[e, 0] = jnp.zeros((16, 128), F32)

    @pl.when(narrow == GROUP_Y - 1)
    def _():
        for e in range(EVENTS):
            hy[e, 1] = jnp.zeros((16, 128), F32)

    from_lane = lax.broadcasted_iota(jnp.int32, (128, 128), 0)
    to_lane = lax.broadcasted_iota(jnp.int32, (128, 128), 1)
    for half in range(2):
        compact[half] = jnp.where(to_lane == 64 * half + from_lane // 2, 0.25, 0.0).astype(jnp.bfloat16)
        spread[half] = jnp.where(from_lane == 64 * half + to_lane // 2, 1.0, 0.0).astype(jnp.bfloat16)

    barrier = pltpu.get_barrier_semaphore()
    for k in range(1, GROUP_Z):
        pl.semaphore_signal(barrier, inc=1, device_id=(lax.rem(gz + k, GROUP_Z), gy), device_id_type=MESH)
    for k in range(1, GROUP_Y):
        pl.semaphore_signal(barrier, inc=1, device_id=(gz, lax.rem(gy + k, GROUP_Y)), device_id_type=MESH)

    for side, near, far in ((-1, 0, 1), (1, GROUP_Y - 1, GROUP_Y - 2)):
        for edge, steps in ((near, 1), (near, 2), (far, 2)):

            @pl.when(gy == edge)
            def _(side=side, steps=steps):
                pl.semaphore_signal(
                    barrier, inc=1, device_id=device(me + side * steps), device_id_type=MESH
                )

    outside = 2 * jnp.logical_or(gy == 0, gy == GROUP_Y - 1).astype(jnp.int32)
    outside = outside + jnp.logical_or(gy == 1, gy == GROUP_Y - 2).astype(jnp.int32)
    pl.semaphore_wait(barrier, GROUP_Z + GROUP_Y - 2 + outside)

    has_up, has_down = me < DEVICES - 1, me > 0

    class Pair:
        def __init__(self, up, down, send_sem, recv_sem, steps=1):
            self.steps = steps
            self.copies = [
                pltpu.make_async_remote_copy(
                    src_ref=src, dst_ref=dst, send_sem=send_sem.at[i], recv_sem=recv_sem.at[i],
                    device_id=device(me + shift), device_id_type=MESH,
                )
                for i, (src, dst), shift in ((0, up, steps), (1, down, -steps))
            ]

        def start(self):
            pl.when(me < DEVICES - self.steps)(self.copies[0].start)
            pl.when(me >= self.steps)(self.copies[1].start)

        def wait(self):
            @pl.when(me < DEVICES - self.steps)
            def _():
                self.copies[0].wait_send()
                self.copies[1].wait_recv()

            @pl.when(me >= self.steps)
            def _():
                self.copies[1].wait_send()
                self.copies[0].wait_recv()

    def pair(i, up, down, steps=1):
        return Pair(up, down, z_send.at[i], z_recv.at[i], steps)

    def exchange0(slot, i):
        rows = pl.ds(PAD, 256)
        both = pair(
            i,
            (vb.at[slot, 6, :, rows], vb.at[slot, 2, :, rows]),
            (vb.at[slot, 3, :, rows], vb.at[slot, 7, :, rows]),
        )
        both.start()
        both.wait()

    def all_wide(src, pick, dst, place, send_sem, recv_sem):
        copies = []
        for k in range(1, GROUP_Z):
            peer = lax.rem(gz + k, GROUP_Z)
            copies.append(
                pltpu.make_async_remote_copy(
                    src_ref=src.at[pick(peer)], dst_ref=dst.at[place], send_sem=send_sem.at[k],
                    recv_sem=recv_sem.at[k], device_id=(peer, gy), device_id_type=MESH,
                )
            )
        for copy in copies:
            copy.start()
        dst[place] = src[pick(gz)]

        def finish():
            for copy in copies:
                copy.wait()

        return finish

    def all_narrow(src, pick, dst, place, send_sem, recv_sem):
        copies = []
        for k in range(1, GROUP_Y):
            peer = lax.rem(gy + k, GROUP_Y)
            copies.append(
                pltpu.make_async_remote_copy(
                    src_ref=src.at[pick(peer)], dst_ref=dst.at[place], send_sem=send_sem.at[k],
                    recv_sem=recv_sem.at[k], device_id=(gz, peer), device_id_type=MESH,
                )
            )
        for copy in copies:
            copy.start()
        dst[place] = src[pick(gy)]

        def finish():
            for copy in copies:
                copy.wait()

        return finish

    BLOCK = 32
    lanes0 = lax.broadcasted_iota(jnp.int32, (BLOCK, 128), 1)

    def around0(slot, p, row):
        rows = pl.ds(PAD + row, BLOCK)
        centre = [vb[slot, p + 3, half, rows, :] for half in range(2)]
        left = [pltpu.roll(c, 1, 1) for c in centre]
        right = [pltpu.roll(c, 127, 1) for c in centre]
        sums = [
            jnp.where(lanes0 == 0, 0.0, left[0]) + jnp.where(lanes0 == 127, right[1], right[0]),
            jnp.where(lanes0 == 0, left[0], left[1]) + jnp.where(lanes0 == 127, 0.0, right[1]),
        ]
        coupled = jnp.broadcast_to(vt[p + 4, 0:1, :], (BLOCK, 128))
        total = []
        for half in range(2):
            beside = vb[slot, p + 3, half, pl.ds(PAD + row - 1, BLOCK), :]
            beside = beside + vb[slot, p + 3, half, pl.ds(PAD + row + 1, BLOCK), :]
            along = vb[slot, p + 2, half, rows, :] + vb[slot, p + 4, half, rows, :]
            total.append(H[0] * (sums[half] + beside) + coupled * along)
        return centre, total

    def sweep0(old, new, reach):
        @pl.loop(0, 4 + 2 * reach)
        def _(i):
            p = i - reach
            for row in range(0, 256, BLOCK):
                centre, total = around0(old, p, row)
                rows = pl.ds(row, BLOCK)
                for half in range(2):
                    fresh = g0[p + 2, half, rows, :] + total[half]
                    fresh = (1.0 - OMEGA) * centre[half] + j0[p + 2, half, rows, :] * fresh
                    vb[new, p + 3, half, pl.ds(PAD + row, BLOCK), :] = fresh

    def residual0(slot, keep, sums):
        @pl.loop(0, 4)
        def _(p):
            for row in range(0, 256, BLOCK):
                centre, total = around0(slot, p, row)
                rows = pl.ds(row, BLOCK)
                for half in range(2):
                    left = g0[p + 2, half, rows, :] + total[half] - d0[p, half, rows, :] * centre[half]
                    if keep:
                        r0[p, half, rows, :] = left
                    else:
                        nacc[sums] += (left * left).reshape(BLOCK // 8, 8, 128).sum(axis=0)

    lanes1 = lax.broadcasted_iota(jnp.int32, (BLOCK, 128), 1)

    def around1(slot, p, row):
        rows = pl.ds(PAD + row, BLOCK)
        centre = wb[slot, p + 5, rows, :]
        sums = jnp.where(lanes1 == 0, 0.0, pltpu.roll(centre, 1, 1))
        sums = sums + jnp.where(lanes1 == 127, 0.0, pltpu.roll(centre, 127, 1))
        sums = sums + wb[slot, p + 5, pl.ds(PAD + row - 1, BLOCK), :]
        sums = sums + wb[slot, p + 5, pl.ds(PAD + row + 1, BLOCK), :]
        along = wb[slot, p + 4, rows, :] + wb[slot, p + 6, rows, :]
        return centre, H[1] * sums + jnp.broadcast_to(vt[p + 4, 0:1, :], (BLOCK, 128)) * along

    def sweep1(old, store, reach):
        @pl.loop(0, 4 + 2 * reach)
        def _(i):
            p = i - reach
            for row in range(0, 128, BLOCK):
                centre, total = around1(old, p, row)
                rows = pl.ds(row, BLOCK)
                fresh = j1[p + 4, rows, :] * (g1[p + 4, rows, :] + total)
                store(p, row, (1.0 - OMEGA) * centre + fresh)

    def store_second(p, row, fresh):
        wb[1, p + 5, pl.ds(PAD + row, BLOCK), :] = fresh

    def store_error(p, row, fresh):
        e1[p + 3, pl.ds(row, BLOCK), :] = fresh

    def residual1():
        @pl.loop(0, 4)
        def _(p):
            for row in range(0, 128, BLOCK):
                centre, total = around1(1, p, row)
                rows = pl.ds(row, BLOCK)
                r1[p, rows, :] = g1[p + 4, rows, :] + total - d1[p, rows, :] * centre

    def shrink0(src, dst, first):
        @pl.loop(0, 4)
        def _(p):
            total = jnp.zeros((128, 128), F32)
            for half in range(2):
                pairs = src[p, half, pl.ds(0, 128, 2), :] + src[p, half, pl.ds(1, 128, 2), :]
                total = total + dot(pairs, compact[half])
            dst[p + first] = total

    def shrink1(src):
        total = jnp.zeros((128, 128), F32)
        for a in range(2):
            for b in range(2):
                for p in range(4):
                    first = 4 * a + 2 * b
                    pairs = src[p, pl.ds(first, 16, 8), :] + src[p, pl.ds(first + 1, 16, 8), :]
                    lhs[a, pl.ds(b * 4 + p, 16, 8), :] = pairs
            total = total + dot(lhs[a], compact[a])
        return total

    early = []
    for i in range(2):
        for half in range(2):
            lanes = pl.ds(half * 128, 128)
            early.append(
                pair(
                    4 + 2 * i + half,
                    (source.at[2 + i, :, lanes], g0.at[i, half]),
                    (source.at[i, :, lanes], g0.at[6 + i, half]),
                )
            )
    early.append(pair(2, (vt.at[4:8], vt.at[0:4]), (vt.at[4:8], vt.at[8:12])))
    for both in early:
        both.start()
    for copy in loads:
        copy.wait()
    shrink0(r0, r1, 0)

    @pl.loop(0, 4)
    def _(p):
        coupled = 2.0 * vertical[p]
        for half in range(2):
            for row in range(0, 256, 64):
                rows = pl.ds(row, 64)
                diagonal = coupled + 4.0 * H[0] + r0[p, half, rows, :]
                d0[p, half, rows, :] = diagonal
                j0[p + 2, half, rows, :] = OMEGA / diagonal
        diagonal = coupled + 4.0 * H[1] + r1[p]
        d1[p] = diagonal
        j1[p + 4] = OMEGA / diagonal

    send_as[:, 0:8, :] = shrink1(r1).reshape(16, 8, 128)
    plane = row_iota() % 4
    coupling = jnp.zeros((8, 128), F32)
    for p in range(4):
        coupling = jnp.where(plane == p, vertical[p], coupling)
    for x in range(16):
        send_as[x, 8:16, :] = coupling
    all_wide(send_as, snake_wide, recv_as, gz, as_send, as_recv)()
    for f in range(2):
        turned = recv_as[:, 8 * f : 8 * f + 8, :].reshape(128, 128).T
        for a in range(2):
            send_bs[:, 2 * f + a] = turned[64 * a : 64 * a + 64].reshape(8, 8, 128)
    finish = all_narrow(send_bs, snake_narrow, recv_bs, gy, bs_send, bs_recv)
    early.append(pair(8, (j0.at[4:6], j0.at[0:2]), (j0.at[2:4], j0.at[6:8])))
    late = pair(9, (j1.at[4:8], j1.at[0:4]), (j1.at[4:8], j1.at[8:12]))
    early[-1].start()
    late.start()
    finish()

    lane, row = lane_iota(), row_iota()
    odd_x = lax.div(lax.rem(lane, 8), 4) == 1

    def tile(g):
        return pl.ds(8 * g, 8)

    def shrink2(v):
        result = []
        for a in range(2):
            mine = []
            for g in range(8):
                t = v[a][g]
                t = t + jnp.where(odd_x, roll_lanes(t, 4), roll_lanes(t, -4))
                t = t + jnp.where(row % 2 == 1, roll_rows(t, 1), roll_rows(t, -1))
                mine.append(0.25 * t)
            result.append(mine)
        return result

    def shrink3(v):
        mine = []
        for g in range(8):
            t = v[0][g] + v[1][g]
            t = t + jnp.where(row % 4 >= 2, roll_rows(t, 2), roll_rows(t, -2))
            mine.append(0.25 * t)
        return [mine]

    couplings = [recv_bs[g, 2] for g in range(8)]
    for g in range(8):
        first = jnp.where(jnp.logical_and(lane < 8, lane % 4 == 0), 0.0, couplings[g]) if g == 0 else couplings[g]
        last = jnp.where(jnp.logical_and(lane >= 120, lane % 4 == 3), 0.0, couplings[g]) if g == 7 else couplings[g]
        vl[0, tile(g), :] = first
        vl[1, tile(g), :] = last
    react2 = [[recv_bs[g, a] for g in range(8)] for a in range(2)]
    react3 = shrink2(react2)
    react4 = shrink3(react3)
    for i, (level, lines) in enumerate(((2, react2[0]), (2, react2[1]), (3, react3[0]), (3, react3[1]), (4, react4[0]))):
        for g in range(8):
            dl[i, tile(g), :] = 2.0 * couplings[g] + 4.0 * H[level] + lines[g]

    @pl.loop(0, 5)
    def _(i):
        low = [-vl[0, tile(g), :] for g in range(8)]
        high = [-vl[1, tile(g), :] for g in range(8)]
        middle = [dl[i, tile(g), :] for g in range(8)]
        for k in range(STEPS):
            s = 1 << k
            middle_below, middle_above = below(middle, s), above(middle, s)
            left = [-low[g] / middle_below[g] for g in range(8)]
            right = [-high[g] / middle_above[g] for g in range(8)]
            for g in range(8):
                cf[i, 2 * k, tile(g), :] = left[g]
                cf[i, 2 * k + 1, tile(g), :] = right[g]
            high_below, low_above = below(high, s), above(low, s)
            middle = [middle[g] + left[g] * high_below[g] + right[g] * low_above[g] for g in range(8)]
            if k < STEPS - 1:
                low_below, high_above = below(low, s), above(high, s)
                low = [left[g] * low_below[g] for g in range(8)]
                high = [right[g] * high_above[g] for g in range(8)]
        for g in range(8):
            cf[i, 2 * STEPS, tile(g), :] = 1.0 / middle[g]

    first_of = {2: 0, 3: 2, 4: 4}
    count_of = {2: 2, 3: 2, 4: 1}

    def solve(level, right):
        solved = []
        for a in range(count_of[level]):
            i = first_of[level] + a
            r = right[a]
            for k in range(STEPS):
                s = 1 << k
                down, up = below(r, s), above(r, s)
                r = [
                    r[g] + cf[i, 2 * k, tile(g), :] * down[g] + cf[i, 2 * k + 1, tile(g), :] * up[g]
                    for g in range(8)
                ]
            solved.append([r[g] * cf[i, 2 * STEPS, tile(g), :] for g in range(8)])
        return solved

    def around(level, event, v, chunks):
        count = count_of[level]
        for a in range(count):
            for g in range(8):
                val[event, pl.ds((a * 8 + g) * 8, 8), :] = v[a][g]
        size = 8 * count
        ys[event, 0, 0:size, :] = val[event, pl.ds(0, size, 8), :]
        ys[event, 1, 0:size, :] = val[event, pl.ds(7, size, 8), :]
        span = pl.ds(0, size)
        copies = []
        for side, src, dst, there in (
            (0, val.at[event, pl.ds(64 * (count - 1), 64)], hx.at[event, 0], (snake_wide(wide + 1), gy)),
            (1, val.at[event, pl.ds(0, 64)], hx.at[event, 1], (snake_wide(wide - 1), gy)),
            (2, ys.at[event, 1, span], hy.at[event, 0, span], (gz, snake_narrow(narrow + 1))),
            (3, ys.at[event, 0, span], hy.at[event, 1, span], (gz, snake_narrow(narrow - 1))),
        ):
            copies.append(
                pltpu.make_async_remote_copy(
                    src_ref=src, dst_ref=dst, send_sem=h_send.at[event, side],
                    recv_sem=h_recv.at[event, side], device_id=there, device_id_type=MESH,
                )
            )
        has = (wide < GROUP_Z - 1, wide > 0, narrow < GROUP_Y - 1, narrow > 0)
        for side in range(4):
            pl.when(has[side])(copies[side].start)
        chunks[event + 2].start()
        for side in range(4):
            pl.when(has[side])(copies[side].wait_send)
            pl.when(has[side])(copies[side ^ 1].wait_recv)
        result = []
        for a in range(count):
            mine = []
            for g in range(8):
                left, right = hx[event, 0, tile(g), :], hx[event, 1, tile(g), :]
                if level == 2:
                    both = v[0][g] + v[1][g]
                    inner, outer = (both, left + v[0][g]) if a == 0 else (v[1][g] + right, both)
                    total = jnp.where(odd_x, roll_lanes(inner, 4), roll_lanes(outer, -4))
                elif level == 3:
                    total = left + v[1][g] if a == 0 else v[0][g] + right
                else:
                    total = left + right
                low = jnp.broadcast_to(hy[event, 0, pl.ds(a * 8 + g, 1), :], (8, 128))
                high = jnp.broadcast_to(hy[event, 1, pl.ds(a * 8 + g, 1), :], (8, 128))
                shift = 1 << (level - 2)
                total = total + jnp.where(row < shift, low, roll_rows(v[a][g], shift))
                total = total + jnp.where(row >= 8 - shift, high, roll_rows(v[a][g], -shift))
                mine.append(total)
            result.append(mine)
        return result

    def relax(level, target, total):
        return solve(
            level,
            [
                [target[a][g] + H[level] * total[a][g] for g in range(8)]
                for a in range(count_of[level])
            ],
        )

    def residual(level, target, v, total):
        result = []
        for a in range(count_of[level]):
            down, up = below(v[a], 1), above(v[a], 1)
            result.append([
                target[a][g] + H[level] * total[a][g] - dl[first_of[level] + a, tile(g), :] * v[a][g]
                + vl[0, tile(g), :] * down[g] + vl[1, tile(g), :] * up[g]
                for g in range(8)
            ])
        return result

    def load(ref, count):
        return [[ref[a, tile(g), :] for g in range(8)] for a in range(count)]

    def keep(ref, v):
        for a in range(len(v)):
            for g in range(8):
                ref[a, tile(g), :] = v[a][g]

    def lines(chunks):
        target2 = lambda: [[recv_b[g, a] for g in range(8)] for a in range(2)]
        v = solve(2, target2())
        v = relax(2, target2(), around(2, 0, v, chunks))
        r = residual(2, target2(), v, around(2, 1, v, chunks))
        keep(rhs2, v)
        keep(rhs3, shrink2(r))
        target3 = lambda: load(rhs3, 2)
        v = solve(3, target3())
        v = relax(3, target3(), around(3, 2, v, chunks))
        r = residual(3, target3(), v, around(3, 3, v, chunks))
        keep(res, v)
        target4 = shrink3(r)
        v = solve(4, target4)
        for e in range(3):
            v = relax(4, target4, around(4, 4 + e, v, chunks))
        w = load(res, 2)
        v = [[w[a][g] + v[0][g] for g in range(8)] for a in range(2)]
        v = relax(3, target3(), around(3, 7, v, chunks))
        v = relax(3, target3(), around(3, 8, v, chunks))
        w = load(rhs2, 2)
        v = [[w[a][g] + v[a][g] for g in range(8)] for a in range(2)]
        v = relax(2, target2(), around(2, 9, v, chunks))
        v = relax(2, target2(), around(2, 10, v, chunks))
        for a in range(2):
            for g in range(8):
                back_b[g, a] = v[a][g]

    nacc[...] = jnp.zeros((CYCLES, 8, 128), F32)

    for both in early:
        both.wait()

    @pl.loop(0, CYCLES)
    def _(cycle):
        this = lax.rem(cycle, 2)
        other = 1 - this

        @pl.when(cycle == 0)
        def _():
            @pl.loop(0, 8)
            def _(p):
                for half in range(2):
                    for row in range(0, 256, 64):
                        fresh = j0[p, half, pl.ds(row, 64), :] * g0[p, half, pl.ds(row, 64), :]
                        vb[2, p + 1, half, pl.ds(PAD + row, 64), :] = fresh

            sweep0(2, 0, 1)
            late.wait()

        @pl.when(cycle > 0)
        def _():
            sweep0(this, 2, 0)
            exchange0(2, 0)
            sweep0(2, this, 0)
            exchange0(this, 1)

        residual0(this, True, 0)
        shrink0(r0, g1, 4)
        both = pair(3, (g1.at[6:8], g1.at[2:4]), (g1.at[4:6], g1.at[8:10]))
        both.start()
        both.wait()

        @pl.loop(0, 8)
        def _(p):
            wb[0, p + 3, pl.ds(PAD, 128), :] = j1[p + 2] * g1[p + 2]

        sweep1(0, store_second, 1)
        residual1()

        chunks = []

        def chunk(up, down, steps=1):
            i = len(chunks)
            chunks.append(Pair(up, down, c_send.at[i], c_recv.at[i], steps))

        for i in range(2):
            chunk((g1.at[4 + i], g1.at[i]), (g1.at[6 + i], g1.at[10 + i]))
        rows = pl.ds(PAD, 128)
        chunk((wb.at[1, 8, rows], wb.at[1, 0, rows]), (wb.at[1, 5, rows], wb.at[1, 13, rows]), 2)
        for i in range(3):
            chunk(
                (wb.at[1, 5 + i, rows], wb.at[1, 1 + i, rows]),
                (wb.at[1, 6 + i, rows], wb.at[1, 10 + i, rows]),
            )
        for i in range(2):
            for half in range(2):
                for row in range(0, 256, 128):
                    rows = pl.ds(PAD + row, 128)
                    chunk(
                        (vb.at[this, 4 + i, half, rows], vb.at[this, i, half, rows]),
                        (vb.at[this, 4 + i, half, rows], vb.at[this, 8 + i, half, rows]),
                    )

        send_a[...] = shrink1(r1).reshape(16, 8, 128)
        finish = all_wide(send_a, snake_wide, recv_a, gz, a_send, a_recv)
        chunks[0].start()
        chunks[1].start()
        finish()
        turned = recv_a[...].reshape(128, 128).T
        for a in range(2):
            send_b[:, a] = turned[64 * a : 64 * a + 64].reshape(8, 8, 128)
        all_narrow(send_b, snake_narrow, recv_b, gy, b_send, b_recv)()
        lines(chunks)
        all_narrow(back_b, lambda g: g, got_b, narrow, bb_send, bb_recv)()
        turned = jnp.concatenate([got_b[:, a].reshape(64, 128) for a in range(2)], axis=0).T
        back_a[...] = turned.reshape(16, 8, 128)
        finish = all_wide(back_a, lambda g: g, got_a.at[1], wide, ba_send, ba_recv)
        chunks[13].start()
        finish()

        lhs[0] = got_a[1].reshape(128, 128)
        ends[0] = lhs[0, pl.ds(3, 32, 4), :]
        ends[1] = lhs[0, pl.ds(0, 32, 4), :]
        whole = pair(10, (got_a.at[1], got_a.at[0]), (got_a.at[1], got_a.at[2]))
        outer = pair(11, (ends.at[0], beyond.at[0]), (ends.at[1], beyond.at[1]), 2)
        whole.start()
        outer.start()
        for each in chunks:
            each.wait()
        whole.wait()
        outer.wait()
        for side in range(3):
            for a in range(2):
                grown[a] = dot(got_a[side].reshape(128, 128), spread[a])
            for a in range(2):
                for b in range(2):
                    for p in range(4):
                        piece = grown[a, pl.ds(b * 4 + p, 16, 8), :]
                        for i in range(2):
                            rows = pl.ds(PAD + 4 * a + 2 * b + i, 16, 8)
                            q = 4 * side + p + 1
                            wb[0, q, rows, :] = wb[1, q, rows, :] + piece
        for side in range(2):
            for a in range(2):
                grown[a, 0:32, :] = dot(beyond[side], spread[a])
                for b in range(2):
                    piece = grown[a, pl.ds(b, 16, 2), :]
                    for i in range(2):
                        rows = pl.ds(PAD + 4 * a + 2 * b + i, 16, 8)
                        wb[0, 13 * side, rows, :] = wb[1, 13 * side, rows, :] + piece
        sweep1(0, store_second, 4)
        sweep1(1, store_error, 3)

        @pl.loop(0, 10)
        def _(p):
            for half in range(2):
                piece = dot(e1[p], spread[half])
                for i in range(2):
                    rows = pl.ds(PAD + i, 128, 2)
                    vb[other, p, half, rows, :] = vb[this, p, half, rows, :] + piece

        sweep0(other, this, 2)
        sweep0(this, other, 1)
        residual0(other, False, cycle)

    stores = []
    for p in range(4):
        for half in range(2):
            stores.append(
                pltpu.make_async_copy(
                    vb.at[CYCLES % 2, p + 3, half, pl.ds(PAD, 256)],
                    out.at[p, :, pl.ds(half * 128, 128)],
                    in_sem.at[0, p, half],
                )
            )
    for copy in stores:
        copy.start()

    all_narrow_sum(nacc, nb, gz, gy, n_send, n_recv)
    total = nb[0]
    for g in range(1, GROUP_Y):
        total = total + nb[g]
    nacc[...] = total
    all_wide_sum(nacc, nz, gz, gy, n_send, n_recv)
    total = nz[0]
    for g in range(1, GROUP_Z):
        total = total + nz[g]
    for c in range(CYCLES):
        norms[c] = jnp.sum(total[c]) * (1.0 / (512 * 256 * 256))
    for copy in stores:
        copy.wait()


def all_narrow_sum(src, dst, gz, gy, send_sem, recv_sem):
    copies = []
    for k in range(1, GROUP_Y):
        peer = lax.rem(gy + k, GROUP_Y)
        copies.append(
            pltpu.make_async_remote_copy(
                src_ref=src, dst_ref=dst.at[gy], send_sem=send_sem.at[0, k],
                recv_sem=recv_sem.at[0, k], device_id=(gz, peer), device_id_type=MESH,
            )
        )
    for copy in copies:
        copy.start()
    dst[gy] = src[...]
    for copy in copies:
        copy.wait()


def all_wide_sum(src, dst, gz, gy, send_sem, recv_sem):
    copies = []
    for k in range(1, GROUP_Z):
        peer = lax.rem(gz + k, GROUP_Z)
        copies.append(
            pltpu.make_async_remote_copy(
                src_ref=src, dst_ref=dst.at[gz], send_sem=send_sem.at[1, k],
                recv_sem=recv_sem.at[1, k], device_id=(peer, gy), device_id_type=MESH,
            )
        )
    for copy in copies:
        copy.start()
    dst[gz] = src[...]
    for copy in copies:
        copy.wait()


def vmem(*shape):
    return pltpu.VMEM(shape, F32)


def shards(source, vertical, reaction):
    dma = pltpu.SemaphoreType.DMA
    solved, norms = pl.pallas_call(
        kernel,
        out_shape=(
            jax.ShapeDtypeStruct((4, 256, 256), F32),
            jax.ShapeDtypeStruct((CYCLES,), F32),
        ),
        in_specs=[
            pl.BlockSpec(memory_space=pl.ANY),
            pl.BlockSpec(memory_space=pltpu.SMEM),
            pl.BlockSpec(memory_space=pl.ANY),
        ],
        out_specs=(pl.BlockSpec(memory_space=pl.ANY), pl.BlockSpec(memory_space=pltpu.SMEM)),
        scratch_shapes=[
            vmem(3, 10, 2, 256 + 2 * PAD, 128),
            vmem(8, 2, 256, 128),
            vmem(4, 2, 256, 128),
            vmem(8, 2, 256, 128),
            vmem(4, 2, 256, 128),
            vmem(12, 8, 128),
            vmem(2, 14, 128 + 2 * PAD, 128),
            vmem(12, 128, 128),
            vmem(4, 128, 128),
            vmem(12, 128, 128),
            vmem(4, 128, 128),
            vmem(10, 128, 128),
            pltpu.VMEM((2, 128, 128), jnp.bfloat16),
            pltpu.VMEM((2, 128, 128), jnp.bfloat16),
            vmem(2, 128, 128),
            vmem(16, 16, 128),
            vmem(16, 16, 128),
            vmem(8, 4, 8, 128),
            vmem(8, 4, 8, 128),
            vmem(16, 8, 128),
            vmem(16, 8, 128),
            vmem(8, 2, 8, 128),
            vmem(8, 2, 8, 128),
            vmem(8, 2, 8, 128),
            vmem(8, 2, 8, 128),
            vmem(16, 8, 128),
            vmem(3, 16, 8, 128),
            vmem(2, 32, 128),
            vmem(2, 32, 128),
            vmem(2, 128, 128),
            vmem(5, 64, 128),
            vmem(2, 64, 128),
            vmem(5, 2 * STEPS + 1, 64, 128),
            vmem(EVENTS, 128, 128),
            vmem(EVENTS, 2, 64, 128),
            vmem(EVENTS, 2, 16, 128),
            vmem(EVENTS, 2, 16, 128),
            vmem(2, 64, 128),
            vmem(2, 64, 128),
            vmem(2, 64, 128),
            vmem(CYCLES, 8, 128),
            vmem(GROUP_Y, CYCLES, 8, 128),
            vmem(GROUP_Z, CYCLES, 8, 128),
            dma((2, 4, 2)),
            dma((12, 2)),
            dma((12, 2)),
            dma((14, 2)),
            dma((14, 2)),
            dma((GROUP_Z,)),
            dma((GROUP_Z,)),
            dma((GROUP_Y,)),
            dma((GROUP_Y,)),
            dma((GROUP_Z,)),
            dma((GROUP_Z,)),
            dma((GROUP_Y,)),
            dma((GROUP_Y,)),
            dma((GROUP_Y,)),
            dma((GROUP_Y,)),
            dma((GROUP_Z,)),
            dma((GROUP_Z,)),
            dma((EVENTS, 4)),
            dma((EVENTS, 4)),
            dma((2, GROUP_Z)),
            dma((2, GROUP_Z)),
        ],
        compiler_params=pltpu.CompilerParams(
            collective_id=0, has_side_effects=True, vmem_limit_bytes=48 * 1024 * 1024
        ),
    )(source, vertical, reaction)
    return solved, norms


def solution(mesh):
    planes = P(("gz", "gy"), None, None)
    return jax.shard_map(
        shards,
        mesh=mesh,
        in_specs=(planes, P(("gz", "gy")), planes),
        out_specs=(planes, P()),
        check_vma=False,
    )
```

```python
import functools

import jax
import jax.numpy as jnp
from jax import lax
from jax.experimental import pallas as pl
from jax.experimental.pallas import tpu as pltpu
from jax.sharding import PartitionSpec as P

F32 = jnp.float32
MESH = pl.DeviceIdType.MESH
CYCLES = 2
STEPS = 9
EVENTS = 11
OMEGA = 0.8
H = (1.0, 0.25, 1.0 / 16, 1.0 / 64, 1.0 / 256)
GROUP_Z = 16
GROUP_Y = 8
DEVICES = 128
PAD = 8


def device_of(a, b):
    wide = lax.div(a, 8) * 8 + lax.rem(lax.div(a, 2), 4) * 2 + lax.div(b, 4)
    return (wide, lax.rem(a, 2) * 4 + lax.rem(b, 4))


def place_wide(a):
    z, x = lax.div(a, 8) * 2 + lax.rem(a, 2), lax.rem(lax.div(a, 2), 4)
    return z * 4 + x + lax.rem(z, 2) * (3 - 2 * x)


def member_wide(place):
    z, x = lax.div(place, 4), lax.rem(place, 4)
    x = x + lax.rem(z, 2) * (3 - 2 * x)
    return (lax.div(z, 2) * 4 + x) * 2 + lax.rem(z, 2)


def place_narrow(b):
    core, y = lax.div(b, 4), lax.rem(b, 4)
    return y * 2 + core + lax.rem(y, 2) * (1 - 2 * core)


def member_narrow(place):
    y, core = lax.div(place, 2), lax.rem(place, 2)
    core = core + lax.rem(y, 2) * (1 - 2 * core)
    return core * 4 + y


def dot(a, b):
    total = None
    for part in range(3):
        piece = a.astype(jnp.bfloat16)
        product = jnp.dot(piece, b, preferred_element_type=F32)
        total = product if total is None else total + product
        if part < 2:
            a = a - piece.astype(F32)
    return total


def roll_lanes(v, s):
    return pltpu.roll(v, s % 128, 1)


def roll_rows(v, s):
    return pltpu.roll(v, s % 8, 0)


def lane_iota():
    return lax.broadcasted_iota(jnp.int32, (8, 128), 1)


def row_iota():
    return lax.broadcasted_iota(jnp.int32, (8, 128), 0)


def below(v, s):
    low = lax.div(lax.rem(lane_iota(), 16), 8) == 1
    result = []
    for g in range(8):
        c, y = divmod(g, 4)
        t = s // 4
        if s < 4:
            if y:
                other = roll_lanes(v[g - 1], s - 4)
            else:
                carry = roll_lanes(v[3], s - 12) if c else roll_lanes(v[7], s + 4)
                other = jnp.where(low, roll_lanes(v[4 * c + 3], s + 4), carry)
            result.append(jnp.where(lane_iota() % 4 >= s, roll_lanes(v[g], s), other))
        elif s < 16 and y >= t:
            result.append(v[g - t])
        elif s < 32:
            y = y - t + 4 if s < 16 else y
            carry = roll_lanes(v[y], -8) if c else roll_lanes(v[4 + y], 8)
            result.append(jnp.where(low, roll_lanes(v[4 * c + y], 8), carry))
        elif s == 32:
            result.append(v[y] if c else roll_lanes(v[4 + y], 16))
        else:
            result.append(roll_lanes(v[g], t))
    return result


def above(v, s):
    low = lax.div(lax.rem(lane_iota(), 16), 8) == 1
    result = []
    for g in range(8):
        c, y = divmod(g, 4)
        t = s // 4
        if s < 4:
            if y < 3:
                other = roll_lanes(v[g + 1], 4 - s)
            else:
                carry = roll_lanes(v[0], -4 - s) if c else roll_lanes(v[4], 12 - s)
                other = jnp.where(low, carry, roll_lanes(v[4 * c], -4 - s))
            result.append(jnp.where(lane_iota() % 4 < 4 - s, roll_lanes(v[g], -s), other))
        elif s < 16 and y + t < 4:
            result.append(v[g + t])
        elif s < 32:
            y = y + t - 4 if s < 16 else y
            carry = roll_lanes(v[y], -8) if c else roll_lanes(v[4 + y], 8)
            result.append(jnp.where(low, carry, roll_lanes(v[4 * c + y], -8)))
        elif s == 32:
            result.append(roll_lanes(v[y], -16) if c else v[4 + y])
        else:
            result.append(roll_lanes(v[g], -t))
    return result


def kernel(
    source, vertical, reaction, out, norms,
    v_a, v_b, v_c, v_d, g0, d0, j0, r0, vt, w_a, w_b, g1, d1, j1, r1, e1, compact, spread, lhs,
    send_as, recv_as, send_bs, recv_bs, send_a, recv_a, send_b, recv_b,
    back_b, got_b, back_a, got_a, beyond, ends, grown,
    dl, vl, cf, val, hx, xs, hy, ys, rhs2, rhs3, res,
    nacc, nb, nz,
    in_sem, z_send, z_recv, c_send, c_recv,
    as_send, as_recv, bs_send, bs_recv, a_send, a_recv, b_send, b_recv,
    bb_send, bb_recv, ba_send, ba_recv, h_send, h_recv, n_send, n_recv,
):
    gz, gy = lax.axis_index("gz"), lax.axis_index("gy")
    me = gz * GROUP_Y + gy
    core = lax.rem(gz, 2)
    ia = (lax.div(gz, 8) * 4 + lax.div(lax.rem(gz, 8), 2)) * 2 + lax.div(gy, 4)
    ib = core * 4 + lax.rem(gy, 4)
    wide, narrow = place_wide(ia), place_narrow(ib)

    def device(d):
        d = lax.rem(d + DEVICES, DEVICES)
        return (lax.div(d, GROUP_Y), lax.rem(d, GROUP_Y))

    loads = []
    for p in range(4):
        for half in range(2):
            lanes = pl.ds(half * 128, 128)
            loads.append(pltpu.make_async_copy(source.at[p, :, lanes], g0.at[p + 2, half], in_sem.at[0, p, half]))
            loads.append(pltpu.make_async_copy(reaction.at[p, :, lanes], r0.at[p, half], in_sem.at[1, p, half]))
    for copy in loads:
        copy.start()

    @pl.loop(0, 10)
    def _(i):
        for ref in (v_a, v_b, v_c, v_d):
            for half in range(2):
                for row in (0, PAD + 256):
                    ref[i, half, pl.ds(row, PAD), :] = jnp.zeros((PAD, 128), F32)

    @pl.loop(0, 14)
    def _(i):
        for ref in (w_a, w_b):
            for row in (0, PAD + 128):
                ref[i, pl.ds(row, PAD), :] = jnp.zeros((PAD, 128), F32)

    for p in range(4):
        vt[p + 4] = jnp.full((8, 128), vertical[p], F32)

    @pl.when(jnp.logical_or(me < 2, me >= DEVICES - 2))
    def _():
        @pl.loop(0, 10)
        def _(i):
            for ref in (v_a, v_b, v_c, v_d):
                for half in range(2):
                    ref[i, half] = jnp.zeros((256 + 2 * PAD, 128), F32)

        @pl.loop(0, 14)
        def _(i):
            for ref in (w_a, w_b):
                ref[i] = jnp.zeros((128 + 2 * PAD, 128), F32)

        for i in (0, 1, 6, 7):
            for half in range(2):
                g0[i, half] = jnp.zeros((256, 128), F32)
                j0[i, half] = jnp.zeros((256, 128), F32)
        for i in (0, 1, 2, 3, 8, 9, 10, 11):
            vt[i] = jnp.zeros((8, 128), F32)
            g1[i] = jnp.zeros((128, 128), F32)
            j1[i] = jnp.zeros((128, 128), F32)
        for i in (0, 2):
            got_a[i] = jnp.zeros((16, 8, 128), F32)
        for i in range(2):
            beyond[i] = jnp.zeros((32, 128), F32)

    @pl.when(wide == 0)
    def _():
        for e in range(EVENTS):
            hx[e, 0] = jnp.zeros((32, 128), F32)

    @pl.when(wide == GROUP_Z - 1)
    def _():
        for e in range(EVENTS):
            hx[e, 1] = jnp.zeros((32, 128), F32)

    @pl.when(narrow == 0)
    def _():
        for e in range(EVENTS):
            hy[e, 0] = jnp.zeros((16, 128), F32)

    @pl.when(narrow == GROUP_Y - 1)
    def _():
        for e in range(EVENTS):
            hy[e, 1] = jnp.zeros((16, 128), F32)

    from_lane = lax.broadcasted_iota(jnp.int32, (128, 128), 0)
    to_lane = lax.broadcasted_iota(jnp.int32, (128, 128), 1)
    for half in range(2):
        compact[half] = jnp.where(to_lane == 64 * half + from_lane // 2, 0.25, 0.0).astype(jnp.bfloat16)
        spread[half] = jnp.where(from_lane == 64 * half + to_lane // 2, 1.0, 0.0).astype(jnp.bfloat16)

    barrier = pltpu.get_barrier_semaphore()
    for k in range(1, GROUP_Z):
        pl.semaphore_signal(barrier, inc=1, device_id=device_of(lax.rem(ia + k, GROUP_Z), ib), device_id_type=MESH)
    for k in range(1, GROUP_Y):
        pl.semaphore_signal(barrier, inc=1, device_id=device_of(ia, lax.rem(ib + k, GROUP_Y)), device_id_type=MESH)

    for shift in (-2, -1, 1, 2):
        pl.semaphore_signal(barrier, inc=1, device_id=device(me + shift), device_id_type=MESH)
    pl.semaphore_wait(barrier, GROUP_Z + GROUP_Y + 2)

    has_up, has_down = me < DEVICES - 1, me > 0

    class Pair:
        def __init__(self, up, down, send_sem, recv_sem, steps=1):
            self.steps = steps
            self.copies = [
                pltpu.make_async_remote_copy(
                    src_ref=src, dst_ref=dst, send_sem=send_sem.at[i], recv_sem=recv_sem.at[i],
                    device_id=device(me + shift), device_id_type=MESH,
                )
                for i, (src, dst), shift in ((0, up, steps), (1, down, -steps))
            ]

        def start(self):
            pl.when(me < DEVICES - self.steps)(self.copies[0].start)
            pl.when(me >= self.steps)(self.copies[1].start)

        def wait(self):
            @pl.when(me < DEVICES - self.steps)
            def _():
                self.copies[0].wait_send()
                self.copies[1].wait_recv()

            @pl.when(me >= self.steps)
            def _():
                self.copies[1].wait_send()
                self.copies[0].wait_recv()

    def pair(i, up, down, steps=1):
        return Pair(up, down, z_send.at[i], z_recv.at[i], steps)

    def exchange0(slot, i):
        rows = pl.ds(PAD, 256)
        both = pair(
            i,
            (slot.at[6, :, rows], slot.at[2, :, rows]),
            (slot.at[3, :, rows], slot.at[7, :, rows]),
        )
        both.start()
        both.wait()

    def all_wide(src, pick, dst, place, send_sem, recv_sem):
        copies = []
        for k in range(1, GROUP_Z):
            peer = lax.rem(ia + k, GROUP_Z)
            copies.append(
                pltpu.make_async_remote_copy(
                    src_ref=src.at[pick(peer)], dst_ref=dst.at[place], send_sem=send_sem.at[k],
                    recv_sem=recv_sem.at[k], device_id=device_of(peer, ib), device_id_type=MESH,
                )
            )
        for copy in copies:
            copy.start()
        dst[place] = src[pick(ia)]

        def finish():
            for copy in copies:
                copy.wait()

        return finish

    def all_narrow(src, pick, dst, place, send_sem, recv_sem):
        copies = []
        for k in range(1, GROUP_Y):
            peer = lax.rem(ib + k, GROUP_Y)
            copies.append(
                pltpu.make_async_remote_copy(
                    src_ref=src.at[pick(peer)], dst_ref=dst.at[place], send_sem=send_sem.at[k],
                    recv_sem=recv_sem.at[k], device_id=device_of(ia, peer), device_id_type=MESH,
                )
            )
        for copy in copies:
            copy.start()
        dst[place] = src[pick(ib)]

        def finish():
            for copy in copies:
                copy.wait()

        return finish

    BLOCK = 32
    lanes0 = lax.broadcasted_iota(jnp.int32, (BLOCK, 128), 1)

    def around0(slot, p, row):
        rows = pl.ds(PAD + row, BLOCK)
        centre = [slot[p + 3, half, rows, :] for half in range(2)]
        left = [pltpu.roll(c, 1, 1) for c in centre]
        right = [pltpu.roll(c, 127, 1) for c in centre]
        sums = [
            jnp.where(lanes0 == 0, 0.0, left[0]) + jnp.where(lanes0 == 127, right[1], right[0]),
            jnp.where(lanes0 == 0, left[0], left[1]) + jnp.where(lanes0 == 127, 0.0, right[1]),
        ]
        coupled = jnp.broadcast_to(vt[p + 4, 0:1, :], (BLOCK, 128))
        total = []
        for half in range(2):
            beside = slot[p + 3, half, pl.ds(PAD + row - 1, BLOCK), :]
            beside = beside + slot[p + 3, half, pl.ds(PAD + row + 1, BLOCK), :]
            along = slot[p + 2, half, rows, :] + slot[p + 4, half, rows, :]
            total.append(H[0] * (sums[half] + beside) + coupled * along)
        return centre, total

    def sweep0(old, new, reach):
        @pl.loop(0, 4 + 2 * reach)
        def _(i):
            p = i - reach
            for row in range(0, 256, BLOCK):
                centre, total = around0(old, p, row)
                rows = pl.ds(row, BLOCK)
                for half in range(2):
                    fresh = g0[p + 2, half, rows, :] + total[half]
                    fresh = (1.0 - OMEGA) * centre[half] + j0[p + 2, half, rows, :] * fresh
                    new[p + 3, half, pl.ds(PAD + row, BLOCK), :] = fresh

    def residual0(slot, keep, sums):
        @pl.loop(0, 4)
        def _(p):
            for row in range(0, 256, BLOCK):
                centre, total = around0(slot, p, row)
                rows = pl.ds(row, BLOCK)
                for half in range(2):
                    left = g0[p + 2, half, rows, :] + total[half] - d0[p, half, rows, :] * centre[half]
                    if keep:
                        r0[p, half, rows, :] = left
                    else:
                        nacc[sums] += (left * left).reshape(BLOCK // 8, 8, 128).sum(axis=0)

    lanes1 = lax.broadcasted_iota(jnp.int32, (BLOCK, 128), 1)

    def around1(slot, p, row):
        rows = pl.ds(PAD + row, BLOCK)
        centre = slot[p + 5, rows, :]
        sums = jnp.where(lanes1 == 0, 0.0, pltpu.roll(centre, 1, 1))
        sums = sums + jnp.where(lanes1 == 127, 0.0, pltpu.roll(centre, 127, 1))
        sums = sums + slot[p + 5, pl.ds(PAD + row - 1, BLOCK), :]
        sums = sums + slot[p + 5, pl.ds(PAD + row + 1, BLOCK), :]
        along = slot[p + 4, rows, :] + slot[p + 6, rows, :]
        return centre, H[1] * sums + jnp.broadcast_to(vt[p + 4, 0:1, :], (BLOCK, 128)) * along

    def sweep1(old, store, reach):
        @pl.loop(0, 4 + 2 * reach)
        def _(i):
            p = i - reach
            for row in range(0, 128, BLOCK):
                centre, total = around1(old, p, row)
                rows = pl.ds(row, BLOCK)
                fresh = j1[p + 4, rows, :] * (g1[p + 4, rows, :] + total)
                store(p, row, (1.0 - OMEGA) * centre + fresh)

    def store_second(p, row, fresh):
        w_b[p + 5, pl.ds(PAD + row, BLOCK), :] = fresh

    def store_error(p, row, fresh):
        e1[p + 3, pl.ds(row, BLOCK), :] = fresh

    def residual1():
        @pl.loop(0, 4)
        def _(p):
            for row in range(0, 128, BLOCK):
                centre, total = around1(w_b, p, row)
                rows = pl.ds(row, BLOCK)
                r1[p, rows, :] = g1[p + 4, rows, :] + total - d1[p, rows, :] * centre

    def shrink0(src, dst, first):
        @pl.loop(0, 4)
        def _(p):
            total = jnp.zeros((128, 128), F32)
            for half in range(2):
                pairs = src[p, half, pl.ds(0, 128, 2), :] + src[p, half, pl.ds(1, 128, 2), :]
                total = total + dot(pairs, compact[half])
            dst[p + first] = total

    def shrink1(src):
        total = jnp.zeros((128, 128), F32)
        for a in range(2):
            for b in range(2):
                for p in range(4):
                    first = 4 * a + 2 * b
                    pairs = src[p, pl.ds(first, 16, 8), :] + src[p, pl.ds(first + 1, 16, 8), :]
                    lhs[a, pl.ds(b * 4 + p, 16, 8), :] = pairs
            total = total + dot(lhs[a], compact[a])
        return total

    early = []
    for i in range(2):
        for half in range(2):
            lanes = pl.ds(half * 128, 128)
            early.append(
                pair(
                    4 + 2 * i + half,
                    (source.at[2 + i, :, lanes], g0.at[i, half]),
                    (source.at[i, :, lanes], g0.at[6 + i, half]),
                )
            )
    early.append(pair(2, (vt.at[4:8], vt.at[0:4]), (vt.at[4:8], vt.at[8:12])))
    for both in early:
        both.start()
    for copy in loads:
        copy.wait()
    shrink0(r0, r1, 0)

    @pl.loop(0, 4)
    def _(p):
        coupled = 2.0 * vertical[p]
        for half in range(2):
            for row in range(0, 256, 64):
                rows = pl.ds(row, 64)
                diagonal = coupled + 4.0 * H[0] + r0[p, half, rows, :]
                d0[p, half, rows, :] = diagonal
                j0[p + 2, half, rows, :] = OMEGA / diagonal
        diagonal = coupled + 4.0 * H[1] + r1[p]
        d1[p] = diagonal
        j1[p + 4] = OMEGA / diagonal

    send_as[:, 0:8, :] = shrink1(r1).reshape(16, 8, 128)
    plane = row_iota() % 4
    coupling = jnp.zeros((8, 128), F32)
    for p in range(4):
        coupling = jnp.where(plane == p, vertical[p], coupling)
    for x in range(16):
        send_as[x, 8:16, :] = coupling
    all_wide(send_as, place_wide, recv_as, ia, as_send, as_recv)()
    for f in range(2):
        turned = recv_as[:, 8 * f : 8 * f + 8, :].reshape(128, 128).T
        for a in range(2):
            send_bs[:, 2 * f + a] = turned[64 * a : 64 * a + 64].reshape(8, 8, 128)
    finish = all_narrow(send_bs, place_narrow, recv_bs, ib, bs_send, bs_recv)
    early.append(pair(8, (j0.at[4:6], j0.at[0:2]), (j0.at[2:4], j0.at[6:8])))
    late = pair(9, (j1.at[4:8], j1.at[0:4]), (j1.at[4:8], j1.at[8:12]))
    early[-1].start()
    late.start()
    finish()

    lane, row = lane_iota(), row_iota()
    odd_x = lax.div(lax.rem(lane, 8), 4) == 1

    def tile(g):
        return pl.ds(8 * g, 8)

    def shrink2(v):
        result = []
        for a in range(2):
            mine = []
            for g in range(8):
                t = v[a][g]
                t = t + jnp.where(odd_x, roll_lanes(t, 4), roll_lanes(t, -4))
                t = t + jnp.where(row % 2 == 1, roll_rows(t, 1), roll_rows(t, -1))
                mine.append(0.25 * t)
            result.append(mine)
        return result

    def shrink3(v):
        mine = []
        for g in range(8):
            t = v[0][g] + v[1][g]
            t = t + jnp.where(row % 4 >= 2, roll_rows(t, 2), roll_rows(t, -2))
            mine.append(0.25 * t)
        return [mine]

    couplings = [recv_bs[g, 2] for g in range(8)]
    for g in range(8):
        first = jnp.where(jnp.logical_and(lane < 8, lane % 4 == 0), 0.0, couplings[g]) if g == 0 else couplings[g]
        last = jnp.where(jnp.logical_and(lane >= 120, lane % 4 == 3), 0.0, couplings[g]) if g == 7 else couplings[g]
        vl[0, tile(g), :] = first
        vl[1, tile(g), :] = last
    react2 = [[recv_bs[g, a] for g in range(8)] for a in range(2)]
    react3 = shrink2(react2)
    react4 = shrink3(react3)
    for i, (level, lines) in enumerate(((2, react2[0]), (2, react2[1]), (3, react3[0]), (3, react3[1]), (4, react4[0]))):
        for g in range(8):
            dl[i, tile(g), :] = 2.0 * couplings[g] + 4.0 * H[level] + lines[g]

    @pl.loop(0, 5)
    def _(i):
        low = [-vl[0, tile(g), :] for g in range(8)]
        high = [-vl[1, tile(g), :] for g in range(8)]
        middle = [dl[i, tile(g), :] for g in range(8)]
        for k in range(STEPS):
            s = 1 << k
            middle_below, middle_above = below(middle, s), above(middle, s)
            left = [-low[g] / middle_below[g] for g in range(8)]
            right = [-high[g] / middle_above[g] for g in range(8)]
            for g in range(8):
                cf[i, 2 * k, tile(g), :] = left[g]
                cf[i, 2 * k + 1, tile(g), :] = right[g]
            high_below, low_above = below(high, s), above(low, s)
            middle = [middle[g] + left[g] * high_below[g] + right[g] * low_above[g] for g in range(8)]
            if k < STEPS - 1:
                low_below, high_above = below(low, s), above(high, s)
                low = [left[g] * low_below[g] for g in range(8)]
                high = [right[g] * high_above[g] for g in range(8)]
        for g in range(8):
            cf[i, 2 * STEPS, tile(g), :] = 1.0 / middle[g]

    first_of = {2: 0, 3: 2, 4: 4}
    count_of = {2: 2, 3: 2, 4: 1}

    def solve(level, right):
        solved = []
        for a in range(count_of[level]):
            i = first_of[level] + a
            r = right[a]
            for k in range(STEPS):
                s = 1 << k
                down, up = below(r, s), above(r, s)
                r = [
                    r[g] + cf[i, 2 * k, tile(g), :] * down[g] + cf[i, 2 * k + 1, tile(g), :] * up[g]
                    for g in range(8)
                ]
            solved.append([r[g] * cf[i, 2 * STEPS, tile(g), :] for g in range(8)])
        return solved

    def around(level, event, v, chunks):
        count = count_of[level]
        for a in range(count):
            for g in range(8):
                val[event, pl.ds((a * 8 + g) * 8, 8), :] = v[a][g]
        size = 8 * count
        ys[event, 0, 0:size, :] = val[event, pl.ds(0, size, 8), :]
        ys[event, 1, 0:size, :] = val[event, pl.ds(7, size, 8), :]
        span = pl.ds(0, size)
        copies = []
        for j in range(4):
            first, last = v[0], v[count - 1]
            if level == 2:
                go_down = jnp.where(odd_x, roll_lanes(first[2 * j + 1], 4), first[2 * j])
                go_up = jnp.where(odd_x, last[2 * j + 1], roll_lanes(last[2 * j], -4))
            else:
                go_down = jnp.where(odd_x, first[2 * j + 1], first[2 * j])
                go_up = jnp.where(odd_x, last[2 * j + 1], last[2 * j])
            xs[event, 0, tile(j), :] = go_down
            xs[event, 1, tile(j), :] = go_up
        for side, src, dst, there in (
            (0, xs.at[event, 1], hx.at[event, 0], device_of(member_wide(wide + 1), ib)),
            (1, xs.at[event, 0], hx.at[event, 1], device_of(member_wide(wide - 1), ib)),
            (2, ys.at[event, 1, span], hy.at[event, 0, span], device_of(ia, member_narrow(narrow + 1))),
            (3, ys.at[event, 0, span], hy.at[event, 1, span], device_of(ia, member_narrow(narrow - 1))),
        ):
            copies.append(
                pltpu.make_async_remote_copy(
                    src_ref=src, dst_ref=dst, send_sem=h_send.at[event, side],
                    recv_sem=h_recv.at[event, side], device_id=there, device_id_type=MESH,
                )
            )
        has = (wide < GROUP_Z - 1, wide > 0, narrow < GROUP_Y - 1, narrow > 0)
        for side in range(4):
            pl.when(has[side])(copies[side].start)
        chunks[event + 2].start()
        for side in range(4):
            pl.when(has[side])(copies[side].wait_send)
            pl.when(has[side])(copies[side ^ 1].wait_recv)
        result = []
        for a in range(count):
            mine = []
            for g in range(8):
                left, right = hx[event, 0, tile(g // 2), :], hx[event, 1, tile(g // 2), :]
                if level == 2:
                    left = left if g % 2 else roll_lanes(left, 4)
                    right = roll_lanes(right, -4) if g % 2 else right
                elif g % 2:
                    left = jnp.where(odd_x, left, roll_lanes(left, -4))
                    right = jnp.where(odd_x, right, roll_lanes(right, -4))
                else:
                    left = jnp.where(odd_x, roll_lanes(left, 4), left)
                    right = jnp.where(odd_x, roll_lanes(right, 4), right)
                if level == 2:
                    both = v[0][g] + v[1][g]
                    inner, outer = (both, left + v[0][g]) if a == 0 else (v[1][g] + right, both)
                    total = jnp.where(odd_x, roll_lanes(inner, 4), roll_lanes(outer, -4))
                elif level == 3:
                    total = left + v[1][g] if a == 0 else v[0][g] + right
                else:
                    total = left + right
                low = jnp.broadcast_to(hy[event, 0, pl.ds(a * 8 + g, 1), :], (8, 128))
                high = jnp.broadcast_to(hy[event, 1, pl.ds(a * 8 + g, 1), :], (8, 128))
                shift = 1 << (level - 2)
                total = total + jnp.where(row < shift, low, roll_rows(v[a][g], shift))
                total = total + jnp.where(row >= 8 - shift, high, roll_rows(v[a][g], -shift))
                mine.append(total)
            result.append(mine)
        return result

    def relax(level, target, total):
        return solve(
            level,
            [
                [target[a][g] + H[level] * total[a][g] for g in range(8)]
                for a in range(count_of[level])
            ],
        )

    def residual(level, target, v, total):
        result = []
        for a in range(count_of[level]):
            down, up = below(v[a], 1), above(v[a], 1)
            result.append([
                target[a][g] + H[level] * total[a][g] - dl[first_of[level] + a, tile(g), :] * v[a][g]
                + vl[0, tile(g), :] * down[g] + vl[1, tile(g), :] * up[g]
                for g in range(8)
            ])
        return result

    def load(ref, count):
        return [[ref[a, tile(g), :] for g in range(8)] for a in range(count)]

    def keep(ref, v):
        for a in range(len(v)):
            for g in range(8):
                ref[a, tile(g), :] = v[a][g]

    def lines(chunks):
        target2 = lambda: [[recv_b[g, a] for g in range(8)] for a in range(2)]
        v = solve(2, target2())
        v = relax(2, target2(), around(2, 0, v, chunks))
        r = residual(2, target2(), v, around(2, 1, v, chunks))
        keep(rhs2, v)
        keep(rhs3, shrink2(r))
        target3 = lambda: load(rhs3, 2)
        v = solve(3, target3())
        v = relax(3, target3(), around(3, 2, v, chunks))
        r = residual(3, target3(), v, around(3, 3, v, chunks))
        keep(res, v)
        target4 = shrink3(r)
        v = solve(4, target4)
        for e in range(3):
            v = relax(4, target4, around(4, 4 + e, v, chunks))
        w = load(res, 2)
        v = [[w[a][g] + v[0][g] for g in range(8)] for a in range(2)]
        v = relax(3, target3(), around(3, 7, v, chunks))
        v = relax(3, target3(), around(3, 8, v, chunks))
        w = load(rhs2, 2)
        v = [[w[a][g] + v[a][g] for g in range(8)] for a in range(2)]
        v = relax(2, target2(), around(2, 9, v, chunks))
        v = relax(2, target2(), around(2, 10, v, chunks))
        for a in range(2):
            for g in range(8):
                back_b[g, a] = v[a][g]

    nacc[...] = jnp.zeros((CYCLES, 8, 128), F32)

    for both in early:
        both.wait()

    @pl.loop(0, CYCLES)
    def _(cycle):
        @pl.when(cycle == 0)
        def _():
            @pl.loop(0, 8)
            def _(p):
                for half in range(2):
                    for row in range(0, 256, 64):
                        fresh = j0[p, half, pl.ds(row, 64), :] * g0[p, half, pl.ds(row, 64), :]
                        v_c[p + 1, half, pl.ds(PAD + row, 64), :] = fresh

            sweep0(v_c, v_b, 1)
            late.wait()

        @pl.when(cycle > 0)
        def _():
            sweep0(v_a, v_d, 0)
            exchange0(v_d, 0)
            sweep0(v_d, v_b, 0)
            exchange0(v_b, 1)

        residual0(v_b, True, 0)
        shrink0(r0, g1, 4)
        both = pair(3, (g1.at[6:8], g1.at[2:4]), (g1.at[4:6], g1.at[8:10]))
        both.start()
        both.wait()

        @pl.loop(0, 8)
        def _(p):
            w_a[p + 3, pl.ds(PAD, 128), :] = j1[p + 2] * g1[p + 2]

        sweep1(w_a, store_second, 1)
        residual1()

        chunks = []

        def chunk(up, down, steps=1):
            i = len(chunks)
            chunks.append(Pair(up, down, c_send.at[i], c_recv.at[i], steps))

        for i in range(2):
            chunk((g1.at[4 + i], g1.at[i]), (g1.at[6 + i], g1.at[10 + i]))
        rows = pl.ds(PAD, 128)
        chunk((w_b.at[8, rows], w_b.at[0, rows]), (w_b.at[5, rows], w_b.at[13, rows]), 2)
        for i in range(3):
            chunk(
                (w_b.at[5 + i, rows], w_b.at[1 + i, rows]),
                (w_b.at[6 + i, rows], w_b.at[10 + i, rows]),
            )
        for i in range(2):
            for half in range(2):
                for row in range(0, 256, 128):
                    rows = pl.ds(PAD + row, 128)
                    chunk(
                        (v_b.at[4 + i, half, rows], v_b.at[i, half, rows]),
                        (v_b.at[4 + i, half, rows], v_b.at[8 + i, half, rows]),
                    )

        send_a[...] = shrink1(r1).reshape(16, 8, 128)
        finish = all_wide(send_a, place_wide, recv_a, ia, a_send, a_recv)
        chunks[0].start()
        chunks[1].start()
        finish()
        turned = recv_a[...].reshape(128, 128).T
        for a in range(2):
            send_b[:, a] = turned[64 * a : 64 * a + 64].reshape(8, 8, 128)
        all_narrow(send_b, place_narrow, recv_b, ib, b_send, b_recv)()
        lines(chunks)
        all_narrow(back_b, lambda g: g, got_b, narrow, bb_send, bb_recv)()
        turned = jnp.concatenate([got_b[:, a].reshape(64, 128) for a in range(2)], axis=0).T
        back_a[...] = turned.reshape(16, 8, 128)
        finish = all_wide(back_a, lambda g: g, got_a.at[1], wide, ba_send, ba_recv)
        chunks[13].start()
        finish()

        lhs[0] = got_a[1].reshape(128, 128)
        ends[0] = lhs[0, pl.ds(3, 32, 4), :]
        ends[1] = lhs[0, pl.ds(0, 32, 4), :]
        whole = pair(10, (got_a.at[1], got_a.at[0]), (got_a.at[1], got_a.at[2]))
        outer = pair(11, (ends.at[0], beyond.at[0]), (ends.at[1], beyond.at[1]), 2)
        whole.start()
        outer.start()
        for each in chunks:
            each.wait()
        whole.wait()
        outer.wait()
        for side in range(3):
            for a in range(2):
                grown[a] = dot(got_a[side].reshape(128, 128), spread[a])
            for a in range(2):
                for b in range(2):
                    for p in range(4):
                        piece = grown[a, pl.ds(b * 4 + p, 16, 8), :]
                        for i in range(2):
                            rows = pl.ds(PAD + 4 * a + 2 * b + i, 16, 8)
                            q = 4 * side + p + 1
                            w_a[q, rows, :] = w_b[q, rows, :] + piece
        for side in range(2):
            for a in range(2):
                grown[a, 0:32, :] = dot(beyond[side], spread[a])
                for b in range(2):
                    piece = grown[a, pl.ds(b, 16, 2), :]
                    for i in range(2):
                        rows = pl.ds(PAD + 4 * a + 2 * b + i, 16, 8)
                        w_a[13 * side, rows, :] = w_b[13 * side, rows, :] + piece
        sweep1(w_a, store_second, 4)
        sweep1(w_b, store_error, 3)

        @pl.loop(0, 10)
        def _(p):
            for half in range(2):
                piece = dot(e1[p], spread[half])
                for i in range(2):
                    rows = pl.ds(PAD + i, 128, 2)
                    v_c[p, half, rows, :] = v_b[p, half, rows, :] + piece

        sweep0(v_c, v_b, 2)
        sweep0(v_b, v_a, 1)
        residual0(v_a, False, cycle)

    stores = []
    for p in range(4):
        for half in range(2):
            stores.append(
                pltpu.make_async_copy(
                    v_a.at[p + 3, half, pl.ds(PAD, 256)],
                    out.at[p, :, pl.ds(half * 128, 128)],
                    in_sem.at[0, p, half],
                )
            )
    for copy in stores:
        copy.start()

    all_narrow_sum(nacc, nb, ia, ib, n_send, n_recv)
    total = nb[0]
    for g in range(1, GROUP_Y):
        total = total + nb[g]
    nacc[...] = total
    all_wide_sum(nacc, nz, ia, ib, n_send, n_recv)
    total = nz[0]
    for g in range(1, GROUP_Z):
        total = total + nz[g]
    for c in range(CYCLES):
        norms[c] = jnp.sum(total[c]) * (1.0 / (512 * 256 * 256))
    for copy in stores:
        copy.wait()


def all_narrow_sum(src, dst, ia, ib, send_sem, recv_sem):
    copies = []
    for k in range(1, GROUP_Y):
        peer = lax.rem(ib + k, GROUP_Y)
        copies.append(
            pltpu.make_async_remote_copy(
                src_ref=src, dst_ref=dst.at[ib], send_sem=send_sem.at[0, k],
                recv_sem=recv_sem.at[0, k], device_id=device_of(ia, peer), device_id_type=MESH,
            )
        )
    for copy in copies:
        copy.start()
    dst[ib] = src[...]
    for copy in copies:
        copy.wait()


def all_wide_sum(src, dst, ia, ib, send_sem, recv_sem):
    copies = []
    for k in range(1, GROUP_Z):
        peer = lax.rem(ia + k, GROUP_Z)
        copies.append(
            pltpu.make_async_remote_copy(
                src_ref=src, dst_ref=dst.at[ia], send_sem=send_sem.at[1, k],
                recv_sem=recv_sem.at[1, k], device_id=device_of(peer, ib), device_id_type=MESH,
            )
        )
    for copy in copies:
        copy.start()
    dst[ia] = src[...]
    for copy in copies:
        copy.wait()


def vmem(*shape):
    return pltpu.VMEM(shape, F32)


def shards(source, vertical, reaction):
    dma = pltpu.SemaphoreType.DMA
    solved, norms = pl.pallas_call(
        kernel,
        out_shape=(
            jax.ShapeDtypeStruct((4, 256, 256), F32),
            jax.ShapeDtypeStruct((CYCLES,), F32),
        ),
        in_specs=[
            pl.BlockSpec(memory_space=pl.ANY),
            pl.BlockSpec(memory_space=pltpu.SMEM),
            pl.BlockSpec(memory_space=pl.ANY),
        ],
        out_specs=(pl.BlockSpec(memory_space=pl.ANY), pl.BlockSpec(memory_space=pltpu.SMEM)),
        scratch_shapes=[
            vmem(10, 2, 256 + 2 * PAD, 128),
            vmem(10, 2, 256 + 2 * PAD, 128),
            vmem(10, 2, 256 + 2 * PAD, 128),
            vmem(10, 2, 256 + 2 * PAD, 128),
            vmem(8, 2, 256, 128),
            vmem(4, 2, 256, 128),
            vmem(8, 2, 256, 128),
            vmem(4, 2, 256, 128),
            vmem(12, 8, 128),
            vmem(14, 128 + 2 * PAD, 128),
            vmem(14, 128 + 2 * PAD, 128),
            vmem(12, 128, 128),
            vmem(4, 128, 128),
            vmem(12, 128, 128),
            vmem(4, 128, 128),
            vmem(10, 128, 128),
            pltpu.VMEM((2, 128, 128), jnp.bfloat16),
            pltpu.VMEM((2, 128, 128), jnp.bfloat16),
            vmem(2, 128, 128),
            vmem(16, 16, 128),
            vmem(16, 16, 128),
            vmem(8, 4, 8, 128),
            vmem(8, 4, 8, 128),
            vmem(16, 8, 128),
            vmem(16, 8, 128),
            vmem(8, 2, 8, 128),
            vmem(8, 2, 8, 128),
            vmem(8, 2, 8, 128),
            vmem(8, 2, 8, 128),
            vmem(16, 8, 128),
            vmem(3, 16, 8, 128),
            vmem(2, 32, 128),
            vmem(2, 32, 128),
            vmem(2, 128, 128),
            vmem(5, 64, 128),
            vmem(2, 64, 128),
            vmem(5, 2 * STEPS + 1, 64, 128),
            vmem(EVENTS, 128, 128),
            vmem(EVENTS, 2, 32, 128),
            vmem(EVENTS, 2, 32, 128),
            vmem(EVENTS, 2, 16, 128),
            vmem(EVENTS, 2, 16, 128),
            vmem(2, 64, 128),
            vmem(2, 64, 128),
            vmem(2, 64, 128),
            vmem(CYCLES, 8, 128),
            vmem(GROUP_Y, CYCLES, 8, 128),
            vmem(GROUP_Z, CYCLES, 8, 128),
            dma((2, 4, 2)),
            dma((12, 2)),
            dma((12, 2)),
            dma((14, 2)),
            dma((14, 2)),
            dma((GROUP_Z,)),
            dma((GROUP_Z,)),
            dma((GROUP_Y,)),
            dma((GROUP_Y,)),
            dma((GROUP_Z,)),
            dma((GROUP_Z,)),
            dma((GROUP_Y,)),
            dma((GROUP_Y,)),
            dma((GROUP_Y,)),
            dma((GROUP_Y,)),
            dma((GROUP_Z,)),
            dma((GROUP_Z,)),
            dma((EVENTS, 4)),
            dma((EVENTS, 4)),
            dma((2, GROUP_Z)),
            dma((2, GROUP_Z)),
        ],
        compiler_params=pltpu.CompilerParams(
            collective_id=0, has_side_effects=True, vmem_limit_bytes=48 * 1024 * 1024
        ),
    )(source, vertical, reaction)
    return solved, norms


def solution(mesh):
    planes = P(("gz", "gy"), None, None)
    return jax.shard_map(
        shards,
        mesh=mesh,
        in_specs=(planes, P(("gz", "gy")), planes),
        out_specs=(planes, P()),
        check_vma=False,
    )
```

```python
import functools

import jax
import jax.numpy as jnp
from jax import lax
from jax.experimental import pallas as pl
from jax.experimental.pallas import tpu as pltpu
from jax.sharding import PartitionSpec as P

F32 = jnp.float32
MESH = pl.DeviceIdType.MESH
CYCLES = 2
STEPS = 9
EVENTS = 11
OMEGA = 0.8
H = (1.0, 0.25, 1.0 / 16, 1.0 / 64, 1.0 / 256)
GROUP_Z = 16
GROUP_Y = 8
DEVICES = 128
PAD = 8


def device_of(a, b):
    wide = lax.div(a, 8) * 8 + lax.rem(lax.div(a, 2), 4) * 2 + lax.div(b, 4)
    return (wide, lax.rem(a, 2) * 4 + lax.rem(b, 4))


def place_wide(a):
    z, x = lax.div(a, 8) * 2 + lax.rem(a, 2), lax.rem(lax.div(a, 2), 4)
    return z * 4 + x + lax.rem(z, 2) * (3 - 2 * x)


def member_wide(place):
    z, x = lax.div(place, 4), lax.rem(place, 4)
    x = x + lax.rem(z, 2) * (3 - 2 * x)
    return (lax.div(z, 2) * 4 + x) * 2 + lax.rem(z, 2)


def place_narrow(b):
    core, y = lax.div(b, 4), lax.rem(b, 4)
    return y * 2 + core + lax.rem(y, 2) * (1 - 2 * core)


def member_narrow(place):
    y, core = lax.div(place, 2), lax.rem(place, 2)
    core = core + lax.rem(y, 2) * (1 - 2 * core)
    return core * 4 + y


def dot(a, b):
    total = None
    for part in range(3):
        piece = a.astype(jnp.bfloat16)
        product = jnp.dot(piece, b, preferred_element_type=F32)
        total = product if total is None else total + product
        if part < 2:
            a = a - piece.astype(F32)
    return total


def roll_lanes(v, s):
    return pltpu.roll(v, s % 128, 1)


def roll_rows(v, s):
    return pltpu.roll(v, s % 8, 0)


def lane_iota():
    return lax.broadcasted_iota(jnp.int32, (8, 128), 1)


def row_iota():
    return lax.broadcasted_iota(jnp.int32, (8, 128), 0)


def below(v, s):
    if s < 4:
        return [v[p - s] if p >= s else roll_lanes(v[p - s + 4], 1) for p in range(4)]
    return [roll_lanes(v[p], s // 4) for p in range(4)]


def above(v, s):
    if s < 4:
        return [v[p + s] if p + s < 4 else roll_lanes(v[p + s - 4], -1) for p in range(4)]
    return [roll_lanes(v[p], -(s // 4)) for p in range(4)]


def exchange_parts(v):
    row, lane = row_iota(), lane_iota()
    for m in (1, 2, 4):
        down = lax.rem(lax.div(row, m), 2)
        across = lax.rem(lax.div(lane, 16 * m), 2)
        moved = jnp.where(
            down == 1,
            roll_rows(roll_lanes(v, -16 * m), m),
            roll_rows(roll_lanes(v, 16 * m), -m),
        )
        v = jnp.where(down == across, v, moved)
    return v


def tile_of(x):
    z, q = divmod(x, 4)
    return ((z // 2) * 4 + (3 - q if z % 2 else q)) * 2 + z % 2


def kernel(
    source, vertical, reaction, out, norms,
    v_a, v_b, v_c, v_d, g0, d0, j0, r0, vt, w_a, w_b, g1, d1, j1, r1, e1, compact, spread, lhs,
    fold, unfold, send_s, recv_s, send_r, recv_r, turn, back_r, got_r, got_a, beyond, ends, grown,
    dl, vl, cf, val, hx, hy, ys, rhs2, rhs3, res,
    nacc, part, nz,
    in_sem, z_send, z_recv, c_send, c_recv,
    all_send, all_recv, h_send, h_recv,
):
    gz, gy = lax.axis_index("gz"), lax.axis_index("gy")
    me = gz * GROUP_Y + gy
    core = lax.rem(gz, 2)
    ia = (lax.div(gz, 8) * 4 + lax.div(lax.rem(gz, 8), 2)) * 2 + lax.div(gy, 4)
    ib = core * 4 + lax.rem(gy, 4)
    wide, narrow = place_wide(ia), place_narrow(ib)

    def device(d):
        d = lax.rem(d + DEVICES, DEVICES)
        return (lax.div(d, GROUP_Y), lax.rem(d, GROUP_Y))

    loads = []
    for p in range(4):
        for half in range(2):
            lanes = pl.ds(half * 128, 128)
            loads.append(pltpu.make_async_copy(source.at[p, :, lanes], g0.at[p + 2, half], in_sem.at[0, p, half]))
            loads.append(pltpu.make_async_copy(reaction.at[p, :, lanes], r0.at[p, half], in_sem.at[1, p, half]))
    for copy in loads:
        copy.start()

    barrier = pltpu.get_barrier_semaphore()

    members = [lax.rem(ib + j, GROUP_Y) for j in range(GROUP_Y)]
    members = [(b, lax.div(b, 4), lax.rem(b, 4)) for b in members]

    def everyone(act):
        def some(k, start):
            a = lax.rem(ia + k, GROUP_Z)
            wide_a, narrow_a = lax.div(a, 2) * 2, lax.rem(a, 2) * 4
            for b, core_b, y_b in members[start:]:
                to = (wide_a + core_b, narrow_a + y_b)
                act(a * GROUP_Y + b, to[0] * GROUP_Y + to[1], to)

        some(0, 1)
        pl.loop(1, GROUP_Z)(lambda k: some(k, 0))

    everyone(
        lambda block, plane, to: pl.semaphore_signal(
            barrier, inc=1, device_id=to, device_id_type=MESH
        )
    )

    for p in range(4):
        vt[p + 4] = jnp.full((8, 128), vertical[p], F32)

    @pl.loop(0, 10)
    def _(i):
        for ref in (v_a, v_b, v_c, v_d):
            for half in range(2):
                for row in (0, PAD + 256):
                    ref[i, half, pl.ds(row, PAD), :] = jnp.zeros((PAD, 128), F32)

    @pl.loop(0, 14)
    def _(i):
        for ref in (w_a, w_b):
            for row in (0, PAD + 128):
                ref[i, pl.ds(row, PAD), :] = jnp.zeros((PAD, 128), F32)

    def clear(side):
        @pl.loop(7 * side, 7 * side + 3)
        def _(i):
            for ref in (v_a, v_b, v_c, v_d):
                for half in range(2):
                    ref[i, half] = jnp.zeros((256 + 2 * PAD, 128), F32)

        @pl.loop(9 * side, 9 * side + 5)
        def _(i):
            for ref in (w_a, w_b):
                ref[i] = jnp.zeros((128 + 2 * PAD, 128), F32)

        for i in range(6 * side, 6 * side + 2):
            for half in range(2):
                g0[i, half] = jnp.zeros((256, 128), F32)
                j0[i, half] = jnp.zeros((256, 128), F32)
        for i in range(8 * side, 8 * side + 4):
            vt[i] = jnp.zeros((8, 128), F32)
            g1[i] = jnp.zeros((128, 128), F32)
            j1[i] = jnp.zeros((128, 128), F32)
        got_a[2 * side] = jnp.zeros((128, 128), F32)
        beyond[side] = jnp.zeros((32, 128), F32)

    for side in range(2):

        @pl.when(me == (DEVICES - 1) * side)
        def _(side=side):
            clear(side)

        @pl.when(me == 1 + (DEVICES - 3) * side)
        def _(side=side):
            for ref in (w_a, w_b):
                ref[13 * side] = jnp.zeros((128 + 2 * PAD, 128), F32)
            beyond[side] = jnp.zeros((32, 128), F32)

    @pl.when(wide == 0)
    def _():
        for e in range(EVENTS):
            hx[e, 0] = jnp.zeros((32, 128), F32)

    @pl.when(wide == GROUP_Z - 1)
    def _():
        for e in range(EVENTS):
            hx[e, 1] = jnp.zeros((32, 128), F32)

    @pl.when(narrow == 0)
    def _():
        for e in range(EVENTS):
            hy[e, 0] = jnp.zeros((16, 128), F32)

    @pl.when(narrow == GROUP_Y - 1)
    def _():
        for e in range(EVENTS):
            hy[e, 1] = jnp.zeros((16, 128), F32)

    from_lane = lax.broadcasted_iota(jnp.int32, (128, 128), 0)
    to_lane = lax.broadcasted_iota(jnp.int32, (128, 128), 1)
    for half in range(2):
        compact[half] = jnp.where(to_lane == 64 * half + from_lane // 2, 0.25, 0.0).astype(jnp.bfloat16)
        part_of = place_narrow(to_lane // 16) * 8 + to_lane % 8
        hit = jnp.logical_and(part_of == from_lane // 2, to_lane // 8 % 2 == half)
        fold[half] = jnp.where(hit, 0.25, 0.0).astype(jnp.bfloat16)
        part_of = place_narrow(from_lane // 16) * 8 + from_lane % 8
        hit = jnp.logical_and(part_of == to_lane // 2, from_lane // 8 % 2 == half)
        unfold[half] = jnp.where(hit, 1.0, 0.0).astype(jnp.bfloat16)
        spread[half] = jnp.where(from_lane == 64 * half + to_lane // 2, 1.0, 0.0).astype(jnp.bfloat16)

    pl.semaphore_wait(barrier, DEVICES - 1)

    has_up, has_down = me < DEVICES - 1, me > 0

    class Pair:
        def __init__(self, up, down, send_sem, recv_sem, steps=1):
            self.steps = steps
            self.copies = [
                pltpu.make_async_remote_copy(
                    src_ref=src, dst_ref=dst, send_sem=send_sem.at[i], recv_sem=recv_sem.at[i],
                    device_id=device(me + shift), device_id_type=MESH,
                )
                for i, (src, dst), shift in ((0, up, steps), (1, down, -steps))
            ]

        def start(self):
            pl.when(me < DEVICES - self.steps)(self.copies[0].start)
            pl.when(me >= self.steps)(self.copies[1].start)

        def wait(self):
            @pl.when(me < DEVICES - self.steps)
            def _():
                self.copies[0].wait_send()
                self.copies[1].wait_recv()

            @pl.when(me >= self.steps)
            def _():
                self.copies[1].wait_send()
                self.copies[0].wait_recv()

    def pair(i, up, down, steps=1):
        return Pair(up, down, z_send.at[i], z_recv.at[i], steps)

    def exchange0(slot, i):
        rows = pl.ds(PAD, 256)
        both = pair(
            i,
            (slot.at[6, :, rows], slot.at[2, :, rows]),
            (slot.at[3, :, rows], slot.at[7, :, rows]),
        )
        both.start()
        return both.wait

    mine = ia * GROUP_Y + ib

    def all_rows(i, src, to_blocks, dst):
        place = me if to_blocks else mine

        def send(block, plane, to):
            pltpu.make_async_remote_copy(
                src_ref=src.at[:, pl.ds(block if to_blocks else plane, 1)],
                dst_ref=dst.at[:, pl.ds(place, 1)],
                send_sem=all_send.at[i], recv_sem=all_recv.at[i], device_id=to,
                device_id_type=MESH,
            ).start()

        everyone(send)
        dst[:, pl.ds(place, 1), :] = src[:, pl.ds(mine if to_blocks else me, 1), :]

        def finish():
            others = pl.ds(0, DEVICES - 1)
            for sem in (all_recv, all_send):
                pltpu.make_async_copy(src.at[:, others], dst.at[:, others], sem.at[i]).wait()

        return finish

    BLOCK = 32
    lanes0 = lax.broadcasted_iota(jnp.int32, (BLOCK, 128), 1)

    def around0(slot, p, row):
        rows = pl.ds(PAD + row, BLOCK)
        centre = [slot[p + 3, half, rows, :] for half in range(2)]
        left = [pltpu.roll(c, 1, 1) for c in centre]
        right = [pltpu.roll(c, 127, 1) for c in centre]
        sums = [
            jnp.where(lanes0 == 0, 0.0, left[0]) + jnp.where(lanes0 == 127, right[1], right[0]),
            jnp.where(lanes0 == 0, left[0], left[1]) + jnp.where(lanes0 == 127, 0.0, right[1]),
        ]
        coupled = jnp.broadcast_to(vt[p + 4, 0:1, :], (BLOCK, 128))
        total = []
        for half in range(2):
            beside = slot[p + 3, half, pl.ds(PAD + row - 1, BLOCK), :]
            beside = beside + slot[p + 3, half, pl.ds(PAD + row + 1, BLOCK), :]
            along = slot[p + 2, half, rows, :] + slot[p + 4, half, rows, :]
            total.append(H[0] * (sums[half] + beside) + coupled * along)
        return centre, total

    def sweep0(old, new, first, count, step=1):
        @pl.loop(0, count)
        def _(i):
            p = first + i * step
            for row in range(0, 256, BLOCK):
                centre, total = around0(old, p, row)
                rows = pl.ds(row, BLOCK)
                for half in range(2):
                    fresh = g0[p + 2, half, rows, :] + total[half]
                    fresh = (1.0 - OMEGA) * centre[half] + j0[p + 2, half, rows, :] * fresh
                    new[p + 3, half, pl.ds(PAD + row, BLOCK), :] = fresh

    def residual0(slot, keep, sums, first, count, step=1):
        @pl.loop(0, count)
        def _(i):
            p = first + i * step
            for row in range(0, 256, BLOCK):
                centre, total = around0(slot, p, row)
                rows = pl.ds(row, BLOCK)
                for half in range(2):
                    left = g0[p + 2, half, rows, :] + total[half] - d0[p, half, rows, :] * centre[half]
                    if keep:
                        r0[p, half, rows, :] = left
                    else:
                        nacc[sums] += (left * left).reshape(BLOCK // 8, 8, 128).sum(axis=0)

    lanes1 = lax.broadcasted_iota(jnp.int32, (BLOCK, 128), 1)

    def around1(slot, p, row):
        rows = pl.ds(PAD + row, BLOCK)
        centre = slot[p + 5, rows, :]
        sums = jnp.where(lanes1 == 0, 0.0, pltpu.roll(centre, 1, 1))
        sums = sums + jnp.where(lanes1 == 127, 0.0, pltpu.roll(centre, 127, 1))
        sums = sums + slot[p + 5, pl.ds(PAD + row - 1, BLOCK), :]
        sums = sums + slot[p + 5, pl.ds(PAD + row + 1, BLOCK), :]
        along = slot[p + 4, rows, :] + slot[p + 6, rows, :]
        return centre, H[1] * sums + jnp.broadcast_to(vt[p + 4, 0:1, :], (BLOCK, 128)) * along

    def sweep1(old, store, reach):
        @pl.loop(0, 4 + 2 * reach)
        def _(i):
            p = i - reach
            for row in range(0, 128, BLOCK):
                centre, total = around1(old, p, row)
                rows = pl.ds(row, BLOCK)
                fresh = j1[p + 4, rows, :] * (g1[p + 4, rows, :] + total)
                store(p, row, (1.0 - OMEGA) * centre + fresh)

    def store_second(p, row, fresh):
        w_b[p + 5, pl.ds(PAD + row, BLOCK), :] = fresh

    def store_error(p, row, fresh):
        e1[p + 3, pl.ds(row, BLOCK), :] = fresh

    def residual1():
        @pl.loop(0, 4)
        def _(p):
            for row in range(0, 128, BLOCK):
                centre, total = around1(w_b, p, row)
                rows = pl.ds(row, BLOCK)
                r1[p, rows, :] = g1[p + 4, rows, :] + total - d1[p, rows, :] * centre

    def shrink0(src, dst, first):
        @pl.loop(0, 4)
        def _(p):
            total = jnp.zeros((128, 128), F32)
            for half in range(2):
                pairs = src[p, half, pl.ds(0, 128, 2), :] + src[p, half, pl.ds(1, 128, 2), :]
                total = total + dot(pairs, compact[half])
            dst[p + first] = total

    def shrink1(src):
        total = jnp.zeros((128, 128), F32)
        for a in range(2):
            for b in range(2):
                for p in range(4):
                    first = 4 * a + 2 * b
                    pairs = src[p, pl.ds(first, 16, 8), :] + src[p, pl.ds(first + 1, 16, 8), :]
                    lhs[a, pl.ds(b * 4 + p, 16, 8), :] = pairs
            total = total + dot(lhs[a], fold[a])
        return total

    early = []
    for i in range(2):
        for half in range(2):
            lanes = pl.ds(half * 128, 128)
            early.append(
                pair(
                    4 + 2 * i + half,
                    (source.at[2 + i, :, lanes], g0.at[i, half]),
                    (source.at[i, :, lanes], g0.at[6 + i, half]),
                )
            )
    early.append(pair(2, (vt.at[4:8], vt.at[0:4]), (vt.at[4:8], vt.at[8:12])))
    for both in early:
        both.start()
    for copy in loads:
        copy.wait()
    shrink0(r0, r1, 0)

    @pl.loop(0, 4)
    def _(p):
        coupled = 2.0 * vertical[p]
        for half in range(2):
            for row in range(0, 256, 64):
                rows = pl.ds(row, 64)
                diagonal = coupled + 4.0 * H[0] + r0[p, half, rows, :]
                d0[p, half, rows, :] = diagonal
                j0[p + 2, half, rows, :] = OMEGA / diagonal
        diagonal = coupled + 4.0 * H[1] + r1[p]
        d1[p] = diagonal
        j1[p + 4] = OMEGA / diagonal

    def send_blocks(f, v, dst):
        for x in range(16):
            dst[f, 8 * tile_of(x) : 8 * tile_of(x) + 8, :] = exchange_parts(v[8 * x : 8 * x + 8])

    send_blocks(0, shrink1(r1), send_s)
    plane = lane_iota() // 16 % 4
    coupling = jnp.zeros((8, 128), F32)
    for p in range(4):
        coupling = jnp.where(plane == p, vertical[p], coupling)
    for x in range(16):
        send_s[1, 8 * x : 8 * x + 8, :] = coupling
    finish = all_rows(0, send_s, True, recv_s)
    early.append(pair(8, (j0.at[4:6], j0.at[0:2]), (j0.at[2:4], j0.at[6:8])))
    late = pair(9, (j1.at[6:8], j1.at[2:4]), (j1.at[4:6], j1.at[8:10]))
    later = pair(12, (j1.at[4:6], j1.at[0:2]), (j1.at[6:8], j1.at[10:12]))
    early[-1].start()
    late.start()
    finish()

    lane, row = lane_iota(), row_iota()

    def tile(p):
        return pl.ds(8 * p, 8)

    def unpack(v):
        return [
            [v[8 * (8 * b + 2 * p + a) : 8 * (8 * b + 2 * p + a) + 8] for p in range(4)]
            for a in range(2)
            for b in range(2)
        ]

    def shrink2(v):
        result = []
        for a in range(2):
            mine = []
            for p in range(4):
                t = v[2 * a][p] + v[2 * a + 1][p]
                t = t + jnp.where(row % 2 == 1, roll_rows(t, 1), roll_rows(t, -1))
                mine.append(0.25 * t)
            result.append(mine)
        return result

    def shrink3(v):
        mine = []
        for p in range(4):
            t = v[0][p] + v[1][p]
            t = t + jnp.where(row % 4 >= 2, roll_rows(t, 2), roll_rows(t, -2))
            mine.append(0.25 * t)
        return [mine]

    couplings = unpack(recv_s[1].T)[0]
    for p in range(4):
        vl[0, tile(p), :] = jnp.where(lane == 0, 0.0, couplings[p]) if p == 0 else couplings[p]
        vl[1, tile(p), :] = jnp.where(lane == 127, 0.0, couplings[p]) if p == 3 else couplings[p]
    react2 = unpack(recv_s[0].T)
    react3 = shrink2(react2)
    react4 = shrink3(react3)
    order = [(2, each) for each in react2] + [(3, each) for each in react3] + [(4, react4[0])]
    for i, (level, lines) in enumerate(order):
        for p in range(4):
            dl[i, tile(p), :] = 2.0 * couplings[p] + 4.0 * H[level] + lines[p]

    @pl.loop(0, 7)
    def _(i):
        low = [-vl[0, tile(g), :] for g in range(4)]
        high = [-vl[1, tile(g), :] for g in range(4)]
        middle = [dl[i, tile(g), :] for g in range(4)]
        for k in range(STEPS):
            s = 1 << k
            middle_below, middle_above = below(middle, s), above(middle, s)
            left = [-low[g] / middle_below[g] for g in range(4)]
            right = [-high[g] / middle_above[g] for g in range(4)]
            for g in range(4):
                cf[i, 2 * k, tile(g), :] = left[g]
                cf[i, 2 * k + 1, tile(g), :] = right[g]
            high_below, low_above = below(high, s), above(low, s)
            middle = [middle[g] + left[g] * high_below[g] + right[g] * low_above[g] for g in range(4)]
            if k < STEPS - 1:
                low_below, high_above = below(low, s), above(high, s)
                low = [left[g] * low_below[g] for g in range(4)]
                high = [right[g] * high_above[g] for g in range(4)]
        for g in range(4):
            cf[i, 2 * STEPS, tile(g), :] = 1.0 / middle[g]

    first_of = {2: 0, 3: 4, 4: 6}
    count_of = {2: 4, 3: 2, 4: 1}

    def solve(level, right):
        solved = []
        for a in range(count_of[level]):
            i = first_of[level] + a
            r = right[a]
            for k in range(STEPS):
                s = 1 << k
                down, up = below(r, s), above(r, s)
                r = [
                    r[g] + cf[i, 2 * k, tile(g), :] * down[g] + cf[i, 2 * k + 1, tile(g), :] * up[g]
                    for g in range(4)
                ]
            solved.append([r[g] * cf[i, 2 * STEPS, tile(g), :] for g in range(4)])
        return solved

    def around(level, event, v, chunks):
        count = count_of[level]
        for x in range(count):
            for p in range(4):
                val[event, pl.ds((x * 4 + p) * 8, 8), :] = v[x][p]
        size = 4 * count
        ys[event, 0, 0:size, :] = val[event, pl.ds(0, size, 8), :]
        ys[event, 1, 0:size, :] = val[event, pl.ds(7, size, 8), :]
        span = pl.ds(0, size)
        copies = []
        for side, src, dst, there in (
            (0, val.at[event, pl.ds(32 * (count - 1), 32)], hx.at[event, 0], device_of(member_wide(wide + 1), ib)),
            (1, val.at[event, pl.ds(0, 32)], hx.at[event, 1], device_of(member_wide(wide - 1), ib)),
            (2, ys.at[event, 1, span], hy.at[event, 0, span], device_of(ia, member_narrow(narrow + 1))),
            (3, ys.at[event, 0, span], hy.at[event, 1, span], device_of(ia, member_narrow(narrow - 1))),
        ):
            copies.append(
                pltpu.make_async_remote_copy(
                    src_ref=src, dst_ref=dst, send_sem=h_send.at[event, side],
                    recv_sem=h_recv.at[event, side], device_id=there, device_id_type=MESH,
                )
            )
        has = (wide < GROUP_Z - 1, wide > 0, narrow < GROUP_Y - 1, narrow > 0)
        for side in range(4):
            pl.when(has[side])(copies[side].start)
        chunks[event + 2].start()
        for side in range(4):
            pl.when(has[side])(copies[side].wait_send)
            pl.when(has[side])(copies[side ^ 1].wait_recv)
        shift = 1 << (level - 2)
        result = []
        for x in range(count):
            mine = []
            for p in range(4):
                total = v[x - 1][p] if x else hx[event, 0, tile(p), :]
                total = total + (v[x + 1][p] if x + 1 < count else hx[event, 1, tile(p), :])
                low = jnp.broadcast_to(hy[event, 0, pl.ds(x * 4 + p, 1), :], (8, 128))
                high = jnp.broadcast_to(hy[event, 1, pl.ds(x * 4 + p, 1), :], (8, 128))
                total = total + jnp.where(row < shift, low, roll_rows(v[x][p], shift))
                total = total + jnp.where(row >= 8 - shift, high, roll_rows(v[x][p], -shift))
                mine.append(total)
            result.append(mine)
        return result

    def relax(level, target, total):
        return solve(
            level,
            [
                [target[a][g] + H[level] * total[a][g] for g in range(4)]
                for a in range(count_of[level])
            ],
        )

    def residual(level, target, v, total):
        result = []
        for a in range(count_of[level]):
            down, up = below(v[a], 1), above(v[a], 1)
            result.append([
                target[a][g] + H[level] * total[a][g] - dl[first_of[level] + a, tile(g), :] * v[a][g]
                + vl[0, tile(g), :] * down[g] + vl[1, tile(g), :] * up[g]
                for g in range(4)
            ])
        return result

    def load(ref, count):
        return [[ref[a, tile(g), :] for g in range(4)] for a in range(count)]

    def keep(ref, v):
        for a in range(len(v)):
            for g in range(4):
                ref[a, tile(g), :] = v[a][g]

    def lines(chunks):
        target2 = lambda: unpack(turn)
        v = solve(2, target2())
        v = relax(2, target2(), around(2, 0, v, chunks))
        r = residual(2, target2(), v, around(2, 1, v, chunks))
        keep(rhs2, v)
        keep(rhs3, shrink2(r))
        target3 = lambda: load(rhs3, 2)
        v = solve(3, target3())
        v = relax(3, target3(), around(3, 2, v, chunks))
        r = residual(3, target3(), v, around(3, 3, v, chunks))
        keep(res, v)
        target4 = shrink3(r)
        v = solve(4, target4)
        for e in range(3):
            v = relax(4, target4, around(4, 4 + e, v, chunks))
        w = load(res, 2)
        v = [[w[a][g] + v[0][g] for g in range(4)] for a in range(2)]
        v = relax(3, target3(), around(3, 7, v, chunks))
        v = relax(3, target3(), around(3, 8, v, chunks))
        w = load(rhs2, 4)
        v = [[w[x][p] + v[x // 2][p] for p in range(4)] for x in range(4)]
        v = relax(2, target2(), around(2, 9, v, chunks))
        v = relax(2, target2(), around(2, 10, v, chunks))
        for a in range(2):
            for b in range(2):
                for p in range(4):
                    turn[pl.ds(8 * (8 * b + 2 * p + a), 8), :] = v[2 * a + b][p]

    nacc[...] = jnp.zeros((CYCLES, 8, 128), F32)

    for both in early:
        both.wait()

    @pl.loop(0, CYCLES)
    def _(cycle):
        @pl.when(cycle == 0)
        def _():
            @pl.loop(0, 8)
            def _(p):
                for half in range(2):
                    for row in range(0, 256, 64):
                        fresh = j0[p, half, pl.ds(row, 64), :] * g0[p, half, pl.ds(row, 64), :]
                        v_c[p + 1, half, pl.ds(PAD + row, 64), :] = fresh

            sweep0(v_c, v_b, -1, 6)
            residual0(v_b, True, 0, 1, 2)
            late.wait()

        @pl.when(cycle > 0)
        def _():
            sweep0(v_a, v_d, 0, 2, 3)
            finish = exchange0(v_d, 0)
            sweep0(v_a, v_d, 1, 2)
            sweep0(v_d, v_b, 1, 2)
            finish()
            sweep0(v_d, v_b, 0, 2, 3)
            finish = exchange0(v_b, 1)
            residual0(v_b, True, 0, 1, 2)
            finish()

        residual0(v_b, True, 0, 0, 2, 3)
        shrink0(r0, g1, 4)
        both = pair(3, (g1.at[6:8], g1.at[2:4]), (g1.at[4:6], g1.at[8:10]))
        both.start()
        both.wait()

        @pl.loop(0, 8)
        def _(p):
            w_a[p + 3, pl.ds(PAD, 128), :] = j1[p + 2] * g1[p + 2]

        sweep1(w_a, store_second, 1)
        residual1()

        chunks = []

        def chunk(up, down, steps=1):
            i = len(chunks)
            chunks.append(Pair(up, down, c_send.at[i], c_recv.at[i], steps))

        for i in range(2):
            chunk((g1.at[4 + i], g1.at[i]), (g1.at[6 + i], g1.at[10 + i]))
        rows = pl.ds(PAD, 128)
        chunk((w_b.at[8, rows], w_b.at[0, rows]), (w_b.at[5, rows], w_b.at[13, rows]), 2)
        for i in range(3):
            chunk(
                (w_b.at[5 + i, rows], w_b.at[1 + i, rows]),
                (w_b.at[6 + i, rows], w_b.at[10 + i, rows]),
            )
        for i in range(2):
            for half in range(2):
                for row in range(0, 256, 128):
                    rows = pl.ds(PAD + row, 128)
                    chunk(
                        (v_b.at[4 + i, half, rows], v_b.at[i, half, rows]),
                        (v_b.at[4 + i, half, rows], v_b.at[8 + i, half, rows]),
                    )

        send_blocks(0, shrink1(r1), send_r)
        finish = all_rows(1, send_r, True, recv_r)
        chunks[0].start()
        chunks[1].start()
        pl.when(cycle == 0)(later.start)
        finish()
        turn[...] = recv_r[0].T
        lines(chunks)
        back_r[0] = turn[...].T
        finish = all_rows(2, back_r, False, got_r)
        chunks[13].start()
        finish()

        for x in range(16):
            piece = got_r[0, 8 * tile_of(x) : 8 * tile_of(x) + 8, :]
            got_a[1, 8 * x : 8 * x + 8, :] = exchange_parts(piece)
        ends[0] = got_a[1, pl.ds(3, 32, 4), :]
        ends[1] = got_a[1, pl.ds(0, 32, 4), :]
        whole = pair(10, (got_a.at[1], got_a.at[0]), (got_a.at[1], got_a.at[2]))
        outer = pair(11, (ends.at[0], beyond.at[0]), (ends.at[1], beyond.at[1]), 2)
        whole.start()
        outer.start()
        pl.when(cycle == 0)(later.wait)
        for side in (1, 0, 2):
            if side == 0:
                for each in chunks:
                    each.wait()
                whole.wait()
                outer.wait()
            for a in range(2):
                grown[a] = dot(got_a[side], unfold[a])
            for a in range(2):
                for b in range(2):
                    for p in range(4):
                        piece = grown[a, pl.ds(b * 4 + p, 16, 8), :]
                        for i in range(2):
                            rows = pl.ds(PAD + 4 * a + 2 * b + i, 16, 8)
                            q = 4 * side + p + 1
                            w_a[q, rows, :] = w_b[q, rows, :] + piece
        for side in range(2):
            for a in range(2):
                grown[a, 0:32, :] = dot(beyond[side], unfold[a])
                for b in range(2):
                    piece = grown[a, pl.ds(b, 16, 2), :]
                    for i in range(2):
                        rows = pl.ds(PAD + 4 * a + 2 * b + i, 16, 8)
                        w_a[13 * side, rows, :] = w_b[13 * side, rows, :] + piece
        sweep1(w_a, store_second, 4)
        sweep1(w_b, store_error, 3)

        @pl.loop(0, 10)
        def _(p):
            for half in range(2):
                piece = dot(e1[p], spread[half])
                for i in range(2):
                    rows = pl.ds(PAD + i, 128, 2)
                    v_c[p, half, rows, :] = v_b[p, half, rows, :] + piece

        sweep0(v_c, v_b, -2, 8)
        sweep0(v_b, v_a, -1, 6)
        residual0(v_a, False, cycle, 0, 4)

    stores = []
    for p in range(4):
        for half in range(2):
            stores.append(
                pltpu.make_async_copy(
                    v_a.at[p + 3, half, pl.ds(PAD, 256)],
                    out.at[p, :, pl.ds(half * 128, 128)],
                    in_sem.at[0, p, half],
                )
            )
    for copy in stores:
        copy.start()

    sums = [jnp.sum(nacc[c], axis=0, keepdims=True) for c in range(CYCLES)]
    sums = [each + roll_lanes(each, 64) for each in sums]
    first = lax.broadcasted_iota(jnp.int32, (1, 128), 1) < 64
    part[0] = jnp.broadcast_to(jnp.where(first, sums[0], sums[1]), (128, 128))
    all_rows(3, part, True, nz)()
    total = jnp.sum(nz[0], axis=0, keepdims=True)
    norms[0] = jnp.sum(jnp.where(first, total, 0.0)) * (1.0 / (512 * 256 * 256))
    norms[1] = jnp.sum(jnp.where(first, 0.0, total)) * (1.0 / (512 * 256 * 256))
    for copy in stores:
        copy.wait()


def vmem(*shape):
    return pltpu.VMEM(shape, F32)


def shards(source, vertical, reaction):
    dma = pltpu.SemaphoreType.DMA
    solved, norms = pl.pallas_call(
        kernel,
        out_shape=(
            jax.ShapeDtypeStruct((4, 256, 256), F32),
            jax.ShapeDtypeStruct((CYCLES,), F32),
        ),
        in_specs=[
            pl.BlockSpec(memory_space=pltpu.HBM),
            pl.BlockSpec(memory_space=pltpu.SMEM),
            pl.BlockSpec(memory_space=pltpu.HBM),
        ],
        out_specs=(pl.BlockSpec(memory_space=pltpu.HBM), pl.BlockSpec(memory_space=pltpu.SMEM)),
        scratch_shapes=[
            vmem(10, 2, 256 + 2 * PAD, 128),
            vmem(10, 2, 256 + 2 * PAD, 128),
            vmem(10, 2, 256 + 2 * PAD, 128),
            vmem(10, 2, 256 + 2 * PAD, 128),
            vmem(8, 2, 256, 128),
            vmem(4, 2, 256, 128),
            vmem(8, 2, 256, 128),
            vmem(4, 2, 256, 128),
            vmem(12, 8, 128),
            vmem(14, 128 + 2 * PAD, 128),
            vmem(14, 128 + 2 * PAD, 128),
            vmem(12, 128, 128),
            vmem(4, 128, 128),
            vmem(12, 128, 128),
            vmem(4, 128, 128),
            vmem(10, 128, 128),
            pltpu.VMEM((2, 128, 128), jnp.bfloat16),
            pltpu.VMEM((2, 128, 128), jnp.bfloat16),
            vmem(2, 128, 128),
            pltpu.VMEM((2, 128, 128), jnp.bfloat16),
            pltpu.VMEM((2, 128, 128), jnp.bfloat16),
            vmem(2, 128, 128),
            vmem(2, 128, 128),
            vmem(1, 128, 128),
            vmem(1, 128, 128),
            vmem(128, 128),
            vmem(1, 128, 128),
            vmem(1, 128, 128),
            vmem(3, 128, 128),
            vmem(2, 32, 128),
            vmem(2, 32, 128),
            vmem(2, 128, 128),
            vmem(7, 32, 128),
            vmem(2, 32, 128),
            vmem(7, 2 * STEPS + 1, 32, 128),
            vmem(EVENTS, 128, 128),
            vmem(EVENTS, 2, 32, 128),
            vmem(EVENTS, 2, 16, 128),
            vmem(EVENTS, 2, 16, 128),
            vmem(4, 32, 128),
            vmem(2, 32, 128),
            vmem(2, 32, 128),
            vmem(CYCLES, 8, 128),
            vmem(1, 128, 128),
            vmem(1, 128, 128),
            dma((2, 4, 2)),
            dma((13, 2)),
            dma((13, 2)),
            dma((14, 2)),
            dma((14, 2)),
            dma((4,)),
            dma((4,)),
            dma((EVENTS, 4)),
            dma((EVENTS, 4)),
        ],
        compiler_params=pltpu.CompilerParams(
            collective_id=0, has_side_effects=True, vmem_limit_bytes=63 * 1024 * 1024
        ),
    )(source, vertical, reaction)
    return solved, norms


def solution(mesh):
    planes = P(("gz", "gy"), None, None)
    return jax.shard_map(
        shards,
        mesh=mesh,
        in_specs=(planes, P(("gz", "gy")), planes),
        out_specs=(planes, P()),
        check_vma=False,
    )
```

```python
import functools

import jax
import jax.numpy as jnp
from jax import lax
from jax.experimental import pallas as pl
from jax.experimental.pallas import tpu as pltpu
from jax.sharding import PartitionSpec as P

F32 = jnp.float32
MESH = pl.DeviceIdType.MESH
CYCLES = 2
STEPS = 9
EVENTS = 11
OMEGA = 0.8
H = (1.0, 0.25, 1.0 / 16, 1.0 / 64, 1.0 / 256)
GROUP_Z = 16
GROUP_Y = 8
DEVICES = 128
PAD = 8
PLAN = {0: (2,), 1: (3,), 2: (4,), 4: (5,), 6: (6,), 8: (7,), 9: (8,), 10: (9,)}


def device_of(a, b):
    wide = lax.div(a, 8) * 8 + lax.rem(lax.div(a, 2), 4) * 2 + lax.div(b, 4)
    return (wide, lax.rem(a, 2) * 4 + lax.rem(b, 4))


def place_wide(a):
    z, x = lax.div(a, 8) * 2 + lax.rem(a, 2), lax.rem(lax.div(a, 2), 4)
    return z * 4 + x + lax.rem(z, 2) * (3 - 2 * x)


def member_wide(place):
    z, x = lax.div(place, 4), lax.rem(place, 4)
    x = x + lax.rem(z, 2) * (3 - 2 * x)
    return (lax.div(z, 2) * 4 + x) * 2 + lax.rem(z, 2)


def place_narrow(b):
    core, y = lax.div(b, 4), lax.rem(b, 4)
    return y * 2 + core + lax.rem(y, 2) * (1 - 2 * core)


def member_narrow(place):
    y, core = lax.div(place, 2), lax.rem(place, 2)
    core = core + lax.rem(y, 2) * (1 - 2 * core)
    return core * 4 + y


def dot(a, b):
    total = None
    for part in range(3):
        piece = a.astype(jnp.bfloat16)
        product = jnp.dot(piece, b, preferred_element_type=F32)
        total = product if total is None else total + product
        if part < 2:
            a = a - piece.astype(F32)
    return total


def roll_lanes(v, s):
    return pltpu.roll(v, s % 128, 1)


def roll_rows(v, s):
    return pltpu.roll(v, s % 8, 0)


def lane_iota():
    return lax.broadcasted_iota(jnp.int32, (8, 128), 1)


def row_iota():
    return lax.broadcasted_iota(jnp.int32, (8, 128), 0)


def below(v, s):
    if s < 4:
        return [v[p - s] if p >= s else roll_lanes(v[p - s + 4], 1) for p in range(4)]
    return [roll_lanes(v[p], s // 4) for p in range(4)]


def above(v, s):
    if s < 4:
        return [v[p + s] if p + s < 4 else roll_lanes(v[p + s - 4], -1) for p in range(4)]
    return [roll_lanes(v[p], -(s // 4)) for p in range(4)]


def exchange_parts(v):
    row, lane = row_iota(), lane_iota()
    for m in (1, 2, 4):
        down = lax.rem(lax.div(row, m), 2)
        across = lax.rem(lax.div(lane, 16 * m), 2)
        moved = jnp.where(
            down == 1,
            roll_rows(roll_lanes(v, -16 * m), m),
            roll_rows(roll_lanes(v, 16 * m), -m),
        )
        v = jnp.where(down == across, v, moved)
    return v


def tile_of(x):
    z, q = divmod(x, 4)
    return ((z // 2) * 4 + (3 - q if z % 2 else q)) * 2 + z % 2


def kernel(
    source, vertical, reaction, out, norms,
    v_a, v_b, v_c, v_d, g0, d0, j0, r0, vt, w_a, w_b, g1, d1, j1, r1, e1, compact, spread, lhs,
    fold, unfold, send_s, recv_s, send_r, recv_r, turn, back_r, got_r, got_a, beyond, ends, grown,
    dl, vl, cf, val, hx, hy, ys, rhs2, rhs3, res, give, take,
    nacc, part, nz,
    in_sem, z_send, z_recv, c_send, c_recv,
    all_send, all_recv, p_send, p_recv, turns, h_send, h_recv,
):
    gz, gy = lax.axis_index("gz"), lax.axis_index("gy")
    me = gz * GROUP_Y + gy
    core = lax.rem(gz, 2)
    ia = (lax.div(gz, 8) * 4 + lax.div(lax.rem(gz, 8), 2)) * 2 + lax.div(gy, 4)
    ib = core * 4 + lax.rem(gy, 4)
    wide, narrow = place_wide(ia), place_narrow(ib)

    def device(d):
        d = lax.rem(d + DEVICES, DEVICES)
        return (lax.div(d, GROUP_Y), lax.rem(d, GROUP_Y))

    loads = []
    for p in range(4):
        for half in range(2):
            lanes = pl.ds(half * 128, 128)
            loads.append(pltpu.make_async_copy(source.at[p, :, lanes], g0.at[p + 2, half], in_sem.at[0, p, half]))
            loads.append(pltpu.make_async_copy(reaction.at[p, :, lanes], r0.at[p, half], in_sem.at[1, p, half]))
    for copy in loads:
        copy.start()

    barrier = pltpu.get_barrier_semaphore()

    members = [lax.rem(ib + j, GROUP_Y) for j in range(GROUP_Y)]
    members = [(b, lax.div(b, 4), lax.rem(b, 4)) for b in members]

    def everyone(act):
        def some(k, start):
            a = lax.rem(ia + k, GROUP_Z)
            wide_a, narrow_a = lax.div(a, 2) * 2, lax.rem(a, 2) * 4
            for b, core_b, y_b in members[start:]:
                to = (wide_a + core_b, narrow_a + y_b)
                act(a * GROUP_Y + b, to[0] * GROUP_Y + to[1], to)

        some(0, 1)
        pl.loop(1, GROUP_Z)(lambda k: some(k, 0))

    everyone(
        lambda block, plane, to: pl.semaphore_signal(
            barrier, inc=1, device_id=to, device_id_type=MESH
        )
    )

    for p in range(4):
        vt[p + 4] = jnp.full((8, 128), vertical[p], F32)

    @pl.loop(0, 10)
    def _(i):
        for ref in (v_a, v_b, v_c, v_d):
            for half in range(2):
                for row in (0, PAD + 256):
                    ref[i, half, pl.ds(row, PAD), :] = jnp.zeros((PAD, 128), F32)

    @pl.loop(0, 14)
    def _(i):
        for ref in (w_a, w_b):
            for row in (0, PAD + 128):
                ref[i, pl.ds(row, PAD), :] = jnp.zeros((PAD, 128), F32)

    def clear(side):
        @pl.loop(7 * side, 7 * side + 3)
        def _(i):
            for ref in (v_a, v_b, v_c, v_d):
                for half in range(2):
                    ref[i, half] = jnp.zeros((256 + 2 * PAD, 128), F32)

        @pl.loop(9 * side, 9 * side + 5)
        def _(i):
            for ref in (w_a, w_b):
                ref[i] = jnp.zeros((128 + 2 * PAD, 128), F32)

        for i in range(6 * side, 6 * side + 2):
            for half in range(2):
                g0[i, half] = jnp.zeros((256, 128), F32)
                j0[i, half] = jnp.zeros((256, 128), F32)
        for i in range(8 * side, 8 * side + 4):
            vt[i] = jnp.zeros((8, 128), F32)
            g1[i] = jnp.zeros((128, 128), F32)
            j1[i] = jnp.zeros((128, 128), F32)
        got_a[2 * side] = jnp.zeros((128, 128), F32)
        beyond[side] = jnp.zeros((32, 128), F32)

    for side in range(2):

        @pl.when(me == (DEVICES - 1) * side)
        def _(side=side):
            clear(side)

        @pl.when(me == 1 + (DEVICES - 3) * side)
        def _(side=side):
            for ref in (w_a, w_b):
                ref[13 * side] = jnp.zeros((128 + 2 * PAD, 128), F32)
            beyond[side] = jnp.zeros((32, 128), F32)

    @pl.when(wide == 0)
    def _():
        for e in range(EVENTS):
            hx[e, 0] = jnp.zeros((32, 128), F32)

    @pl.when(wide == GROUP_Z - 1)
    def _():
        for e in range(EVENTS):
            hx[e, 1] = jnp.zeros((32, 128), F32)

    place_y = lax.rem(ib, 4)
    for side in range(2):

        @pl.when(narrow == (GROUP_Y - 1) * side)
        def _(side=side):
            for e in (0, 1, 9, 10):
                hy[e, side] = jnp.zeros((16, 128), F32)

        @pl.when(jnp.logical_and(core == 1, place_y == 3 * side))
        def _(side=side):
            for e in range(2, 9):
                hy[e, side] = jnp.zeros((16, 128), F32)

    from_lane = lax.broadcasted_iota(jnp.int32, (128, 128), 0)
    to_lane = lax.broadcasted_iota(jnp.int32, (128, 128), 1)
    for half in range(2):
        compact[half] = jnp.where(to_lane == 64 * half + from_lane // 2, 0.25, 0.0).astype(jnp.bfloat16)
        part_of = place_narrow(to_lane // 16) * 8 + to_lane % 8
        hit = jnp.logical_and(part_of == from_lane // 2, to_lane // 8 % 2 == half)
        fold[half] = jnp.where(hit, 0.25, 0.0).astype(jnp.bfloat16)
        part_of = place_narrow(from_lane // 16) * 8 + from_lane % 8
        hit = jnp.logical_and(part_of == to_lane // 2, from_lane // 8 % 2 == half)
        unfold[half] = jnp.where(hit, 1.0, 0.0).astype(jnp.bfloat16)
        spread[half] = jnp.where(from_lane == 64 * half + to_lane // 2, 1.0, 0.0).astype(jnp.bfloat16)

    pl.semaphore_wait(barrier, DEVICES - 1)

    has_up, has_down = me < DEVICES - 1, me > 0

    class Pair:
        def __init__(self, up, down, send_sem, recv_sem, steps=1):
            self.steps = steps
            self.copies = [
                pltpu.make_async_remote_copy(
                    src_ref=src, dst_ref=dst, send_sem=send_sem.at[i], recv_sem=recv_sem.at[i],
                    device_id=device(me + shift), device_id_type=MESH,
                )
                for i, (src, dst), shift in ((0, up, steps), (1, down, -steps))
            ]

        def start(self):
            pl.when(me < DEVICES - self.steps)(self.copies[0].start)
            pl.when(me >= self.steps)(self.copies[1].start)

        def wait(self):
            @pl.when(me < DEVICES - self.steps)
            def _():
                self.copies[0].wait_send()
                self.copies[1].wait_recv()

            @pl.when(me >= self.steps)
            def _():
                self.copies[1].wait_send()
                self.copies[0].wait_recv()

    def pair(i, up, down, steps=1):
        return Pair(up, down, z_send.at[i], z_recv.at[i], steps)

    def exchange0(slot, i):
        rows = pl.ds(PAD, 256)
        both = pair(
            i,
            (slot.at[6, :, rows], slot.at[2, :, rows]),
            (slot.at[3, :, rows], slot.at[7, :, rows]),
        )
        both.start()
        return both.wait

    mine = ia * GROUP_Y + ib

    def all_rows(i, src, to_blocks, dst):
        place = me if to_blocks else mine

        def send(block, plane, to):
            pltpu.make_async_remote_copy(
                src_ref=src.at[:, pl.ds(block if to_blocks else plane, 1)],
                dst_ref=dst.at[:, pl.ds(place, 1)],
                send_sem=all_send.at[i], recv_sem=all_recv.at[i], device_id=to,
                device_id_type=MESH,
            ).start()

        everyone(send)
        dst[:, pl.ds(place, 1), :] = src[:, pl.ds(mine if to_blocks else me, 1), :]

        def finish():
            others = pl.ds(0, DEVICES - 1)
            for sem in (all_recv, all_send):
                pltpu.make_async_copy(src.at[:, others], dst.at[:, others], sem.at[i]).wait()

        return finish

    BLOCK = 32
    lanes0 = lax.broadcasted_iota(jnp.int32, (BLOCK, 128), 1)

    def around0(slot, p, row):
        rows = pl.ds(PAD + row, BLOCK)
        centre = [slot[p + 3, half, rows, :] for half in range(2)]
        left = [pltpu.roll(c, 1, 1) for c in centre]
        right = [pltpu.roll(c, 127, 1) for c in centre]
        sums = [
            jnp.where(lanes0 == 0, 0.0, left[0]) + jnp.where(lanes0 == 127, right[1], right[0]),
            jnp.where(lanes0 == 0, left[0], left[1]) + jnp.where(lanes0 == 127, 0.0, right[1]),
        ]
        coupled = jnp.broadcast_to(vt[p + 4, 0:1, :], (BLOCK, 128))
        total = []
        for half in range(2):
            beside = slot[p + 3, half, pl.ds(PAD + row - 1, BLOCK), :]
            beside = beside + slot[p + 3, half, pl.ds(PAD + row + 1, BLOCK), :]
            along = slot[p + 2, half, rows, :] + slot[p + 4, half, rows, :]
            total.append(H[0] * (sums[half] + beside) + coupled * along)
        return centre, total

    def sweep0(old, new, first, count, step=1):
        @pl.loop(0, count)
        def _(i):
            p = first + i * step
            for row in range(0, 256, BLOCK):
                centre, total = around0(old, p, row)
                rows = pl.ds(row, BLOCK)
                for half in range(2):
                    fresh = g0[p + 2, half, rows, :] + total[half]
                    fresh = (1.0 - OMEGA) * centre[half] + j0[p + 2, half, rows, :] * fresh
                    new[p + 3, half, pl.ds(PAD + row, BLOCK), :] = fresh

    def residual0(slot, keep, sums, first, count, step=1):
        @pl.loop(0, count)
        def _(i):
            p = first + i * step
            for row in range(0, 256, BLOCK):
                centre, total = around0(slot, p, row)
                rows = pl.ds(row, BLOCK)
                for half in range(2):
                    left = g0[p + 2, half, rows, :] + total[half] - d0[p, half, rows, :] * centre[half]
                    if keep:
                        r0[p, half, rows, :] = left
                    else:
                        nacc[sums] += (left * left).reshape(BLOCK // 8, 8, 128).sum(axis=0)

    lanes1 = lax.broadcasted_iota(jnp.int32, (BLOCK, 128), 1)

    def around1(slot, p, row):
        rows = pl.ds(PAD + row, BLOCK)
        centre = slot[p + 5, rows, :]
        sums = jnp.where(lanes1 == 0, 0.0, pltpu.roll(centre, 1, 1))
        sums = sums + jnp.where(lanes1 == 127, 0.0, pltpu.roll(centre, 127, 1))
        sums = sums + slot[p + 5, pl.ds(PAD + row - 1, BLOCK), :]
        sums = sums + slot[p + 5, pl.ds(PAD + row + 1, BLOCK), :]
        along = slot[p + 4, rows, :] + slot[p + 6, rows, :]
        return centre, H[1] * sums + jnp.broadcast_to(vt[p + 4, 0:1, :], (BLOCK, 128)) * along

    def sweep1(old, store, reach):
        @pl.loop(0, 4 + 2 * reach)
        def _(i):
            p = i - reach
            for row in range(0, 128, BLOCK):
                centre, total = around1(old, p, row)
                rows = pl.ds(row, BLOCK)
                fresh = j1[p + 4, rows, :] * (g1[p + 4, rows, :] + total)
                store(p, row, (1.0 - OMEGA) * centre + fresh)

    def store_second(p, row, fresh):
        w_b[p + 5, pl.ds(PAD + row, BLOCK), :] = fresh

    def store_error(p, row, fresh):
        e1[p + 3, pl.ds(row, BLOCK), :] = fresh

    def residual1():
        @pl.loop(0, 4)
        def _(p):
            for row in range(0, 128, BLOCK):
                centre, total = around1(w_b, p, row)
                rows = pl.ds(row, BLOCK)
                r1[p, rows, :] = g1[p + 4, rows, :] + total - d1[p, rows, :] * centre

    def shrink0(src, dst, first):
        @pl.loop(0, 4)
        def _(p):
            total = jnp.zeros((128, 128), F32)
            for half in range(2):
                pairs = src[p, half, pl.ds(0, 128, 2), :] + src[p, half, pl.ds(1, 128, 2), :]
                total = total + dot(pairs, compact[half])
            dst[p + first] = total

    def shrink1(src):
        total = jnp.zeros((128, 128), F32)
        for a in range(2):
            for b in range(2):
                for p in range(4):
                    first = 4 * a + 2 * b
                    pairs = src[p, pl.ds(first, 16, 8), :] + src[p, pl.ds(first + 1, 16, 8), :]
                    lhs[a, pl.ds(b * 4 + p, 16, 8), :] = pairs
            total = total + dot(lhs[a], fold[a])
        return total

    early = []
    for i in range(2):
        for half in range(2):
            lanes = pl.ds(half * 128, 128)
            early.append(
                pair(
                    4 + 2 * i + half,
                    (source.at[2 + i, :, lanes], g0.at[i, half]),
                    (source.at[i, :, lanes], g0.at[6 + i, half]),
                )
            )
    early.append(pair(2, (vt.at[4:8], vt.at[0:4]), (vt.at[4:8], vt.at[8:12])))
    for both in early:
        both.start()
    for copy in loads:
        copy.wait()
    shrink0(r0, r1, 0)

    @pl.loop(0, 4)
    def _(p):
        coupled = 2.0 * vertical[p]
        for half in range(2):
            for row in range(0, 256, 64):
                rows = pl.ds(row, 64)
                diagonal = coupled + 4.0 * H[0] + r0[p, half, rows, :]
                d0[p, half, rows, :] = diagonal
                j0[p + 2, half, rows, :] = OMEGA / diagonal
        diagonal = coupled + 4.0 * H[1] + r1[p]
        d1[p] = diagonal
        j1[p + 4] = OMEGA / diagonal

    def send_blocks(f, v, dst):
        for x in range(16):
            dst[f, 8 * tile_of(x) : 8 * tile_of(x) + 8, :] = exchange_parts(v[8 * x : 8 * x + 8])

    send_blocks(0, shrink1(r1), send_s)
    plane = lane_iota() // 16 % 4
    coupling = jnp.zeros((8, 128), F32)
    for p in range(4):
        coupling = jnp.where(plane == p, vertical[p], coupling)
    for x in range(16):
        send_s[1, 8 * x : 8 * x + 8, :] = coupling
    finish = all_rows(0, send_s, True, recv_s)
    early.append(pair(8, (j0.at[4:6], j0.at[0:2]), (j0.at[2:4], j0.at[6:8])))
    late = pair(9, (j1.at[6:8], j1.at[2:4]), (j1.at[4:6], j1.at[8:10]))
    later = pair(12, (j1.at[4:6], j1.at[0:2]), (j1.at[6:8], j1.at[10:12]))
    early[-1].start()
    late.start()
    finish()

    lane, row = lane_iota(), row_iota()

    def tile(p):
        return pl.ds(8 * p, 8)

    def unpack(v):
        return [
            [v[8 * (8 * b + 2 * p + a) : 8 * (8 * b + 2 * p + a) + 8] for p in range(4)]
            for a in range(2)
            for b in range(2)
        ]

    def shrink2(v):
        result = []
        for a in range(2):
            mine = []
            for p in range(4):
                t = v[2 * a][p] + v[2 * a + 1][p]
                t = t + jnp.where(row % 2 == 1, roll_rows(t, 1), roll_rows(t, -1))
                mine.append(0.25 * t)
            result.append(mine)
        return result

    def shrink3(v):
        mine = []
        for p in range(4):
            t = v[0][p] + v[1][p]
            t = t + jnp.where(row % 4 >= 2, roll_rows(t, 2), roll_rows(t, -2))
            mine.append(0.25 * t)
        return [mine]

    couplings = unpack(recv_s[1].T)[0]
    for p in range(4):
        vl[0, tile(p), :] = jnp.where(lane == 0, 0.0, couplings[p]) if p == 0 else couplings[p]
        vl[1, tile(p), :] = jnp.where(lane == 127, 0.0, couplings[p]) if p == 3 else couplings[p]
    react2 = unpack(recv_s[0].T)
    own_row = row % 2 == lax.rem(narrow, 2)

    def to_partner(i):
        return pltpu.make_async_remote_copy(
            src_ref=give.at[i], dst_ref=take.at[i], send_sem=p_send.at[i], recv_sem=p_recv.at[i],
            device_id=device_of(ia, lax.rem(ib + 4, GROUP_Y)), device_id_type=MESH,
        )

    def merge(i, v):
        for x in range(2):
            for p in range(4):
                give[i, tile(4 * x + p), :] = v[x][p]
        copy = to_partner(i)
        copy.start()
        copy.wait()
        return [
            [jnp.where(own_row, v[x][p], take[i, tile(4 * x + p), :]) for p in range(4)]
            for x in range(2)
        ]

    def unmerge(v):
        shifted = jnp.where(lax.rem(narrow, 2) == 0, roll_rows(v, 1), roll_rows(v, -1))
        return jnp.where(own_row, v, shifted)

    react3 = merge(0, shrink2(react2))
    react4 = shrink3(react3)
    order = [(2, each) for each in react2] + [(3, each) for each in react3] + [(4, react4[0])]
    for i, (level, lines) in enumerate(order):
        for p in range(4):
            dl[i, tile(p), :] = 2.0 * couplings[p] + 4.0 * H[level] + lines[p]

    @pl.loop(0, 7)
    def _(i):
        def put(n, v):
            cf[i, tile(n), :] = v

        def next_lane(v):
            return roll_lanes(v, -1)

        a = [-vl[0, tile(p), :] for p in range(4)]
        c = [-vl[1, tile(p), :] for p in range(4)]
        b = [dl[i, tile(p), :] for p in range(4)]
        left1, right1 = -a[1] / b[0], -c[1] / b[2]
        left3, right3 = -a[3] / b[2], -c[3] / next_lane(b[0])
        b1 = b[1] + left1 * c[0] + right1 * a[2]
        a1, c1 = left1 * a[0], right1 * c[2]
        b3 = b[3] + left3 * c[2] + right3 * next_lane(a[0])
        a3, c3 = left3 * a[2], right3 * next_lane(c[0])
        for n, v in enumerate((left1, right1, left3, right3)):
            put(n, v)
        left, right = -a3 / b1, -c3 / next_lane(b1)
        put(4, left)
        put(5, right)
        middle = b3 + left * c1 + right * next_lane(a1)
        low, high = left * a1, right * next_lane(c1)
        for k in range(STEPS - 2):
            t = 1 << k
            left = -low / roll_lanes(middle, t)
            right = -high / roll_lanes(middle, -t)
            put(6 + 2 * k, left)
            put(7 + 2 * k, right)
            middle = middle + left * roll_lanes(high, t) + right * roll_lanes(low, -t)
            low, high = left * roll_lanes(low, t), right * roll_lanes(high, -t)
        put(20, 1.0 / middle)
        for n, (below_it, it, above_it) in enumerate(((a1, b1, c1), (a[0], b[0], c[0]), (a[2], b[2], c[2]))):
            inverse = 1.0 / it
            put(21 + 3 * n, inverse)
            put(22 + 3 * n, below_it * inverse)
            put(23 + 3 * n, above_it * inverse)

    first_of = {2: 0, 3: 4, 4: 6}
    count_of = {2: 4, 3: 2, 4: 1}

    def solve(level, right):
        solved = []
        for x in range(count_of[level]):
            i = first_of[level] + x

            def at(n, i=i):
                return cf[i, tile(n), :]

            r0_, r1_, r2_, r3_ = right[x]
            odd = r1_ + at(0) * r0_ + at(1) * r2_
            r = r3_ + at(2) * r2_ + at(3) * roll_lanes(r0_, -1)
            r = r + at(4) * odd + at(5) * roll_lanes(odd, -1)
            for k in range(STEPS - 2):
                t = 1 << k
                r = r + at(6 + 2 * k) * roll_lanes(r, t) + at(7 + 2 * k) * roll_lanes(r, -t)
            w3 = r * at(20)
            before = roll_lanes(w3, 1)
            w1 = odd * at(21) - at(22) * before - at(23) * w3
            w0 = r0_ * at(24) - at(25) * before - at(26) * w1
            w2 = r2_ * at(27) - at(28) * w1 - at(29) * w3
            solved.append([w0, w1, w2, w3])
        return solved

    def around(level, event, v, chunks):
        count = count_of[level]
        for x in range(count):
            for p in range(4):
                val[event, pl.ds((x * 4 + p) * 8, 8), :] = v[x][p]
        size = 4 * count
        ys[event, 0, 0:size, :] = val[event, pl.ds(0, size, 8), :]
        ys[event, 1, 0:size, :] = val[event, pl.ds(7, size, 8), :]
        span = pl.ds(0, size)
        if level == 2:
            above_y, below_y = member_narrow(narrow + 1), member_narrow(narrow - 1)
            has_y = (narrow < GROUP_Y - 1, narrow > 0)
        else:
            above_y, below_y = ib + 1, ib - 1
            has_y = (place_y < 3, place_y > 0)
        copies = []
        for side, src, dst, there in (
            (0, val.at[event, pl.ds(32 * (count - 1), 32)], hx.at[event, 0], device_of(member_wide(wide + 1), ib)),
            (1, val.at[event, pl.ds(0, 32)], hx.at[event, 1], device_of(member_wide(wide - 1), ib)),
            (2, ys.at[event, 1, span], hy.at[event, 0, span], device_of(ia, above_y)),
            (3, ys.at[event, 0, span], hy.at[event, 1, span], device_of(ia, below_y)),
        ):
            copies.append(
                pltpu.make_async_remote_copy(
                    src_ref=src, dst_ref=dst, send_sem=h_send.at[event, side],
                    recv_sem=h_recv.at[event, side], device_id=there, device_id_type=MESH,
                )
            )
        has = (wide < GROUP_Z - 1, wide > 0) + has_y
        for side in range(4):
            pl.when(has[side])(copies[side].start)
        for n in PLAN.get(event, ()):
            chunks[n].start()
        if level > 2:
            pl.semaphore_signal(
                turns.at[event], inc=1, device_id=device_of(ia, lax.rem(ib + 4, GROUP_Y)),
                device_id_type=MESH,
            )
        for side in range(4):
            pl.when(has[side])(copies[side].wait_send)
            pl.when(has[side])(copies[side ^ 1].wait_recv)

        def beside(mine, low, high):
            def rolled(s):
                return roll_rows(mine, s)

            if level == 2:
                return jnp.where(row < 1, low, rolled(1)) + jnp.where(row >= 7, high, rolled(-1))
            if level == 3:
                before = jnp.where(row == 0, low, jnp.where(row == 1, rolled(3), rolled(2)))
                after = jnp.where(row == 7, high, jnp.where(row == 6, rolled(-3), rolled(-2)))
                return before + after
            even = row % 2 == 0
            before = jnp.where(row >= 4, rolled(4), jnp.where(even, low, rolled(-3)))
            after = jnp.where(row < 4, rolled(4), jnp.where(even, rolled(3), high))
            return before + after

        result = []
        for x in range(count):
            mine = []
            for p in range(4):
                total = v[x - 1][p] if x else hx[event, 0, tile(p), :]
                total = total + (v[x + 1][p] if x + 1 < count else hx[event, 1, tile(p), :])
                low = jnp.broadcast_to(hy[event, 0, pl.ds(x * 4 + p, 1), :], (8, 128))
                high = jnp.broadcast_to(hy[event, 1, pl.ds(x * 4 + p, 1), :], (8, 128))
                mine.append(total + beside(v[x][p], low, high))
            result.append(mine)
        return result

    def relax(level, target, total):
        return solve(
            level,
            [
                [target[a][g] + H[level] * total[a][g] for g in range(4)]
                for a in range(count_of[level])
            ],
        )

    def residual(level, target, v, total):
        result = []
        for a in range(count_of[level]):
            down, up = below(v[a], 1), above(v[a], 1)
            result.append([
                target[a][g] + H[level] * total[a][g] - dl[first_of[level] + a, tile(g), :] * v[a][g]
                + vl[0, tile(g), :] * down[g] + vl[1, tile(g), :] * up[g]
                for g in range(4)
            ])
        return result

    def load(ref, count):
        return [[ref[a, tile(g), :] for g in range(4)] for a in range(count)]

    def keep(ref, v):
        for a in range(len(v)):
            for g in range(4):
                ref[a, tile(g), :] = v[a][g]

    def lines(chunks):
        target2 = lambda: unpack(turn)
        v = solve(2, target2())
        v = relax(2, target2(), around(2, 0, v, chunks))
        r = residual(2, target2(), v, around(2, 1, v, chunks))
        keep(rhs2, v)
        keep(rhs3, merge(1, shrink2(r)))
        back = to_partner(2)

        @pl.when(core == 0)
        def _():
            for e in range(2, 9):
                pl.semaphore_wait(turns.at[e], 1)
                for n in PLAN.get(e, ()):
                    chunks[n].start()
            back.wait_recv()

        @pl.when(core == 1)
        def _():
            target3 = lambda: load(rhs3, 2)
            v = solve(3, target3())
            v = relax(3, target3(), around(3, 2, v, chunks))
            r = residual(3, target3(), v, around(3, 3, v, chunks))
            keep(res, v)
            target4 = shrink3(r)
            v = solve(4, target4)
            for e in range(3):
                v = relax(4, target4, around(4, 4 + e, v, chunks))
            w = load(res, 2)
            v = [[w[a][g] + v[0][g] for g in range(4)] for a in range(2)]
            v = relax(3, target3(), around(3, 7, v, chunks))
            v = relax(3, target3(), around(3, 8, v, chunks))
            for x in range(2):
                for p in range(4):
                    give[2, tile(4 * x + p), :] = v[x][p]
                    take[2, tile(4 * x + p), :] = v[x][p]
            back.start()
            back.wait_send()

        v = [[unmerge(take[2, tile(4 * x + p), :]) for p in range(4)] for x in range(2)]
        w = load(rhs2, 4)
        v = [[w[x][p] + v[x // 2][p] for p in range(4)] for x in range(4)]
        v = relax(2, target2(), around(2, 9, v, chunks))
        v = relax(2, target2(), around(2, 10, v, chunks))
        for a in range(2):
            for b in range(2):
                for p in range(4):
                    turn[pl.ds(8 * (8 * b + 2 * p + a), 8), :] = v[2 * a + b][p]

    nacc[...] = jnp.zeros((CYCLES, 8, 128), F32)

    for both in early:
        both.wait()

    @pl.loop(0, CYCLES)
    def _(cycle):
        @pl.when(cycle == 0)
        def _():
            @pl.loop(0, 8)
            def _(p):
                for half in range(2):
                    for row in range(0, 256, 64):
                        fresh = j0[p, half, pl.ds(row, 64), :] * g0[p, half, pl.ds(row, 64), :]
                        v_c[p + 1, half, pl.ds(PAD + row, 64), :] = fresh

            sweep0(v_c, v_b, -1, 6)
            residual0(v_b, True, 0, 1, 2)
            late.wait()

        @pl.when(cycle > 0)
        def _():
            sweep0(v_a, v_d, 0, 2, 3)
            finish = exchange0(v_d, 0)
            sweep0(v_a, v_d, 1, 2)
            sweep0(v_d, v_b, 1, 2)
            finish()
            sweep0(v_d, v_b, 0, 2, 3)
            finish = exchange0(v_b, 1)
            residual0(v_b, True, 0, 1, 2)
            finish()

        residual0(v_b, True, 0, 0, 2, 3)
        shrink0(r0, g1, 4)
        both = pair(3, (g1.at[6:8], g1.at[2:4]), (g1.at[4:6], g1.at[8:10]))
        both.start()
        both.wait()

        @pl.loop(0, 8)
        def _(p):
            w_a[p + 3, pl.ds(PAD, 128), :] = j1[p + 2] * g1[p + 2]

        sweep1(w_a, store_second, 1)
        residual1()

        chunks = []

        def chunk(up, down, steps=1):
            i = len(chunks)
            chunks.append(Pair(up, down, c_send.at[i], c_recv.at[i], steps))

        for i in range(2):
            chunk((g1.at[4 + i], g1.at[i]), (g1.at[6 + i], g1.at[10 + i]))
        rows = pl.ds(PAD, 128)
        chunk((w_b.at[8, rows], w_b.at[0, rows]), (w_b.at[5, rows], w_b.at[13, rows]), 2)
        for i in range(3):
            chunk(
                (w_b.at[5 + i, rows], w_b.at[1 + i, rows]),
                (w_b.at[6 + i, rows], w_b.at[10 + i, rows]),
            )
        for i in range(2):
            for half in range(2):
                for row in range(0, 256, 128):
                    rows = pl.ds(PAD + row, 128)
                    chunk(
                        (v_b.at[4 + i, half, rows], v_b.at[i, half, rows]),
                        (v_b.at[4 + i, half, rows], v_b.at[8 + i, half, rows]),
                    )

        send_blocks(0, shrink1(r1), send_r)
        finish = all_rows(1, send_r, True, recv_r)
        chunks[0].start()
        chunks[1].start()
        chunks[10].start()
        pl.when(cycle == 0)(later.start)
        finish()
        turn[...] = recv_r[0].T
        lines(chunks)
        back_r[0] = turn[...].T
        finish = all_rows(2, back_r, False, got_r)
        chunks[11].start()
        chunks[12].start()
        chunks[13].start()
        finish()

        for x in range(16):
            piece = got_r[0, 8 * tile_of(x) : 8 * tile_of(x) + 8, :]
            got_a[1, 8 * x : 8 * x + 8, :] = exchange_parts(piece)
        ends[0] = got_a[1, pl.ds(3, 32, 4), :]
        ends[1] = got_a[1, pl.ds(0, 32, 4), :]
        whole = pair(10, (got_a.at[1], got_a.at[0]), (got_a.at[1], got_a.at[2]))
        outer = pair(11, (ends.at[0], beyond.at[0]), (ends.at[1], beyond.at[1]), 2)
        whole.start()
        outer.start()
        pl.when(cycle == 0)(later.wait)
        for side in (1, 0, 2):
            if side == 0:
                for each in chunks:
                    each.wait()
                whole.wait()
                outer.wait()
            for a in range(2):
                grown[a] = dot(got_a[side], unfold[a])
            for a in range(2):
                for b in range(2):
                    for p in range(4):
                        piece = grown[a, pl.ds(b * 4 + p, 16, 8), :]
                        for i in range(2):
                            rows = pl.ds(PAD + 4 * a + 2 * b + i, 16, 8)
                            q = 4 * side + p + 1
                            w_a[q, rows, :] = w_b[q, rows, :] + piece
        for side in range(2):
            for a in range(2):
                grown[a, 0:32, :] = dot(beyond[side], unfold[a])
                for b in range(2):
                    piece = grown[a, pl.ds(b, 16, 2), :]
                    for i in range(2):
                        rows = pl.ds(PAD + 4 * a + 2 * b + i, 16, 8)
                        w_a[13 * side, rows, :] = w_b[13 * side, rows, :] + piece
        sweep1(w_a, store_second, 4)
        sweep1(w_b, store_error, 3)

        @pl.loop(0, 10)
        def _(p):
            for half in range(2):
                piece = dot(e1[p], spread[half])
                for i in range(2):
                    rows = pl.ds(PAD + i, 128, 2)
                    v_c[p, half, rows, :] = v_b[p, half, rows, :] + piece

        sweep0(v_c, v_b, -2, 8)
        sweep0(v_b, v_a, -1, 6)
        residual0(v_a, False, cycle, 0, 4)

    stores = []
    for p in range(4):
        for half in range(2):
            stores.append(
                pltpu.make_async_copy(
                    v_a.at[p + 3, half, pl.ds(PAD, 256)],
                    out.at[p, :, pl.ds(half * 128, 128)],
                    in_sem.at[0, p, half],
                )
            )
    for copy in stores:
        copy.start()

    sums = [jnp.sum(nacc[c], axis=0, keepdims=True) for c in range(CYCLES)]
    sums = [each + roll_lanes(each, 64) for each in sums]
    first = lax.broadcasted_iota(jnp.int32, (1, 128), 1) < 64
    part[0] = jnp.broadcast_to(jnp.where(first, sums[0], sums[1]), (128, 128))
    all_rows(3, part, True, nz)()
    total = jnp.sum(nz[0], axis=0, keepdims=True)
    norms[0] = jnp.sum(jnp.where(first, total, 0.0)) * (1.0 / (512 * 256 * 256))
    norms[1] = jnp.sum(jnp.where(first, 0.0, total)) * (1.0 / (512 * 256 * 256))
    for copy in stores:
        copy.wait()


def vmem(*shape):
    return pltpu.VMEM(shape, F32)


def shards(source, vertical, reaction):
    dma = pltpu.SemaphoreType.DMA
    solved, norms = pl.pallas_call(
        kernel,
        out_shape=(
            jax.ShapeDtypeStruct((4, 256, 256), F32),
            jax.ShapeDtypeStruct((CYCLES,), F32),
        ),
        in_specs=[
            pl.BlockSpec(memory_space=pltpu.HBM),
            pl.BlockSpec(memory_space=pltpu.SMEM),
            pl.BlockSpec(memory_space=pltpu.HBM),
        ],
        out_specs=(pl.BlockSpec(memory_space=pltpu.HBM), pl.BlockSpec(memory_space=pltpu.SMEM)),
        scratch_shapes=[
            vmem(10, 2, 256 + 2 * PAD, 128),
            vmem(10, 2, 256 + 2 * PAD, 128),
            vmem(10, 2, 256 + 2 * PAD, 128),
            vmem(10, 2, 256 + 2 * PAD, 128),
            vmem(8, 2, 256, 128),
            vmem(4, 2, 256, 128),
            vmem(8, 2, 256, 128),
            vmem(4, 2, 256, 128),
            vmem(12, 8, 128),
            vmem(14, 128 + 2 * PAD, 128),
            vmem(14, 128 + 2 * PAD, 128),
            vmem(12, 128, 128),
            vmem(4, 128, 128),
            vmem(12, 128, 128),
            vmem(4, 128, 128),
            vmem(10, 128, 128),
            pltpu.VMEM((2, 128, 128), jnp.bfloat16),
            pltpu.VMEM((2, 128, 128), jnp.bfloat16),
            vmem(2, 128, 128),
            pltpu.VMEM((2, 128, 128), jnp.bfloat16),
            pltpu.VMEM((2, 128, 128), jnp.bfloat16),
            vmem(2, 128, 128),
            vmem(2, 128, 128),
            vmem(1, 128, 128),
            vmem(1, 128, 128),
            vmem(128, 128),
            vmem(1, 128, 128),
            vmem(1, 128, 128),
            vmem(3, 128, 128),
            vmem(2, 32, 128),
            vmem(2, 32, 128),
            vmem(2, 128, 128),
            vmem(7, 32, 128),
            vmem(2, 32, 128),
            vmem(7, 240, 128),
            vmem(EVENTS, 128, 128),
            vmem(EVENTS, 2, 32, 128),
            vmem(EVENTS, 2, 16, 128),
            vmem(EVENTS, 2, 16, 128),
            vmem(4, 32, 128),
            vmem(2, 32, 128),
            vmem(2, 32, 128),
            vmem(3, 64, 128),
            vmem(3, 64, 128),
            vmem(CYCLES, 8, 128),
            vmem(1, 128, 128),
            vmem(1, 128, 128),
            dma((2, 4, 2)),
            dma((13, 2)),
            dma((13, 2)),
            dma((14, 2)),
            dma((14, 2)),
            dma((4,)),
            dma((4,)),
            dma((3,)),
            dma((3,)),
            pltpu.SemaphoreType.REGULAR((9,)),
            dma((EVENTS, 4)),
            dma((EVENTS, 4)),
        ],
        compiler_params=pltpu.CompilerParams(
            collective_id=0, has_side_effects=True, vmem_limit_bytes=63 * 1024 * 1024
        ),
    )(source, vertical, reaction)
    return solved, norms


def solution(mesh):
    planes = P(("gz", "gy"), None, None)
    return jax.shard_map(
        shards,
        mesh=mesh,
        in_specs=(planes, P(("gz", "gy")), planes),
        out_specs=(planes, P()),
        check_vma=False,
    )
```

```python
import functools

import jax
import jax.numpy as jnp
from jax import lax
from jax.experimental import pallas as pl
from jax.experimental.pallas import tpu as pltpu
from jax.sharding import PartitionSpec as P

F32 = jnp.float32
MESH = pl.DeviceIdType.MESH
CYCLES = 2
STEPS = 9
EVENTS = 11
OMEGA = 0.8
H = (1.0, 0.25, 1.0 / 16, 1.0 / 64, 1.0 / 256)
GROUP_Z = 16
GROUP_Y = 8
DEVICES = 128
PAD = 8
PLAN = {0: (2,), 1: (3,), 3: (4,), 5: (5,), 7: (6,), 9: (7,), 10: (8,)}


def device_of(a, b):
    wide = lax.div(a, 8) * 8 + lax.rem(lax.div(a, 2), 4) * 2 + lax.div(b, 4)
    return (wide, lax.rem(a, 2) * 4 + lax.rem(b, 4))


def place_wide(a):
    z, x = lax.div(a, 8) * 2 + lax.rem(a, 2), lax.rem(lax.div(a, 2), 4)
    return z * 4 + x + lax.rem(z, 2) * (3 - 2 * x)


def member_wide(place):
    z, x = lax.div(place, 4), lax.rem(place, 4)
    x = x + lax.rem(z, 2) * (3 - 2 * x)
    return (lax.div(z, 2) * 4 + x) * 2 + lax.rem(z, 2)


def place_narrow(b):
    core, y = lax.div(b, 4), lax.rem(b, 4)
    return y * 2 + core + lax.rem(y, 2) * (1 - 2 * core)


def member_narrow(place):
    y, core = lax.div(place, 2), lax.rem(place, 2)
    core = core + lax.rem(y, 2) * (1 - 2 * core)
    return core * 4 + y


def dot(a, b):
    total = None
    for part in range(3):
        piece = a.astype(jnp.bfloat16)
        product = jnp.dot(piece, b, preferred_element_type=F32)
        total = product if total is None else total + product
        if part < 2:
            a = a - piece.astype(F32)
    return total


def roll_lanes(v, s):
    return pltpu.roll(v, s % 128, 1)


def roll_rows(v, s):
    return pltpu.roll(v, s % 8, 0)


def lane_iota():
    return lax.broadcasted_iota(jnp.int32, (8, 128), 1)


def row_iota():
    return lax.broadcasted_iota(jnp.int32, (8, 128), 0)


def below(v, s):
    if s < 4:
        return [v[p - s] if p >= s else roll_lanes(v[p - s + 4], 1) for p in range(4)]
    return [roll_lanes(v[p], s // 4) for p in range(4)]


def above(v, s):
    if s < 4:
        return [v[p + s] if p + s < 4 else roll_lanes(v[p + s - 4], -1) for p in range(4)]
    return [roll_lanes(v[p], -(s // 4)) for p in range(4)]


def exchange_parts(v):
    row, lane = row_iota(), lane_iota()
    for m in (1, 2, 4):
        down = lax.rem(lax.div(row, m), 2)
        across = lax.rem(lax.div(lane, 16 * m), 2)
        moved = jnp.where(
            down == 1,
            roll_rows(roll_lanes(v, -16 * m), m),
            roll_rows(roll_lanes(v, 16 * m), -m),
        )
        v = jnp.where(down == across, v, moved)
    return v


def tile_of(x):
    z, q = divmod(x, 4)
    return ((z // 2) * 4 + (3 - q if z % 2 else q)) * 2 + z % 2


def kernel(
    source, vertical, reaction, out, norms,
    v_a, v_b, v_c, v_d, g0, d0, j0, r0, vt, w_a, w_b, g1, d1, j1, r1, e1, compact, spread, lhs,
    fold, unfold, send_s, recv_s, send_r, recv_r, turn, back_r, got_r, got_a, beyond, ends, grown,
    dl, vl, cf, val, hx, hy, ys, rhs2, rhs3, res, give, take,
    nacc, part, nz,
    in_sem, z_send, z_recv, c_send, c_recv,
    all_send, all_recv, p_send, p_recv, turns, h_send, h_recv,
):
    gz, gy = lax.axis_index("gz"), lax.axis_index("gy")
    me = gz * GROUP_Y + gy
    core = lax.rem(gz, 2)
    ia = (lax.div(gz, 8) * 4 + lax.div(lax.rem(gz, 8), 2)) * 2 + lax.div(gy, 4)
    ib = core * 4 + lax.rem(gy, 4)
    wide, narrow = place_wide(ia), place_narrow(ib)

    def device(d):
        d = lax.rem(d + DEVICES, DEVICES)
        return (lax.div(d, GROUP_Y), lax.rem(d, GROUP_Y))

    loads = []
    for p in range(4):
        for half in range(2):
            lanes = pl.ds(half * 128, 128)
            loads.append(pltpu.make_async_copy(source.at[p, :, lanes], g0.at[p + 2, half], in_sem.at[0, p, half]))
            loads.append(pltpu.make_async_copy(reaction.at[p, :, lanes], r0.at[p, half], in_sem.at[1, p, half]))
    for copy in loads:
        copy.start()

    barrier = pltpu.get_barrier_semaphore()

    members = [lax.rem(ib + j, GROUP_Y) for j in range(GROUP_Y)]
    members = [(b, lax.div(b, 4), lax.rem(b, 4)) for b in members]

    def everyone(act):
        def some(k, start):
            a = lax.rem(ia + k, GROUP_Z)
            wide_a, narrow_a = lax.div(a, 2) * 2, lax.rem(a, 2) * 4
            for b, core_b, y_b in members[start:]:
                to = (wide_a + core_b, narrow_a + y_b)
                act(a * GROUP_Y + b, to[0] * GROUP_Y + to[1], to)

        some(0, 1)
        pl.loop(1, GROUP_Z)(lambda k: some(k, 0))

    everyone(
        lambda block, plane, to: pl.semaphore_signal(
            barrier, inc=1, device_id=to, device_id_type=MESH
        )
    )

    for p in range(4):
        vt[p + 4] = jnp.full((8, 128), vertical[p], F32)

    @pl.loop(0, 10)
    def _(i):
        for ref in (v_a, v_b, v_c, v_d):
            for half in range(2):
                for row in (0, PAD + 256):
                    ref[i, half, pl.ds(row, PAD), :] = jnp.zeros((PAD, 128), F32)

    @pl.loop(0, 14)
    def _(i):
        for ref in (w_a, w_b):
            for row in (0, PAD + 128):
                ref[i, pl.ds(row, PAD), :] = jnp.zeros((PAD, 128), F32)

    def clear(side):
        @pl.loop(7 * side, 7 * side + 3)
        def _(i):
            for ref in (v_a, v_b, v_c, v_d):
                for half in range(2):
                    ref[i, half] = jnp.zeros((256 + 2 * PAD, 128), F32)

        @pl.loop(9 * side, 9 * side + 5)
        def _(i):
            for ref in (w_a, w_b):
                ref[i] = jnp.zeros((128 + 2 * PAD, 128), F32)

        for i in range(6 * side, 6 * side + 2):
            for half in range(2):
                g0[i, half] = jnp.zeros((256, 128), F32)
                j0[i, half] = jnp.zeros((256, 128), F32)
        for i in range(8 * side, 8 * side + 4):
            vt[i] = jnp.zeros((8, 128), F32)
            g1[i] = jnp.zeros((128, 128), F32)
            j1[i] = jnp.zeros((128, 128), F32)
        got_a[2 * side] = jnp.zeros((128, 128), F32)
        beyond[side] = jnp.zeros((32, 128), F32)

    for side in range(2):

        @pl.when(me == (DEVICES - 1) * side)
        def _(side=side):
            clear(side)

        @pl.when(me == 1 + (DEVICES - 3) * side)
        def _(side=side):
            for ref in (w_a, w_b):
                ref[13 * side] = jnp.zeros((128 + 2 * PAD, 128), F32)
            beyond[side] = jnp.zeros((32, 128), F32)

    @pl.when(wide == 0)
    def _():
        for e in range(EVENTS):
            hx[e, 0] = jnp.zeros((32, 128), F32)

    @pl.when(wide == GROUP_Z - 1)
    def _():
        for e in range(EVENTS):
            hx[e, 1] = jnp.zeros((32, 128), F32)

    place_y = lax.rem(ib, 4)
    for side in range(2):

        @pl.when(narrow == (GROUP_Y - 1) * side)
        def _(side=side):
            for e in (0, 1, 9, 10):
                hy[e, side] = jnp.zeros((16, 128), F32)

        @pl.when(jnp.logical_and(core == 1, place_y == 3 * side))
        def _(side=side):
            for e in range(2, 9):
                hy[e, side] = jnp.zeros((16, 128), F32)

    from_lane = lax.broadcasted_iota(jnp.int32, (128, 128), 0)
    to_lane = lax.broadcasted_iota(jnp.int32, (128, 128), 1)
    for half in range(2):
        compact[half] = jnp.where(to_lane == 64 * half + from_lane // 2, 0.25, 0.0).astype(jnp.bfloat16)
        part_of = place_narrow(to_lane // 16) * 8 + to_lane % 8
        hit = jnp.logical_and(part_of == from_lane // 2, to_lane // 8 % 2 == half)
        fold[half] = jnp.where(hit, 0.25, 0.0).astype(jnp.bfloat16)
        part_of = place_narrow(from_lane // 16) * 8 + from_lane % 8
        hit = jnp.logical_and(part_of == to_lane // 2, from_lane // 8 % 2 == half)
        unfold[half] = jnp.where(hit, 1.0, 0.0).astype(jnp.bfloat16)
        spread[half] = jnp.where(from_lane == 64 * half + to_lane // 2, 1.0, 0.0).astype(jnp.bfloat16)

    pl.semaphore_wait(barrier, DEVICES - 1)

    has_up, has_down = me < DEVICES - 1, me > 0

    class Pair:
        def __init__(self, up, down, send_sem, recv_sem, steps=1):
            self.steps = steps
            self.copies = [
                pltpu.make_async_remote_copy(
                    src_ref=src, dst_ref=dst, send_sem=send_sem.at[i], recv_sem=recv_sem.at[i],
                    device_id=device(me + shift), device_id_type=MESH,
                )
                for i, (src, dst), shift in ((0, up, steps), (1, down, -steps))
            ]

        def start(self):
            pl.when(me < DEVICES - self.steps)(self.copies[0].start)
            pl.when(me >= self.steps)(self.copies[1].start)

        def wait(self):
            @pl.when(me < DEVICES - self.steps)
            def _():
                self.copies[0].wait_send()
                self.copies[1].wait_recv()

            @pl.when(me >= self.steps)
            def _():
                self.copies[1].wait_send()
                self.copies[0].wait_recv()

    def pair(i, up, down, steps=1):
        return Pair(up, down, z_send.at[i], z_recv.at[i], steps)

    def exchange0(slot, i):
        rows = pl.ds(PAD, 256)
        both = pair(
            i,
            (slot.at[6, :, rows], slot.at[2, :, rows]),
            (slot.at[3, :, rows], slot.at[7, :, rows]),
        )
        both.start()
        return both.wait

    mine = ia * GROUP_Y + ib

    def all_rows(i, src, to_blocks, dst):
        place = me if to_blocks else mine

        def send(block, plane, to):
            pltpu.make_async_remote_copy(
                src_ref=src.at[:, pl.ds(block if to_blocks else plane, 1)],
                dst_ref=dst.at[:, pl.ds(place, 1)],
                send_sem=all_send.at[i], recv_sem=all_recv.at[i], device_id=to,
                device_id_type=MESH,
            ).start()

        everyone(send)
        dst[:, pl.ds(place, 1), :] = src[:, pl.ds(mine if to_blocks else me, 1), :]

        def finish():
            others = pl.ds(0, DEVICES - 1)
            for sem in (all_recv, all_send):
                pltpu.make_async_copy(src.at[:, others], dst.at[:, others], sem.at[i]).wait()

        return finish

    BLOCK = 32
    lanes0 = lax.broadcasted_iota(jnp.int32, (BLOCK, 128), 1)

    def around0(slot, p, row):
        rows = pl.ds(PAD + row, BLOCK)
        centre = [slot[p + 3, half, rows, :] for half in range(2)]
        left = [pltpu.roll(c, 1, 1) for c in centre]
        right = [pltpu.roll(c, 127, 1) for c in centre]
        sums = [
            jnp.where(lanes0 == 0, 0.0, left[0]) + jnp.where(lanes0 == 127, right[1], right[0]),
            jnp.where(lanes0 == 0, left[0], left[1]) + jnp.where(lanes0 == 127, 0.0, right[1]),
        ]
        coupled = jnp.broadcast_to(vt[p + 4, 0:1, :], (BLOCK, 128))
        total = []
        for half in range(2):
            beside = slot[p + 3, half, pl.ds(PAD + row - 1, BLOCK), :]
            beside = beside + slot[p + 3, half, pl.ds(PAD + row + 1, BLOCK), :]
            along = slot[p + 2, half, rows, :] + slot[p + 4, half, rows, :]
            total.append(H[0] * (sums[half] + beside) + coupled * along)
        return centre, total

    def sweep0(old, new, first, count, step=1):
        @pl.loop(0, count)
        def _(i):
            p = first + i * step
            for row in range(0, 256, BLOCK):
                centre, total = around0(old, p, row)
                rows = pl.ds(row, BLOCK)
                for half in range(2):
                    fresh = g0[p + 2, half, rows, :] + total[half]
                    fresh = (1.0 - OMEGA) * centre[half] + j0[p + 2, half, rows, :] * fresh
                    new[p + 3, half, pl.ds(PAD + row, BLOCK), :] = fresh

    def residual0(slot, keep, sums, first, count, step=1):
        @pl.loop(0, count)
        def _(i):
            p = first + i * step
            for row in range(0, 256, BLOCK):
                centre, total = around0(slot, p, row)
                rows = pl.ds(row, BLOCK)
                for half in range(2):
                    left = g0[p + 2, half, rows, :] + total[half] - d0[p, half, rows, :] * centre[half]
                    if keep:
                        r0[p, half, rows, :] = left
                    else:
                        nacc[sums] += (left * left).reshape(BLOCK // 8, 8, 128).sum(axis=0)

    lanes1 = lax.broadcasted_iota(jnp.int32, (BLOCK, 128), 1)

    def around1(slot, p, row):
        rows = pl.ds(PAD + row, BLOCK)
        centre = slot[p + 5, rows, :]
        sums = jnp.where(lanes1 == 0, 0.0, pltpu.roll(centre, 1, 1))
        sums = sums + jnp.where(lanes1 == 127, 0.0, pltpu.roll(centre, 127, 1))
        sums = sums + slot[p + 5, pl.ds(PAD + row - 1, BLOCK), :]
        sums = sums + slot[p + 5, pl.ds(PAD + row + 1, BLOCK), :]
        along = slot[p + 4, rows, :] + slot[p + 6, rows, :]
        return centre, H[1] * sums + jnp.broadcast_to(vt[p + 4, 0:1, :], (BLOCK, 128)) * along

    def sweep1(old, store, reach):
        @pl.loop(0, 4 + 2 * reach)
        def _(i):
            p = i - reach
            for row in range(0, 128, BLOCK):
                centre, total = around1(old, p, row)
                rows = pl.ds(row, BLOCK)
                fresh = j1[p + 4, rows, :] * (g1[p + 4, rows, :] + total)
                store(p, row, (1.0 - OMEGA) * centre + fresh)

    def store_second(p, row, fresh):
        w_b[p + 5, pl.ds(PAD + row, BLOCK), :] = fresh

    def store_error(p, row, fresh):
        e1[p + 3, pl.ds(row, BLOCK), :] = fresh

    def residual1():
        @pl.loop(0, 4)
        def _(p):
            for row in range(0, 128, BLOCK):
                centre, total = around1(w_b, p, row)
                rows = pl.ds(row, BLOCK)
                r1[p, rows, :] = g1[p + 4, rows, :] + total - d1[p, rows, :] * centre

    def shrink0(src, dst, first):
        @pl.loop(0, 4)
        def _(p):
            total = jnp.zeros((128, 128), F32)
            for half in range(2):
                pairs = src[p, half, pl.ds(0, 128, 2), :] + src[p, half, pl.ds(1, 128, 2), :]
                total = total + dot(pairs, compact[half])
            dst[p + first] = total

    def shrink1(src):
        total = jnp.zeros((128, 128), F32)
        for a in range(2):
            for b in range(2):
                for p in range(4):
                    first = 4 * a + 2 * b
                    pairs = src[p, pl.ds(first, 16, 8), :] + src[p, pl.ds(first + 1, 16, 8), :]
                    lhs[a, pl.ds(b * 4 + p, 16, 8), :] = pairs
            total = total + dot(lhs[a], fold[a])
        return total

    early = []
    for i in range(2):
        for half in range(2):
            lanes = pl.ds(half * 128, 128)
            early.append(
                pair(
                    4 + 2 * i + half,
                    (source.at[2 + i, :, lanes], g0.at[i, half]),
                    (source.at[i, :, lanes], g0.at[6 + i, half]),
                )
            )
    early.append(pair(2, (vt.at[4:8], vt.at[0:4]), (vt.at[4:8], vt.at[8:12])))
    for both in early:
        both.start()
    for copy in loads:
        copy.wait()
    shrink0(r0, r1, 0)

    @pl.loop(0, 4)
    def _(p):
        coupled = 2.0 * vertical[p]
        for half in range(2):
            for row in range(0, 256, 64):
                rows = pl.ds(row, 64)
                diagonal = coupled + 4.0 * H[0] + r0[p, half, rows, :]
                d0[p, half, rows, :] = diagonal
                j0[p + 2, half, rows, :] = OMEGA / diagonal
        diagonal = coupled + 4.0 * H[1] + r1[p]
        d1[p] = diagonal
        j1[p + 4] = OMEGA / diagonal

    def send_blocks(f, v, dst):
        for x in range(16):
            dst[f, 8 * tile_of(x) : 8 * tile_of(x) + 8, :] = exchange_parts(v[8 * x : 8 * x + 8])

    send_blocks(0, shrink1(r1), send_s)
    plane = lane_iota() // 16 % 4
    coupling = jnp.zeros((8, 128), F32)
    for p in range(4):
        coupling = jnp.where(plane == p, vertical[p], coupling)
    for x in range(16):
        send_s[1, 8 * x : 8 * x + 8, :] = coupling
    finish = all_rows(0, send_s, True, recv_s)
    early.append(pair(8, (j0.at[4:6], j0.at[0:2]), (j0.at[2:4], j0.at[6:8])))
    late = pair(9, (j1.at[6:8], j1.at[2:4]), (j1.at[4:6], j1.at[8:10]))
    later = pair(12, (j1.at[4:6], j1.at[0:2]), (j1.at[6:8], j1.at[10:12]))
    early[-1].start()
    late.start()
    finish()

    lane, row = lane_iota(), row_iota()

    def tile(p):
        return pl.ds(8 * p, 8)

    def unpack(v):
        return [
            [v[8 * (8 * b + 2 * p + a) : 8 * (8 * b + 2 * p + a) + 8] for p in range(4)]
            for a in range(2)
            for b in range(2)
        ]

    def shrink2(v):
        result = []
        for a in range(2):
            mine = []
            for p in range(4):
                t = v[2 * a][p] + v[2 * a + 1][p]
                t = t + jnp.where(row % 2 == 1, roll_rows(t, 1), roll_rows(t, -1))
                mine.append(0.25 * t)
            result.append(mine)
        return result

    def shrink3(v):
        mine = []
        for p in range(4):
            t = v[0][p] + v[1][p]
            t = t + jnp.where(row % 4 >= 2, roll_rows(t, 2), roll_rows(t, -2))
            mine.append(0.25 * t)
        return [mine]

    couplings = unpack(recv_s[1].T)[0]
    for p in range(4):
        vl[0, tile(p), :] = jnp.where(lane == 0, 0.0, couplings[p]) if p == 0 else couplings[p]
        vl[1, tile(p), :] = jnp.where(lane == 127, 0.0, couplings[p]) if p == 3 else couplings[p]
    react2 = unpack(recv_s[0].T)
    own_row = row % 2 == lax.rem(narrow, 2)

    def to_partner(i):
        return pltpu.make_async_remote_copy(
            src_ref=give.at[i], dst_ref=take.at[i], send_sem=p_send.at[i], recv_sem=p_recv.at[i],
            device_id=device_of(ia, lax.rem(ib + 4, GROUP_Y)), device_id_type=MESH,
        )

    def merge(i, v):
        for x in range(2):
            for p in range(4):
                give[i, tile(4 * x + p), :] = v[x][p]
        copy = to_partner(i)
        copy.start()
        copy.wait()
        return [
            [jnp.where(own_row, v[x][p], take[i, tile(4 * x + p), :]) for p in range(4)]
            for x in range(2)
        ]

    def unmerge(v):
        shifted = jnp.where(lax.rem(narrow, 2) == 0, roll_rows(v, 1), roll_rows(v, -1))
        return jnp.where(own_row, v, shifted)

    react3 = merge(0, shrink2(react2))
    react4 = shrink3(react3)
    order = [(2, each) for each in react2] + [(3, each) for each in react3] + [(4, react4[0])]
    for i, (level, lines) in enumerate(order):
        for p in range(4):
            dl[i, tile(p), :] = 2.0 * couplings[p] + 4.0 * H[level] + lines[p]

    @pl.loop(0, 7)
    def _(i):
        def put(n, v):
            cf[i, tile(n), :] = v

        def next_lane(v):
            return roll_lanes(v, -1)

        a = [-vl[0, tile(p), :] for p in range(4)]
        c = [-vl[1, tile(p), :] for p in range(4)]
        b = [dl[i, tile(p), :] for p in range(4)]
        left1, right1 = -a[1] / b[0], -c[1] / b[2]
        left3, right3 = -a[3] / b[2], -c[3] / next_lane(b[0])
        b1 = b[1] + left1 * c[0] + right1 * a[2]
        a1, c1 = left1 * a[0], right1 * c[2]
        b3 = b[3] + left3 * c[2] + right3 * next_lane(a[0])
        a3, c3 = left3 * a[2], right3 * next_lane(c[0])
        for n, v in enumerate((left1, right1, left3, right3)):
            put(n, v)
        left, right = -a3 / b1, -c3 / next_lane(b1)
        put(4, left)
        put(5, right)
        middle = b3 + left * c1 + right * next_lane(a1)
        low, high = left * a1, right * next_lane(c1)
        for k in range(STEPS - 2):
            t = 1 << k
            left = -low / roll_lanes(middle, t)
            right = -high / roll_lanes(middle, -t)
            put(6 + 2 * k, left)
            put(7 + 2 * k, right)
            middle = middle + left * roll_lanes(high, t) + right * roll_lanes(low, -t)
            low, high = left * roll_lanes(low, t), right * roll_lanes(high, -t)
        put(20, 1.0 / middle)
        for n, (below_it, it, above_it) in enumerate(((a1, b1, c1), (a[0], b[0], c[0]), (a[2], b[2], c[2]))):
            inverse = 1.0 / it
            put(21 + 3 * n, inverse)
            put(22 + 3 * n, below_it * inverse)
            put(23 + 3 * n, above_it * inverse)

    first_of = {2: 0, 3: 4, 4: 6}
    count_of = {2: 4, 3: 2, 4: 1}

    def solve(level, right):
        solved = []
        for x in range(count_of[level]):
            i = first_of[level] + x

            def at(n, i=i):
                return cf[i, tile(n), :]

            r0_, r1_, r2_, r3_ = right[x]
            odd = r1_ + at(0) * r0_ + at(1) * r2_
            r = r3_ + at(2) * r2_ + at(3) * roll_lanes(r0_, -1)
            r = r + at(4) * odd + at(5) * roll_lanes(odd, -1)
            for k in range(STEPS - 2):
                t = 1 << k
                r = r + at(6 + 2 * k) * roll_lanes(r, t) + at(7 + 2 * k) * roll_lanes(r, -t)
            w3 = r * at(20)
            before = roll_lanes(w3, 1)
            w1 = odd * at(21) - at(22) * before - at(23) * w3
            w0 = r0_ * at(24) - at(25) * before - at(26) * w1
            w2 = r2_ * at(27) - at(28) * w1 - at(29) * w3
            solved.append([w0, w1, w2, w3])
        return solved

    def around(level, event, v, chunks):
        count = count_of[level]
        for x in range(count):
            for p in range(4):
                val[event, pl.ds((x * 4 + p) * 8, 8), :] = v[x][p]
        size = 4 * count
        ys[event, 0, 0:size, :] = val[event, pl.ds(0, size, 8), :]
        ys[event, 1, 0:size, :] = val[event, pl.ds(7, size, 8), :]
        span = pl.ds(0, size)
        if level == 2:
            above_y, below_y = member_narrow(narrow + 1), member_narrow(narrow - 1)
            has_y = (narrow < GROUP_Y - 1, narrow > 0)
        else:
            above_y, below_y = ib + 1, ib - 1
            has_y = (place_y < 3, place_y > 0)
        copies = []
        for side, src, dst, there in (
            (0, val.at[event, pl.ds(32 * (count - 1), 32)], hx.at[event, 0], device_of(member_wide(wide + 1), ib)),
            (1, val.at[event, pl.ds(0, 32)], hx.at[event, 1], device_of(member_wide(wide - 1), ib)),
            (2, ys.at[event, 1, span], hy.at[event, 0, span], device_of(ia, above_y)),
            (3, ys.at[event, 0, span], hy.at[event, 1, span], device_of(ia, below_y)),
        ):
            copies.append(
                pltpu.make_async_remote_copy(
                    src_ref=src, dst_ref=dst, send_sem=h_send.at[event, side],
                    recv_sem=h_recv.at[event, side], device_id=there, device_id_type=MESH,
                )
            )
        has = (wide < GROUP_Z - 1, wide > 0) + has_y
        for side in range(4):
            pl.when(has[side])(copies[side].start)
        for n in PLAN.get(event, ()):
            chunks[n].start()
        if level > 2:
            pl.semaphore_signal(
                turns.at[event], inc=1, device_id=device_of(ia, lax.rem(ib + 4, GROUP_Y)),
                device_id_type=MESH,
            )
        for side in range(4):
            pl.when(has[side])(copies[side].wait_send)
            pl.when(has[side])(copies[side ^ 1].wait_recv)

        def beside(mine, low, high):
            def rolled(s):
                return roll_rows(mine, s)

            if level == 2:
                return jnp.where(row < 1, low, rolled(1)) + jnp.where(row >= 7, high, rolled(-1))
            if level == 3:
                before = jnp.where(row == 0, low, jnp.where(row == 1, rolled(3), rolled(2)))
                after = jnp.where(row == 7, high, jnp.where(row == 6, rolled(-3), rolled(-2)))
                return before + after
            even = row % 2 == 0
            before = jnp.where(row >= 4, rolled(4), jnp.where(even, low, rolled(-3)))
            after = jnp.where(row < 4, rolled(4), jnp.where(even, rolled(3), high))
            return before + after

        result = []
        for x in range(count):
            mine = []
            for p in range(4):
                total = v[x - 1][p] if x else hx[event, 0, tile(p), :]
                total = total + (v[x + 1][p] if x + 1 < count else hx[event, 1, tile(p), :])
                low = jnp.broadcast_to(hy[event, 0, pl.ds(x * 4 + p, 1), :], (8, 128))
                high = jnp.broadcast_to(hy[event, 1, pl.ds(x * 4 + p, 1), :], (8, 128))
                mine.append(total + beside(v[x][p], low, high))
            result.append(mine)
        return result

    def relax(level, target, total):
        return solve(
            level,
            [
                [target[a][g] + H[level] * total[a][g] for g in range(4)]
                for a in range(count_of[level])
            ],
        )

    def residual(level, target, v, total):
        result = []
        for a in range(count_of[level]):
            down, up = below(v[a], 1), above(v[a], 1)
            result.append([
                target[a][g] + H[level] * total[a][g] - dl[first_of[level] + a, tile(g), :] * v[a][g]
                + vl[0, tile(g), :] * down[g] + vl[1, tile(g), :] * up[g]
                for g in range(4)
            ])
        return result

    def load(ref, count):
        return [[ref[a, tile(g), :] for g in range(4)] for a in range(count)]

    def keep(ref, v):
        for a in range(len(v)):
            for g in range(4):
                ref[a, tile(g), :] = v[a][g]

    def lines(chunks):
        target2 = lambda: unpack(turn)
        v = solve(2, target2())
        v = relax(2, target2(), around(2, 0, v, chunks))
        r = residual(2, target2(), v, around(2, 1, v, chunks))
        keep(rhs2, v)
        keep(rhs3, merge(1, shrink2(r)))
        back = to_partner(2)

        @pl.when(core == 0)
        def _():
            for e in range(2, 9):
                pl.semaphore_wait(turns.at[e], 1)
                for n in PLAN.get(e, ()):
                    chunks[n].start()
            back.wait_recv()

        @pl.when(core == 1)
        def _():
            target3 = lambda: load(rhs3, 2)
            v = solve(3, target3())
            v = relax(3, target3(), around(3, 2, v, chunks))
            r = residual(3, target3(), v, around(3, 3, v, chunks))
            keep(res, v)
            target4 = shrink3(r)
            v = solve(4, target4)
            for e in range(3):
                v = relax(4, target4, around(4, 4 + e, v, chunks))
            w = load(res, 2)
            v = [[w[a][g] + v[0][g] for g in range(4)] for a in range(2)]
            v = relax(3, target3(), around(3, 7, v, chunks))
            v = relax(3, target3(), around(3, 8, v, chunks))
            for x in range(2):
                for p in range(4):
                    give[2, tile(4 * x + p), :] = v[x][p]
                    take[2, tile(4 * x + p), :] = v[x][p]
            back.start()
            back.wait_send()

        v = [[unmerge(take[2, tile(4 * x + p), :]) for p in range(4)] for x in range(2)]
        w = load(rhs2, 4)
        v = [[w[x][p] + v[x // 2][p] for p in range(4)] for x in range(4)]
        v = relax(2, target2(), around(2, 9, v, chunks))
        v = relax(2, target2(), around(2, 10, v, chunks))
        for a in range(2):
            for b in range(2):
                for p in range(4):
                    turn[pl.ds(8 * (8 * b + 2 * p + a), 8), :] = v[2 * a + b][p]

    nacc[...] = jnp.zeros((CYCLES, 8, 128), F32)

    for both in early:
        both.wait()

    @pl.loop(0, CYCLES)
    def _(cycle):
        @pl.when(cycle == 0)
        def _():
            @pl.loop(0, 8)
            def _(p):
                for half in range(2):
                    for row in range(0, 256, 64):
                        fresh = j0[p, half, pl.ds(row, 64), :] * g0[p, half, pl.ds(row, 64), :]
                        v_c[p + 1, half, pl.ds(PAD + row, 64), :] = fresh

            sweep0(v_c, v_b, -1, 6)
            residual0(v_b, True, 0, 1, 2)
            late.wait()

        @pl.when(cycle > 0)
        def _():
            sweep0(v_a, v_d, 0, 2, 3)
            finish = exchange0(v_d, 0)
            sweep0(v_a, v_d, 1, 2)
            sweep0(v_d, v_b, 1, 2)
            finish()
            sweep0(v_d, v_b, 0, 2, 3)
            finish = exchange0(v_b, 1)
            residual0(v_b, True, 0, 1, 2)
            finish()

        residual0(v_b, True, 0, 0, 2, 3)
        shrink0(r0, g1, 4)
        both = pair(3, (g1.at[6:8], g1.at[2:4]), (g1.at[4:6], g1.at[8:10]))
        both.start()
        both.wait()

        @pl.loop(0, 8)
        def _(p):
            w_a[p + 3, pl.ds(PAD, 128), :] = j1[p + 2] * g1[p + 2]

        sweep1(w_a, store_second, 1)
        residual1()

        chunks = []

        def chunk(up, down, steps=1):
            i = len(chunks)
            chunks.append(Pair(up, down, c_send.at[i], c_recv.at[i], steps))

        for i in range(2):
            chunk((g1.at[4 + i], g1.at[i]), (g1.at[6 + i], g1.at[10 + i]))
        rows = pl.ds(PAD, 128)
        chunk((w_b.at[8, rows], w_b.at[0, rows]), (w_b.at[5, rows], w_b.at[13, rows]), 2)
        for i in range(3):
            chunk(
                (w_b.at[5 + i, rows], w_b.at[1 + i, rows]),
                (w_b.at[6 + i, rows], w_b.at[10 + i, rows]),
            )
        for i in range(2):
            for half in range(2):
                for row in range(0, 256, 128):
                    rows = pl.ds(PAD + row, 128)
                    chunk(
                        (v_b.at[4 + i, half, rows], v_b.at[i, half, rows]),
                        (v_b.at[4 + i, half, rows], v_b.at[8 + i, half, rows]),
                    )

        send_blocks(0, shrink1(r1), send_r)
        finish = all_rows(1, send_r, True, recv_r)
        chunks[0].start()
        chunks[1].start()
        chunks[10].start()
        pl.when(cycle == 0)(later.start)
        finish()
        turn[...] = recv_r[0].T
        lines(chunks)
        back_r[0] = turn[...].T
        finish = all_rows(2, back_r, False, got_r)
        chunks[9].start()
        chunks[11].start()
        chunks[12].start()
        chunks[13].start()
        finish()

        for x in range(16):
            piece = got_r[0, 8 * tile_of(x) : 8 * tile_of(x) + 8, :]
            got_a[1, 8 * x : 8 * x + 8, :] = exchange_parts(piece)
        ends[0] = got_a[1, pl.ds(3, 32, 4), :]
        ends[1] = got_a[1, pl.ds(0, 32, 4), :]
        whole = pair(10, (got_a.at[1], got_a.at[0]), (got_a.at[1], got_a.at[2]))
        outer = pair(11, (ends.at[0], beyond.at[0]), (ends.at[1], beyond.at[1]), 2)
        whole.start()
        outer.start()
        pl.when(cycle == 0)(later.wait)
        for side in (1, 0, 2):
            if side == 0:
                for each in chunks:
                    each.wait()
                whole.wait()
                outer.wait()
            for a in range(2):
                grown[a] = dot(got_a[side], unfold[a])
            for a in range(2):
                for b in range(2):
                    for p in range(4):
                        piece = grown[a, pl.ds(b * 4 + p, 16, 8), :]
                        for i in range(2):
                            rows = pl.ds(PAD + 4 * a + 2 * b + i, 16, 8)
                            q = 4 * side + p + 1
                            w_a[q, rows, :] = w_b[q, rows, :] + piece
        for side in range(2):
            for a in range(2):
                grown[a, 0:32, :] = dot(beyond[side], unfold[a])
                for b in range(2):
                    piece = grown[a, pl.ds(b, 16, 2), :]
                    for i in range(2):
                        rows = pl.ds(PAD + 4 * a + 2 * b + i, 16, 8)
                        w_a[13 * side, rows, :] = w_b[13 * side, rows, :] + piece
        sweep1(w_a, store_second, 4)
        sweep1(w_b, store_error, 3)

        @pl.loop(0, 10)
        def _(p):
            for half in range(2):
                piece = dot(e1[p], spread[half])
                for i in range(2):
                    rows = pl.ds(PAD + i, 128, 2)
                    v_c[p, half, rows, :] = v_b[p, half, rows, :] + piece

        sweep0(v_c, v_b, -2, 8)
        sweep0(v_b, v_a, -1, 6)
        residual0(v_a, False, cycle, 0, 4)

    stores = []
    for p in range(4):
        for half in range(2):
            stores.append(
                pltpu.make_async_copy(
                    v_a.at[p + 3, half, pl.ds(PAD, 256)],
                    out.at[p, :, pl.ds(half * 128, 128)],
                    in_sem.at[0, p, half],
                )
            )
    for copy in stores:
        copy.start()

    sums = [jnp.sum(nacc[c], axis=0, keepdims=True) for c in range(CYCLES)]
    sums = [each + roll_lanes(each, 64) for each in sums]
    first = lax.broadcasted_iota(jnp.int32, (1, 128), 1) < 64
    part[0] = jnp.broadcast_to(jnp.where(first, sums[0], sums[1]), (128, 128))
    all_rows(3, part, True, nz)()
    total = jnp.sum(nz[0], axis=0, keepdims=True)
    norms[0] = jnp.sum(jnp.where(first, total, 0.0)) * (1.0 / (512 * 256 * 256))
    norms[1] = jnp.sum(jnp.where(first, 0.0, total)) * (1.0 / (512 * 256 * 256))
    for copy in stores:
        copy.wait()


def vmem(*shape):
    return pltpu.VMEM(shape, F32)


def shards(source, vertical, reaction):
    dma = pltpu.SemaphoreType.DMA
    solved, norms = pl.pallas_call(
        kernel,
        out_shape=(
            jax.ShapeDtypeStruct((4, 256, 256), F32),
            jax.ShapeDtypeStruct((CYCLES,), F32),
        ),
        in_specs=[
            pl.BlockSpec(memory_space=pltpu.HBM),
            pl.BlockSpec(memory_space=pltpu.SMEM),
            pl.BlockSpec(memory_space=pltpu.HBM),
        ],
        out_specs=(pl.BlockSpec(memory_space=pltpu.HBM), pl.BlockSpec(memory_space=pltpu.SMEM)),
        scratch_shapes=[
            vmem(10, 2, 256 + 2 * PAD, 128),
            vmem(10, 2, 256 + 2 * PAD, 128),
            vmem(10, 2, 256 + 2 * PAD, 128),
            vmem(10, 2, 256 + 2 * PAD, 128),
            vmem(8, 2, 256, 128),
            vmem(4, 2, 256, 128),
            vmem(8, 2, 256, 128),
            vmem(4, 2, 256, 128),
            vmem(12, 8, 128),
            vmem(14, 128 + 2 * PAD, 128),
            vmem(14, 128 + 2 * PAD, 128),
            vmem(12, 128, 128),
            vmem(4, 128, 128),
            vmem(12, 128, 128),
            vmem(4, 128, 128),
            vmem(10, 128, 128),
            pltpu.VMEM((2, 128, 128), jnp.bfloat16),
            pltpu.VMEM((2, 128, 128), jnp.bfloat16),
            vmem(2, 128, 128),
            pltpu.VMEM((2, 128, 128), jnp.bfloat16),
            pltpu.VMEM((2, 128, 128), jnp.bfloat16),
            vmem(2, 128, 128),
            vmem(2, 128, 128),
            vmem(1, 128, 128),
            vmem(1, 128, 128),
            vmem(128, 128),
            vmem(1, 128, 128),
            vmem(1, 128, 128),
            vmem(3, 128, 128),
            vmem(2, 32, 128),
            vmem(2, 32, 128),
            vmem(2, 128, 128),
            vmem(7, 32, 128),
            vmem(2, 32, 128),
            vmem(7, 240, 128),
            vmem(EVENTS, 128, 128),
            vmem(EVENTS, 2, 32, 128),
            vmem(EVENTS, 2, 16, 128),
            vmem(EVENTS, 2, 16, 128),
            vmem(4, 32, 128),
            vmem(2, 32, 128),
            vmem(2, 32, 128),
            vmem(3, 64, 128),
            vmem(3, 64, 128),
            vmem(CYCLES, 8, 128),
            vmem(1, 128, 128),
            vmem(1, 128, 128),
            dma((2, 4, 2)),
            dma((13, 2)),
            dma((13, 2)),
            dma((14, 2)),
            dma((14, 2)),
            dma((4,)),
            dma((4,)),
            dma((3,)),
            dma((3,)),
            pltpu.SemaphoreType.REGULAR((9,)),
            dma((EVENTS, 4)),
            dma((EVENTS, 4)),
        ],
        compiler_params=pltpu.CompilerParams(
            collective_id=0, has_side_effects=True, vmem_limit_bytes=63 * 1024 * 1024
        ),
    )(source, vertical, reaction)
    return solved, norms


def solution(mesh):
    planes = P(("gz", "gy"), None, None)
    return jax.shard_map(
        shards,
        mesh=mesh,
        in_specs=(planes, P(("gz", "gy")), planes),
        out_specs=(planes, P()),
        check_vma=False,
    )
```
